32 devices in a mesh: dp: 2 (over x), vp: 4 (over z), tp: 4 (over y, core).
Axes of the slice: x: 2, y: 2, z: 4, core: 2. Of those that a mesh axis runs over, the one named last changes fastest.
Arguments:
- hidden: bfloat16 [128, 1536], P('dp', 'tp'), parts along dimension 0
- lnf_gain: float32 [1536], P('tp')
- lnf_bias: float32 [1536], P('tp')
- emb_table: bfloat16 [250880, 1536], P('vp', 'tp')
- next_tok: int32 [128], P('dp'), parts along dimension 0
- eln_gain: float32 [1536], P('tp')
- eln_bias: float32 [1536], P('tp')
Outputs:
- output 1: float32 [128, 250880], P('dp', ('vp', 'tp')), parts along dimension 0
- output 2: float32 [128], P('dp'), parts along dimension 0
- output 3: bfloat16 [128, 1536], P('dp', 'tp'), parts along dimension 0
There are 2 independent parts. The reference program is written for one: setup_inputs(seed, part) draws one part's arguments, and reference() takes and returns one part's arrays. A program takes and returns all parts, laid end to end along the dimension named above; an argument that names none is the same for every part.
All inputs are finite; a program needn't handle non-finite values.
Results may differ from the reference program's by a relative error of at most 0.001.
Values sent between devices are 32-bit elements.
A program may use at most 1 GiB of HBM per device.

```python
import jax
import jax.numpy as jnp

BATCH_ROWS = 64
D = 1536
VOCAB_SIZE = 250880
VP_BLOCKS = 4
HOT_COUNT = min(2, VP_BLOCKS)
NORM_EPS = 1e-5


def draw_tokens(key):
    key_hot, key_pick, key_any, key_sel, key_pos = jax.random.split(key, 5)
    block_len = VOCAB_SIZE // VP_BLOCKS
    hot_blocks = jax.random.permutation(key_hot, VP_BLOCKS)[:HOT_COUNT]
    hot_pick = jax.random.randint(key_pick, (BATCH_ROWS,), 0, HOT_COUNT)
    any_block = jax.random.randint(key_any, (BATCH_ROWS,), 0, VP_BLOCKS)
    use_hot = jax.random.randint(key_sel, (BATCH_ROWS,), 0, 4) < 3
    tok_block = jnp.where(use_hot, hot_blocks[hot_pick], any_block)
    tok_within = jax.random.randint(key_pos, (BATCH_ROWS,), 0, block_len)
    return (tok_block * block_len + tok_within).astype(jnp.int32)


def setup_inputs(seed: int = 0, part: int = 0) -> dict:
    shared_key, part_root = jax.random.split(jax.random.key(seed))
    part_key = jax.random.fold_in(part_root, part)
    key_hid, key_off, key_tok = jax.random.split(part_key, 3)
    key_tab, key_rowm, key_g1, key_b1, key_g2, key_b2 = jax.random.split(shared_key, 6)
    col_pos = jnp.arange(D, dtype=jnp.float32) / D
    hidden = jax.random.normal(key_hid, (BATCH_ROWS, D), jnp.float32) * (0.5 + 1.5 * col_pos)
    hidden = hidden + jax.random.normal(key_off, (BATCH_ROWS, 1), jnp.float32) * (1.0 + 2.0 * col_pos)
    tab_vals = jax.random.normal(key_tab, (VOCAB_SIZE, D), jnp.float32) * (0.5 + col_pos)
    tab_vals = (tab_vals + jax.random.normal(key_rowm, (VOCAB_SIZE, 1), jnp.float32)) * (D ** -0.5)
    return {
        "hidden": hidden.astype(jnp.bfloat16),
        "lnf_gain": 1.5 + 0.5 * jax.random.normal(key_g1, (D,), jnp.float32),
        "lnf_bias": 0.5 * jax.random.normal(key_b1, (D,), jnp.float32),
        "emb_table": tab_vals.astype(jnp.bfloat16),
        "next_tok": draw_tokens(key_tok),
        "eln_gain": 1.0 + 0.3 * jax.random.normal(key_g2, (D,), jnp.float32),
        "eln_bias": 0.5 * jax.random.normal(key_b2, (D,), jnp.float32),
    }


def layer_norm(rows_in, norm_gain, norm_bias):
    rows_f32 = rows_in.astype(jnp.float32)
    row_mean = jnp.mean(rows_f32, axis=-1, keepdims=True)
    row_var = jnp.mean(rows_f32 * rows_f32, axis=-1, keepdims=True) - row_mean * row_mean
    return (rows_f32 - row_mean) / jnp.sqrt(row_var + NORM_EPS) * norm_gain + norm_bias


def reference(hidden, lnf_gain, lnf_bias, emb_table, next_tok, eln_gain, eln_bias):
    normed = layer_norm(hidden, lnf_gain, lnf_bias).astype(jnp.bfloat16)
    logits = jnp.dot(normed, emb_table.T, preferred_element_type=jnp.float32)
    log_sum = jax.nn.logsumexp(logits, axis=-1)
    logprobs = logits - log_sum[:, None]
    tok_rows = jnp.take(emb_table, next_tok, axis=0)
    next_in = layer_norm(tok_rows, eln_gain, eln_bias).astype(jnp.bfloat16)
    return (logprobs, log_sum, next_in)
```

```python
import functools

import jax
import jax.numpy as jnp
from jax import lax
from jax.experimental import pallas as pl
from jax.experimental.pallas import tpu as pltpu
from jax.sharding import PartitionSpec as P

NORM_EPS = 1e-5
CHUNK = 1024
LANES = 128
DEPTH = 3
MESH = pl.DeviceIdType.MESH


def head_kernel(
    n_vp, n_full, rem, width,
    hid_hbm, gain1_hbm, bias1_hbm, tab_hbm, tok_hbm, gain2_hbm, bias2_hbm,
    logits, lse_out, next_out,
    hid, gain1, bias1, gain2, bias2, tok, tab, tab_rem, normed, picked, picked_rx,
    tx, rx, acc, y_rx, m_run, s_run, stat_slots, stat2_slots, lse_slots,
    in_sem, tab_sem, rem_sem, stat_send, stat_recv, stat2_send, stat2_recv,
    tx_send, tx_recv, y_send, y_recv, pick_send, pick_recv, lse_send, lse_recv,
):
    rows = hid.shape[0]
    n_chunks = n_full + 1
    seg = n_full * CHUNK + rem
    rem_pad = tab_rem.shape[1]
    vp = lax.axis_index("vp")
    tp = lax.axis_index("tp")
    chip_y = tp // 2
    core = lax.rem(tp, 2)
    sibling = tp + 1 - 2 * core
    across = lax.rem(tp + 2, 4)
    my_rank = vp * 4 + tp

    peers = []
    for dz in reversed(range(n_vp)):
        for dt in reversed(range(4)):
            if dz or dt:
                peers.append((dz, dt, dz * 4 + dt))

    def peer_id(dz, dt):
        return {"vp": lax.rem(vp + dz, n_vp), "tp": lax.rem(tp + dt, 4)}

    barrier = pltpu.get_barrier_semaphore()
    for dz, dt, _ in peers:
        pl.semaphore_signal(barrier, inc=1, device_id=peer_id(dz, dt), device_id_type=MESH)

    def seg_start(phase, which):
        y = chip_y + (1 - phase) * (1 - 2 * chip_y)
        c = core + (1 - which) * (1 - 2 * core)
        return (y * 2 + c) * seg

    def row_start(i, which):
        phase = jnp.where(i >= n_full, 1, 0)
        k = i - phase * n_full
        return pl.multiple_of(seg_start(phase, which) + k * CHUNK, 64)

    def tab_copy(i, which):
        slot = lax.rem(i, DEPTH)
        return pltpu.make_async_copy(
            tab_hbm.at[pl.ds(row_start(i, which), CHUNK), :], tab.at[slot, which], tab_sem.at[slot, which]
        )

    def rem_start(phase, which):
        return pl.multiple_of(seg_start(phase, which) + n_full * CHUNK, 64)

    def rem_copy(phase, which):
        return pltpu.make_async_copy(
            tab_hbm.at[pl.ds(rem_start(phase, which), rem), :],
            tab_rem.at[phase * 2 + which, pl.ds(0, rem), :],
            rem_sem.at[phase * 2 + which],
        )

    small = [
        pltpu.make_async_copy(hid_hbm, hid, in_sem.at[0]),
        pltpu.make_async_copy(gain1_hbm, gain1, in_sem.at[1]),
        pltpu.make_async_copy(bias1_hbm, bias1, in_sem.at[2]),
        pltpu.make_async_copy(gain2_hbm, gain2, in_sem.at[3]),
        pltpu.make_async_copy(bias2_hbm, bias2, in_sem.at[4]),
        pltpu.make_async_copy(tok_hbm, tok, in_sem.at[5]),
    ]
    for copy in small:
        copy.start()
    for i in range(min(DEPTH - 1, 2 * n_full)):
        for which in range(2):
            tab_copy(i, which).start()
    for phase in range(2):
        for which in range(2):
            rem_copy(phase, which).start()

    picked[...] = jnp.zeros_like(picked)
    m_run[...] = jnp.full_like(m_run, -jnp.inf)
    s_run[...] = jnp.zeros_like(s_run)
    empty = jnp.zeros((1, 8, LANES), jnp.float32)
    stat_slots[pl.ds(tp, 1)] = empty
    stat2_slots[pl.ds(tp, 1)] = empty
    lse_slots[pl.ds(my_rank, 1)] = empty
    tab_rem[:, rem:, :] = jnp.zeros((4, rem_pad - rem, width), jnp.bfloat16)

    lane = lax.broadcasted_iota(jnp.int32, (rows, LANES), 1)

    def stat_tile(x):
        s1 = jnp.sum(x, axis=1, keepdims=True)
        s2 = jnp.sum(x * x, axis=1, keepdims=True)
        both = jnp.where(lane == 0, s1, jnp.where(lane == 1, s2, 0.0))
        return both.T[:8, :]

    def stat_copy(slots, send, recv, d):
        return pltpu.make_async_remote_copy(
            src_ref=slots.at[tp], dst_ref=slots.at[tp], send_sem=send.at[d - 1], recv_sem=recv.at[d - 1],
            device_id=peer_id(0, d), device_id_type=MESH,
        )

    def norm(x, slots, send, recv, gain, bias):
        for d in (2, 3, 1):
            stat_copy(slots, send, recv, d).wait_recv()
        total = (slots[0] + slots[1]) + (slots[2] + slots[3])
        full_width = 4.0 * width
        mean = total[0:1, :] / full_width
        var = total[1:2, :] / full_width - mean * mean
        inv = lax.rsqrt(var + NORM_EPS)
        row = lax.broadcasted_iota(jnp.int32, (8, LANES), 0)
        back = jnp.where(row == 0, mean, inv).T
        mean_c = back[:rows, 0:1]
        inv_c = back[:rows, 1:2]
        return (x - mean_c) * inv_c * gain + bias

    small[0].wait()
    x1 = hid[...].astype(jnp.float32)
    stat_slots[pl.ds(tp, 1), :, 0:rows] = stat_tile(x1)[None]
    for copy in small[1:]:
        copy.wait()
    pl.semaphore_wait(barrier, len(peers))
    for d in (2, 3, 1):
        stat_copy(stat_slots, stat_send, stat_recv, d).start()
    normed[...] = norm(
        x1, stat_slots, stat_send, stat_recv, gain1[...].reshape(1, width), bias1[...].reshape(1, width)
    ).astype(jnp.bfloat16)

    def tx_copy(e, cols=None):
        view = (lambda r: r.at[e]) if cols is None else (lambda r: r.at[e, :, pl.ds(0, cols)])
        return pltpu.make_async_remote_copy(
            src_ref=view(tx), dst_ref=view(rx), send_sem=tx_send.at[e], recv_sem=tx_recv.at[e],
            device_id={"tp": sibling}, device_id_type=MESH,
        )

    def y_copy(e, cols=None):
        view = (lambda r: r.at[e]) if cols is None else (lambda r: r.at[e, :, pl.ds(0, cols)])
        return pltpu.make_async_remote_copy(
            src_ref=view(acc), dst_ref=view(y_rx), send_sem=y_send.at[e], recv_sem=y_recv.at[e],
            device_id={"tp": across}, device_id_type=MESH,
        )

    def partial(block):
        return lax.dot_general(
            normed[...], block, (((1,), (1,)), ((), ())), preferred_element_type=jnp.float32
        )

    tok_col = jnp.broadcast_to(tok[...], (8, rows)).T[:, 0:1]
    tok_local = tok_col - vp * (4 * seg)

    def add_picked(block, start):
        n = block.shape[0]
        at = lax.broadcasted_iota(jnp.int32, (rows, n), 1)
        hot = jnp.where(at == tok_local - start, 1.0, 0.0).astype(jnp.bfloat16)
        picked[...] += lax.dot_general(
            hot, block, (((1,), (0,)), ((), ())), preferred_element_type=jnp.float32
        )

    def run_phase(phase):
        base = phase * n_chunks

        def body(i, carry):
            k = i - phase * n_full
            e = base + k

            @pl.when(i + DEPTH - 1 < 2 * n_full)
            def _():
                tab_copy(i + DEPTH - 1, 0).start()
                tab_copy(i + DEPTH - 1, 1).start()

            slot = lax.rem(i, DEPTH)
            tab_copy(i, 0).wait()
            tx[e] = partial(tab[slot, 0])
            tab_copy(i, 1).wait()
            acc[e] = partial(tab[slot, 1])
            tx_copy(e).start()

            @pl.when(k > 0)
            def _():
                tx_copy(e - 1).wait_recv()
                acc[e - 1] = acc[e - 1] + rx[e - 1]

            add_picked(tab[slot, 0], row_start(i, 0))
            add_picked(tab[slot, 1], row_start(i, 1))
            if phase == 0:
                @pl.when(k > 0)
                def _():
                    y_copy(e - 1).start()
            return carry

        lax.fori_loop(phase * n_full, (phase + 1) * n_full, body, 0)
        last = base + n_full
        rem_copy(phase, 0).wait()
        tx[last, :, 0:rem_pad] = partial(tab_rem[phase * 2])
        rem_copy(phase, 1).wait()
        acc[last, :, 0:rem_pad] = partial(tab_rem[phase * 2 + 1])
        tx_copy(last, rem_pad).start()
        tx_copy(last - 1).wait_recv()
        acc[last - 1] = acc[last - 1] + rx[last - 1]
        for which in range(2):
            block = tab_rem[phase * 2 + which]
            at = lax.broadcasted_iota(jnp.int32, (rows, rem_pad), 1)
            hit = (at == tok_local - rem_start(phase, which)) & (at < rem)
            hot = jnp.where(hit, 1.0, 0.0).astype(jnp.bfloat16)
            picked[...] += lax.dot_general(
                hot, block, (((1,), (0,)), ((), ())), preferred_element_type=jnp.float32
            )
        if phase == 0:
            y_copy(last - 1).start()
        tx_copy(last, rem_pad).wait_recv()
        acc[last, :, 0:rem_pad] = acc[last, :, 0:rem_pad] + rx[last, :, 0:rem_pad]

    run_phase(0)
    y_copy(n_full, rem_pad).start()
    run_phase(1)

    def pick_copy(dz):
        return pltpu.make_async_remote_copy(
            src_ref=picked, dst_ref=picked_rx.at[vp], send_sem=pick_send.at[dz - 1], recv_sem=pick_recv.at[dz - 1],
            device_id=peer_id(dz, 0), device_id_type=MESH,
        )

    for dz in range(1, n_vp):
        pick_copy(dz).start()
    picked_rx[pl.ds(vp, 1)] = picked[...][None]
    for dz in range(1, n_vp):
        pick_copy(dz).wait_recv()
    x2 = picked_rx[0]
    for z in range(1, n_vp):
        x2 = x2 + picked_rx[z]
    stat2_slots[pl.ds(tp, 1), :, 0:rows] = stat_tile(x2)[None]
    for d in (2, 3, 1):
        stat_copy(stat2_slots, stat2_send, stat2_recv, d).start()
    next_out[...] = norm(
        x2, stat2_slots, stat2_send, stat2_recv, gain2[...].reshape(1, width), bias2[...].reshape(1, width)
    ).astype(jnp.bfloat16)

    def absorb(k, cols):
        e = n_chunks + k
        blocks = cols // LANES
        top = m_run[...]
        for b in range(blocks):
            sl = pl.ds(b * LANES, LANES)
            z = acc[e, :, sl] + y_rx[k, :, sl]
            logits[k, :, sl] = z
            if cols != CHUNK and (b + 1) * LANES > rem:
                z = jnp.where(lane < rem - b * LANES, z, -jnp.inf)
            top = jnp.maximum(top, z)
        total = s_run[...] * jnp.exp(m_run[...] - top)
        for b in range(blocks):
            z = logits[k, :, pl.ds(b * LANES, LANES)]
            if cols != CHUNK and (b + 1) * LANES > rem:
                z = jnp.where(lane < rem - b * LANES, z, -jnp.inf)
            total = total + jnp.exp(z - top)
        m_run[...] = top
        s_run[...] = total

    def absorb_body(k, carry):
        y_copy(k).wait_recv()
        absorb(k, CHUNK)
        return carry

    lax.fori_loop(0, n_full, absorb_body, 0)
    y_copy(n_full, rem_pad).wait_recv()
    absorb(n_full, rem_pad)

    m_t = m_run[...].T
    top = jnp.max(m_t, axis=0, keepdims=True)
    tot = jnp.sum(s_run[...].T * jnp.exp(m_t - top), axis=0, keepdims=True)
    row = lax.broadcasted_iota(jnp.int32, (8, rows), 0)
    lse_slots[pl.ds(my_rank, 1), :, 0:rows] = jnp.where(row == 0, top, tot)[None]

    def lse_copy(dz, dt, j):
        return pltpu.make_async_remote_copy(
            src_ref=lse_slots.at[my_rank], dst_ref=lse_slots.at[my_rank],
            send_sem=lse_send.at[j - 1], recv_sem=lse_recv.at[j - 1],
            device_id=peer_id(dz, dt), device_id_type=MESH,
        )

    for dz, dt, j in peers:
        lse_copy(dz, dt, j).start()

    def drain(e, carry):
        tx_copy(e).wait_send()
        tx_copy(n_chunks + e).wait_send()
        y_copy(e).wait_send()
        return carry

    lax.fori_loop(0, n_full, drain, 0)
    tx_copy(n_full, rem_pad).wait_send()
    tx_copy(n_chunks + n_full, rem_pad).wait_send()
    y_copy(n_full, rem_pad).wait_send()
    for d in (1, 2, 3):
        stat_copy(stat_slots, stat_send, stat_recv, d).wait_send()
        stat_copy(stat2_slots, stat2_send, stat2_recv, d).wait_send()
    for dz in range(1, n_vp):
        pick_copy(dz).wait_send()

    for dz, dt, j in peers:
        lse_copy(dz, dt, j).wait_recv()
    tops = [lse_slots[r, 0:1, :] for r in range(n_vp * 4)]
    top = functools.reduce(jnp.maximum, tops)
    tot = functools.reduce(
        jnp.add, [lse_slots[r, 1:2, :] * jnp.exp(tops[r] - top) for r in range(n_vp * 4)]
    )
    lse_out[...] = jnp.broadcast_to(top + jnp.log(tot), (8, LANES))
    for dz, dt, j in peers:
        lse_copy(dz, dt, j).wait_send()


def finish_kernel(n_full, rem, logits, lse, next_rows, out_hbm, sum_out, next_out, stage, sem):
    rows = stage.shape[0]
    log_sum = lse[...].T[:rows, 0:1]
    copies = []
    for r in range(rows // 8):
        here = slice(8 * r, 8 * r + 8)
        part = jnp.broadcast_to(log_sum[here], (8, LANES))
        for k in range(n_full + 1):
            cols = CHUNK if k < n_full else rem
            for b in range(0, cols, LANES):
                w = min(LANES, cols - b)
                at = k * CHUNK + b
                stage[here, at:at + w] = logits[k, here, b:b + w] - part[:, :w]
        copy = pltpu.make_async_copy(stage.at[here, :], out_hbm.at[here, :], sem.at[r])
        copy.start()
        copies.append(copy)
    sum_out[...] = lse[0:1, 0:rows]
    next_out[...] = next_rows[...]
    for copy in copies:
        copy.wait()


def solution(mesh):
    n_vp = mesh.shape["vp"]
    assert mesh.shape["tp"] == 4

    def per_device(hidden, lnf_gain, lnf_bias, emb_table, next_tok, eln_gain, eln_bias):
        rows, width = hidden.shape
        seg = emb_table.shape[0] // 4
        n_full, rem = divmod(seg, CHUNK)
        n_chunks = n_full + 1
        rem_pad = -(-rem // LANES) * LANES
        f32, bf16 = jnp.float32, jnp.bfloat16
        dma = pltpu.SemaphoreType.DMA
        hbm = pl.BlockSpec(memory_space=pltpu.HBM)
        vmem = pl.BlockSpec(memory_space=pltpu.VMEM)
        big = (64 * 1024 * 1024)
        logits, lse, next_rows = pl.pallas_call(
            functools.partial(head_kernel, n_vp, n_full, rem, width),
            out_shape=(
                pltpu.VMEM((n_chunks, rows, CHUNK), f32),
                pltpu.VMEM((8, LANES), f32),
                pltpu.VMEM((rows, width), bf16),
            ),
            in_specs=[hbm] * 7,
            out_specs=(vmem, vmem, vmem),
            scratch_shapes=[
                pltpu.VMEM((rows, width), bf16),
                *[pltpu.VMEM((width,), f32)] * 4,
                pltpu.VMEM((1, rows), jnp.int32),
                pltpu.VMEM((DEPTH, 2, CHUNK, width), bf16),
                pltpu.VMEM((4, rem_pad, width), bf16),
                pltpu.VMEM((rows, width), bf16),
                pltpu.VMEM((rows, width), f32),
                pltpu.VMEM((n_vp, rows, width), f32),
                pltpu.VMEM((2 * n_chunks, rows, CHUNK), f32),
                pltpu.VMEM((2 * n_chunks, rows, CHUNK), f32),
                pltpu.VMEM((2 * n_chunks, rows, CHUNK), f32),
                pltpu.VMEM((n_chunks, rows, CHUNK), f32),
                pltpu.VMEM((rows, LANES), f32),
                pltpu.VMEM((rows, LANES), f32),
                pltpu.VMEM((4, 8, LANES), f32),
                pltpu.VMEM((4, 8, LANES), f32),
                pltpu.VMEM((n_vp * 4, 8, LANES), f32),
                dma((6,)), dma((DEPTH, 2)), dma((4,)),
                dma((3,)), dma((3,)), dma((3,)), dma((3,)),
                dma((2 * n_chunks,)), dma((2 * n_chunks,)),
                dma((n_chunks,)), dma((n_chunks,)),
                dma((n_vp - 1,)), dma((n_vp - 1,)),
                dma((n_vp * 4 - 1,)), dma((n_vp * 4 - 1,)),
            ],
            compiler_params=pltpu.CompilerParams(
                collective_id=0, has_side_effects=True, vmem_limit_bytes=52 * 1024 * 1024
            ),
            name="head",
        )(
            *[
                pltpu.with_memory_space_constraint(a, pltpu.HBM)
                for a in (hidden, lnf_gain, lnf_bias, emb_table, next_tok.reshape(1, rows), eln_gain, eln_bias)
            ]
        )
        logprobs, log_sum, next_in = pl.pallas_call(
            functools.partial(finish_kernel, n_full, rem),
            out_shape=(
                jax.ShapeDtypeStruct((rows, seg), f32),
                jax.ShapeDtypeStruct((1, rows), f32),
                jax.ShapeDtypeStruct((rows, width), bf16),
            ),
            in_specs=[vmem, vmem, vmem],
            out_specs=(hbm, vmem, vmem),
            scratch_shapes=[pltpu.VMEM((rows, seg), f32), dma((rows // 8,))],
            compiler_params=pltpu.CompilerParams(vmem_limit_bytes=24 * 1024 * 1024),
            name="finish",
        )(logits, lse, next_rows)
        return logprobs, log_sum.reshape(rows), next_in

    return jax.shard_map(
        per_device,
        mesh=mesh,
        in_specs=(P("dp", "tp"), P("tp"), P("tp"), P("vp", "tp"), P("dp"), P("tp"), P("tp")),
        out_specs=(P("dp", ("vp", "tp")), P("dp"), P("dp", "tp")),
        check_vma=False,
    )
```

```python
import functools

import jax
import jax.numpy as jnp
from jax import lax
from jax.experimental import pallas as pl
from jax.experimental.pallas import tpu as pltpu
from jax.sharding import PartitionSpec as P

NORM_EPS = 1e-5
CHUNK = 768
LANES = 128
DEPTH = 3
LOWEST = -3.0e38
MESH = pl.DeviceIdType.MESH


def head_kernel(
    n_vp, n_full, rem, width,
    hid_hbm, gain1_hbm, bias1_hbm, tab_hbm, tok_hbm, gain2_hbm, bias2_hbm,
    logits, lse_out, next_out,
    hid, gain1, bias1, gain2, bias2, tok, tab, tab_rem, normed, picked, picked_rx,
    tx, rx, acc, y_rx, m_run, s_run, stat_slots, stat2_slots, lse_slots,
    in_sem, tab_sem, rem_sem, stat_send, stat_recv, stat2_send, stat2_recv,
    tx_send, tx_recv, y_send, y_recv, pick_send, pick_recv, lse_send, lse_recv, near_sem,
):
    rows = hid.shape[0]
    n_chunks = n_full + 1
    seg = n_full * CHUNK + rem
    rem_pad = tab_rem.shape[1]
    vp = lax.axis_index("vp")
    tp = lax.axis_index("tp")
    chip_y = tp // 2
    core = lax.rem(tp, 2)
    sibling = tp + 1 - 2 * core
    across = lax.rem(tp + 2, 4)
    my_rank = vp * 4 + tp

    peers = []
    for dz in reversed(range(n_vp)):
        for dt in reversed(range(4)):
            if dz or dt:
                peers.append((dz, dt, dz * 4 + dt))

    def peer_id(dz, dt):
        return {"vp": lax.rem(vp + dz, n_vp), "tp": lax.rem(tp + dt, 4)}

    hid_copy = pltpu.make_async_copy(hid_hbm, hid, in_sem.at[0])
    hid_copy.start()

    has_low = jnp.where(vp > 0, 1, 0)
    has_high = jnp.where(vp < n_vp - 1, 1, 0)

    def signal_vp(sem):
        @pl.when(vp > 0)
        def _():
            pl.semaphore_signal(sem, inc=1, device_id={"vp": vp - 1}, device_id_type=MESH)

        @pl.when(vp < n_vp - 1)
        def _():
            pl.semaphore_signal(sem, inc=1, device_id={"vp": vp + 1}, device_id_type=MESH)

    def signal_tp(sem):
        for dt in (2, 3, 1):
            pl.semaphore_signal(sem, inc=1, device_id=peer_id(0, dt), device_id_type=MESH)

    barrier = pltpu.get_barrier_semaphore()
    signal_tp(barrier)
    signal_vp(barrier)

    def seg_start(phase, which):
        y = chip_y + (1 - phase) * (1 - 2 * chip_y)
        c = core + (1 - which) * (1 - 2 * core)
        return (y * 2 + c) * seg

    def row_start(i, which):
        phase = jnp.where(i >= n_full, 1, 0)
        k = i - phase * n_full
        return pl.multiple_of(seg_start(phase, which) + k * CHUNK, 64)

    def tab_copy(i, which):
        slot = lax.rem(i, DEPTH)
        return pltpu.make_async_copy(
            tab_hbm.at[pl.ds(row_start(i, which), CHUNK), :], tab.at[slot, which], tab_sem.at[slot, which]
        )

    def rem_start(phase, which):
        return pl.multiple_of(seg_start(phase, which) + n_full * CHUNK, 64)

    def rem_copy(phase, which):
        return pltpu.make_async_copy(
            tab_hbm.at[pl.ds(rem_start(phase, which), rem), :],
            tab_rem.at[phase * 2 + which, pl.ds(0, rem), :],
            rem_sem.at[phase * 2 + which],
        )

    small = [
        pltpu.make_async_copy(gain1_hbm, gain1, in_sem.at[1]),
        pltpu.make_async_copy(bias1_hbm, bias1, in_sem.at[2]),
        pltpu.make_async_copy(gain2_hbm, gain2, in_sem.at[3]),
        pltpu.make_async_copy(bias2_hbm, bias2, in_sem.at[4]),
        pltpu.make_async_copy(tok_hbm, tok, in_sem.at[5]),
    ]
    for copy in small:
        copy.start()
    for which in range(2):
        rem_copy(0, which).start()
    for i in range(min(DEPTH - 1, 2 * n_full)):
        for which in range(2):
            tab_copy(i, which).start()
    for which in range(2):
        rem_copy(1, which).start()

    picked[...] = jnp.zeros_like(picked)
    m_run[...] = jnp.full_like(m_run, LOWEST)
    s_run[...] = jnp.zeros_like(s_run)
    tab_rem[:, rem:, :] = jnp.zeros((4, rem_pad - rem, width), jnp.bfloat16)

    lane = lax.broadcasted_iota(jnp.int32, (rows, LANES), 1)

    def stat_row(x):
        s1 = jnp.sum(x, axis=1, keepdims=True)
        s2 = jnp.sum(x * x, axis=1, keepdims=True)
        return jnp.broadcast_to(jnp.concatenate([s1, s2], axis=0), (LANES, LANES)).T[0:1, :]

    def stat_copy(slots, send, recv, d):
        return pltpu.make_async_remote_copy(
            src_ref=slots.at[tp], dst_ref=slots.at[tp], send_sem=send.at[d - 1], recv_sem=recv.at[d - 1],
            device_id=peer_id(0, d), device_id_type=MESH,
        )

    def norm(x, slots, send, recv, gain, bias):
        for d in (1, 2, 3):
            stat_copy(slots, send, recv, d).wait_recv()
        total = (slots[0] + slots[1]) + (slots[2] + slots[3])
        full_width = 4.0 * width
        total = jnp.broadcast_to(total, (8, LANES)) / full_width
        mean = total
        var = pltpu.roll(total, rows, axis=1) - mean * mean
        inv = lax.rsqrt(var + NORM_EPS)
        row = lax.broadcasted_iota(jnp.int32, (8, LANES), 0)
        back = jnp.where(row == 0, mean, inv).T
        mean_c = back[:rows, 0:1]
        inv_c = back[:rows, 1:2]
        return (x - mean_c) * inv_c * gain + bias

    hid_copy.wait()
    x1 = hid[...].astype(jnp.float32)
    stat_slots[pl.ds(tp, 1)] = stat_row(x1)[None]
    for copy in small:
        copy.wait()
    pl.semaphore_wait(barrier, 3 + has_low + has_high)
    for d in (2, 3, 1):
        stat_copy(stat_slots, stat_send, stat_recv, d).start()
    normed[...] = norm(
        x1, stat_slots, stat_send, stat_recv, gain1[...].reshape(1, width), bias1[...].reshape(1, width)
    ).astype(jnp.bfloat16)

    def tx_copy(e, cols=None):
        view = (lambda r: r.at[e]) if cols is None else (lambda r: r.at[e, :, pl.ds(0, cols)])
        return pltpu.make_async_remote_copy(
            src_ref=view(tx), dst_ref=view(rx), send_sem=tx_send.at[e], recv_sem=tx_recv.at[e],
            device_id={"tp": sibling}, device_id_type=MESH,
        )

    def y_copy(e, cols=None):
        view = (lambda r: r.at[e]) if cols is None else (lambda r: r.at[e, :, pl.ds(0, cols)])
        return pltpu.make_async_remote_copy(
            src_ref=view(acc), dst_ref=view(y_rx), send_sem=y_send.at[e], recv_sem=y_recv.at[e],
            device_id={"tp": across}, device_id_type=MESH,
        )

    def partial(block):
        return lax.dot_general(
            normed[...], block, (((1,), (1,)), ((), ())), preferred_element_type=jnp.float32
        )

    tok_col = jnp.broadcast_to(tok[...], (8, rows)).T[:, 0:1]
    tok_local = tok_col - vp * (4 * seg)

    def add_picked(block, start):
        n = block.shape[0]
        at = lax.broadcasted_iota(jnp.int32, (rows, n), 1)
        hot = jnp.where(at == tok_local - start, 1.0, 0.0).astype(jnp.bfloat16)
        picked[...] += lax.dot_general(
            hot, block, (((1,), (0,)), ((), ())), preferred_element_type=jnp.float32
        )

    def add_picked_rem(phase, which):
        at = lax.broadcasted_iota(jnp.int32, (rows, rem_pad), 1)
        hit = (at == tok_local - rem_start(phase, which)) & (at < rem)
        hot = jnp.where(hit, 1.0, 0.0).astype(jnp.bfloat16)
        picked[...] += lax.dot_general(
            hot, tab_rem[phase * 2 + which], (((1,), (0,)), ((), ())), preferred_element_type=jnp.float32
        )

    def run_phase(phase):
        base = phase * n_chunks

        last = base + n_full
        rem_copy(phase, 0).wait()
        tx[last, :, 0:rem_pad] = partial(tab_rem[phase * 2])
        rem_copy(phase, 1).wait()
        acc[last, :, 0:rem_pad] = partial(tab_rem[phase * 2 + 1])
        tx_copy(last, rem_pad).start()
        add_picked_rem(phase, 0)
        add_picked_rem(phase, 1)
        tx_copy(last, rem_pad).wait_recv()
        acc[last, :, 0:rem_pad] = acc[last, :, 0:rem_pad] + rx[last, :, 0:rem_pad]
        if phase == 0:
            y_copy(n_full, rem_pad).start()

        def body(i, carry):
            k = i - phase * n_full
            e = base + k

            @pl.when(i + DEPTH - 1 < 2 * n_full)
            def _():
                tab_copy(i + DEPTH - 1, 0).start()
                tab_copy(i + DEPTH - 1, 1).start()

            slot = lax.rem(i, DEPTH)
            tab_copy(i, 0).wait()
            tx[e] = partial(tab[slot, 0])
            tab_copy(i, 1).wait()
            acc[e] = partial(tab[slot, 1])
            tx_copy(e).start()

            @pl.when(k > 0)
            def _():
                tx_copy(e - 1).wait_recv()
                acc[e - 1] = acc[e - 1] + rx[e - 1]
                if phase == 0:
                    y_copy(e - 1).start()

            add_picked(tab[slot, 0], row_start(i, 0))
            add_picked(tab[slot, 1], row_start(i, 1))
            return carry

        lax.fori_loop(phase * n_full, (phase + 1) * n_full, body, 0)
        end = last - 1
        tx_copy(end).wait_recv()
        acc[end] = acc[end] + rx[end]
        if phase == 0:
            y_copy(end).start()

    signal_vp(near_sem.at[0])
    run_phase(0)
    pl.semaphore_wait(near_sem.at[0], has_low + has_high)
    signal_vp(near_sem.at[1])
    run_phase(1)
    pl.semaphore_wait(near_sem.at[1], has_low + has_high)
    signal_tp(near_sem.at[2])

    def pick_copy(dz):
        return pltpu.make_async_remote_copy(
            src_ref=picked, dst_ref=picked_rx.at[vp], send_sem=pick_send.at[dz - 1], recv_sem=pick_recv.at[dz - 1],
            device_id=peer_id(dz, 0), device_id_type=MESH,
        )

    for dz in range(1, n_vp):
        pick_copy(dz).start()
    picked_rx[pl.ds(vp, 1)] = picked[...][None]
    for dz in range(1, n_vp):
        pick_copy(dz).wait_recv()
    x2 = picked_rx[0]
    for z in range(1, n_vp):
        x2 = x2 + picked_rx[z]
    stat2_slots[pl.ds(tp, 1)] = stat_row(x2)[None]
    for d in (2, 3, 1):
        stat_copy(stat2_slots, stat2_send, stat2_recv, d).start()
    next_out[...] = norm(
        x2, stat2_slots, stat2_send, stat2_recv, gain2[...].reshape(1, width), bias2[...].reshape(1, width)
    ).astype(jnp.bfloat16)

    def absorb(k, cols):
        e = n_chunks + k
        blocks = cols // LANES
        top = m_run[...]
        for b in range(blocks):
            sl = pl.ds(b * LANES, LANES)
            z = acc[e, :, sl] + y_rx[k, :, sl]
            logits[k, :, sl] = z
            if cols != CHUNK and (b + 1) * LANES > rem:
                z = jnp.where(lane < rem - b * LANES, z, -jnp.inf)
            top = jnp.maximum(top, z)
        total = s_run[...] * jnp.exp(m_run[...] - top)
        for b in range(blocks):
            z = logits[k, :, pl.ds(b * LANES, LANES)]
            if cols != CHUNK and (b + 1) * LANES > rem:
                z = jnp.where(lane < rem - b * LANES, z, -jnp.inf)
            total = total + jnp.exp(z - top)
        m_run[...] = top
        s_run[...] = total

    def absorb_body(k, carry):
        y_copy(k).wait_recv()
        absorb(k, CHUNK)
        return carry

    y_copy(n_full, rem_pad).wait_recv()
    absorb(n_full, rem_pad)
    pl.semaphore_wait(near_sem.at[2], 3)
    lax.fori_loop(0, n_full, absorb_body, 0)

    m_t = m_run[...].T
    top = jnp.max(m_t, axis=0, keepdims=True)
    tot = jnp.sum(s_run[...].T * jnp.exp(m_t - top), axis=0, keepdims=True)
    lse_slots[pl.ds(my_rank, 1), :, 0:rows] = top[None]
    lse_slots[pl.ds(my_rank, 1), :, rows:LANES] = tot[None]

    def lse_copy(dz, dt, j):
        return pltpu.make_async_remote_copy(
            src_ref=lse_slots.at[my_rank], dst_ref=lse_slots.at[my_rank],
            send_sem=lse_send.at[j - 1], recv_sem=lse_recv.at[j - 1],
            device_id=peer_id(dz, dt), device_id_type=MESH,
        )

    for dz, dt, j in peers:
        lse_copy(dz, dt, j).start()

    def drain(e, carry):
        tx_copy(e).wait_send()
        tx_copy(n_chunks + e).wait_send()
        y_copy(e).wait_send()
        return carry

    lax.fori_loop(0, n_full, drain, 0)
    tx_copy(n_full, rem_pad).wait_send()
    tx_copy(n_chunks + n_full, rem_pad).wait_send()
    y_copy(n_full, rem_pad).wait_send()
    for d in (1, 2, 3):
        stat_copy(stat_slots, stat_send, stat_recv, d).wait_send()
        stat_copy(stat2_slots, stat2_send, stat2_recv, d).wait_send()
    for dz in range(1, n_vp):
        pick_copy(dz).wait_send()

    for dz, dt, j in peers:
        lse_copy(dz, dt, j).wait_recv()
    pairs = lse_slots[:, 0, :]
    top = jnp.max(pairs, axis=0, keepdims=True)
    scaled = pltpu.roll(pairs, rows, axis=1) * jnp.exp(pairs - top)
    tot = jnp.sum(scaled, axis=0, keepdims=True)
    lse_out[...] = jnp.broadcast_to(top + jnp.log(tot), (8, LANES))
    for dz, dt, j in peers:
        lse_copy(dz, dt, j).wait_send()


def finish_kernel(n_full, rem, logits, lse, next_rows, out_hbm, sum_hbm, next_hbm, stage, sums, sem, small_sem):
    rows = stage.shape[0]
    next_copy = pltpu.make_async_copy(next_rows, next_hbm, small_sem.at[0])
    next_copy.start()
    sums[...] = lse[0:1, 0:rows]
    sum_copy = pltpu.make_async_copy(sums, sum_hbm, small_sem.at[1])
    sum_copy.start()
    log_sum = lse[...].T[:rows, 0:1]
    copies = []
    for r in range(rows // 8):
        here = slice(8 * r, 8 * r + 8)
        part = jnp.broadcast_to(log_sum[here], (8, LANES))
        for k in range(n_full + 1):
            cols = CHUNK if k < n_full else rem
            for b in range(0, cols, LANES):
                w = min(LANES, cols - b)
                at = k * CHUNK + b
                stage[here, at:at + w] = logits[k, here, b:b + w] - part[:, :w]
        copy = pltpu.make_async_copy(stage.at[here, :], out_hbm.at[here, :], sem.at[r])
        copy.start()
        copies.append(copy)
    for copy in [next_copy, sum_copy] + copies:
        copy.wait()


def solution(mesh):
    n_vp = mesh.shape["vp"]
    assert mesh.shape["tp"] == 4

    def per_device(hidden, lnf_gain, lnf_bias, emb_table, next_tok, eln_gain, eln_bias):
        rows, width = hidden.shape
        seg = emb_table.shape[0] // 4
        n_full, rem = divmod(seg, CHUNK)
        n_chunks = n_full + 1
        rem_pad = -(-rem // LANES) * LANES
        assert 2 * rows == LANES and n_vp == 4 and rem
        f32, bf16 = jnp.float32, jnp.bfloat16
        dma = pltpu.SemaphoreType.DMA
        hbm = pl.BlockSpec(memory_space=pltpu.HBM)
        vmem = pl.BlockSpec(memory_space=pltpu.VMEM)
        logits, lse, next_rows = pl.pallas_call(
            functools.partial(head_kernel, n_vp, n_full, rem, width),
            out_shape=(
                pltpu.VMEM((n_chunks, rows, CHUNK), f32),
                pltpu.VMEM((8, LANES), f32),
                pltpu.VMEM((rows, width), bf16),
            ),
            in_specs=[hbm] * 7,
            out_specs=(vmem, vmem, vmem),
            scratch_shapes=[
                pltpu.VMEM((rows, width), bf16),
                *[pltpu.VMEM((width,), f32)] * 4,
                pltpu.VMEM((1, rows), jnp.int32),
                pltpu.VMEM((DEPTH, 2, CHUNK, width), bf16),
                pltpu.VMEM((4, rem_pad, width), bf16),
                pltpu.VMEM((rows, width), bf16),
                pltpu.VMEM((rows, width), f32),
                pltpu.VMEM((n_vp, rows, width), f32),
                pltpu.VMEM((2 * n_chunks, rows, CHUNK), f32),
                pltpu.VMEM((2 * n_chunks, rows, CHUNK), f32),
                pltpu.VMEM((2 * n_chunks, rows, CHUNK), f32),
                pltpu.VMEM((n_chunks, rows, CHUNK), f32),
                pltpu.VMEM((rows, LANES), f32),
                pltpu.VMEM((rows, LANES), f32),
                pltpu.VMEM((4, 1, LANES), f32),
                pltpu.VMEM((4, 1, LANES), f32),
                pltpu.VMEM((n_vp * 4, 1, LANES), f32),
                dma((6,)), dma((DEPTH, 2)), dma((4,)),
                dma((3,)), dma((3,)), dma((3,)), dma((3,)),
                dma((2 * n_chunks,)), dma((2 * n_chunks,)),
                dma((n_chunks,)), dma((n_chunks,)),
                dma((n_vp - 1,)), dma((n_vp - 1,)),
                dma((n_vp * 4 - 1,)), dma((n_vp * 4 - 1,)),
                pltpu.SemaphoreType.REGULAR((3,)),
            ],
            compiler_params=pltpu.CompilerParams(
                collective_id=0, has_side_effects=True, vmem_limit_bytes=52 * 1024 * 1024
            ),
            name="head",
        )(
            *[
                pltpu.with_memory_space_constraint(a, pltpu.HBM)
                for a in (hidden, lnf_gain, lnf_bias, emb_table, next_tok.reshape(1, rows), eln_gain, eln_bias)
            ]
        )
        logprobs, log_sum, next_in = pl.pallas_call(
            functools.partial(finish_kernel, n_full, rem),
            out_shape=(
                jax.ShapeDtypeStruct((rows, seg), f32),
                jax.ShapeDtypeStruct((1, rows), f32),
                jax.ShapeDtypeStruct((rows, width), bf16),
            ),
            in_specs=[vmem, vmem, vmem],
            out_specs=(hbm, hbm, hbm),
            scratch_shapes=[pltpu.VMEM((rows, seg), f32), pltpu.VMEM((1, rows), f32), dma((rows // 8,)), dma((2,))],
            compiler_params=pltpu.CompilerParams(vmem_limit_bytes=24 * 1024 * 1024),
            name="finish",
        )(logits, lse, next_rows)
        return logprobs, log_sum.reshape(rows), next_in

    return jax.shard_map(
        per_device,
        mesh=mesh,
        in_specs=(P("dp", "tp"), P("tp"), P("tp"), P("vp", "tp"), P("dp"), P("tp"), P("tp")),
        out_specs=(P("dp", ("vp", "tp")), P("dp"), P("dp", "tp")),
        check_vma=False,
    )
```

```python
import functools

import jax
import jax.numpy as jnp
from jax import lax
from jax.experimental import pallas as pl
from jax.experimental.pallas import tpu as pltpu
from jax.sharding import PartitionSpec as P

NORM_EPS = 1e-5
CHUNK = 768
LANES = 128
DEPTH = 3
LOWEST = -3.0e38
MESH = pl.DeviceIdType.MESH


def head_kernel(
    n_vp, n_full, rem, width,
    hid_hbm, gain1_hbm, bias1_hbm, tab_hbm, tok_hbm, gain2_hbm, bias2_hbm,
    logits, lse_out, next_out,
    hid, gain1, bias1, gain2, bias2, tok, tab, tab_rem, normed, picked, picked_rx,
    tx, rx, acc, y_rx, m_run, s_run, stat_slots, stat2_slots, lse_slots,
    in_sem, tab_sem, rem_sem, stat_send, stat_recv, stat2_send, stat2_recv,
    tx_send, tx_recv, y_send, y_recv, pick_send, pick_recv, lse_send, lse_recv, near_sem, y_tail, y_tail_rx,
):
    rows = hid.shape[0]
    n_chunks = n_full + 1
    seg = n_full * CHUNK + rem
    rem_pad = tab_rem.shape[1]
    vp = lax.axis_index("vp")
    tp = lax.axis_index("tp")
    chip_y = tp // 2
    core = lax.rem(tp, 2)
    sibling = tp + 1 - 2 * core
    across = lax.rem(tp + 2, 4)
    my_rank = vp * 4 + tp

    peers = []
    for dz in reversed(range(n_vp)):
        for dt in reversed(range(4)):
            if dz or dt:
                peers.append((dz, dt, dz * 4 + dt))

    def peer_id(dz, dt):
        return {"vp": lax.rem(vp + dz, n_vp), "tp": lax.rem(tp + dt, 4)}

    hid_copy = pltpu.make_async_copy(hid_hbm, hid, in_sem.at[0])
    hid_copy.start()

    has_low = jnp.where(vp > 0, 1, 0)
    has_high = jnp.where(vp < n_vp - 1, 1, 0)

    def signal_vp(sem):
        @pl.when(vp > 0)
        def _():
            pl.semaphore_signal(sem, inc=1, device_id={"vp": vp - 1}, device_id_type=MESH)

        @pl.when(vp < n_vp - 1)
        def _():
            pl.semaphore_signal(sem, inc=1, device_id={"vp": vp + 1}, device_id_type=MESH)

    def signal_tp(sem):
        for dt in (2, 3, 1):
            pl.semaphore_signal(sem, inc=1, device_id=peer_id(0, dt), device_id_type=MESH)

    barrier = pltpu.get_barrier_semaphore()
    signal_tp(barrier)
    signal_vp(barrier)

    def seg_start(phase, which):
        y = chip_y + (1 - phase) * (1 - 2 * chip_y)
        c = core + (1 - which) * (1 - 2 * core)
        return (y * 2 + c) * seg

    def row_start(i, which):
        phase = jnp.where(i >= n_full, 1, 0)
        k = i - phase * n_full
        return pl.multiple_of(seg_start(phase, which) + k * CHUNK, 64)

    def tab_copy(i, which):
        slot = lax.rem(i, DEPTH)
        return pltpu.make_async_copy(
            tab_hbm.at[pl.ds(row_start(i, which), CHUNK), :], tab.at[slot, which], tab_sem.at[slot, which]
        )

    def rem_start(phase, which):
        return pl.multiple_of(seg_start(phase, which) + n_full * CHUNK, 64)

    def rem_copy(phase, which):
        return pltpu.make_async_copy(
            tab_hbm.at[pl.ds(rem_start(phase, which), rem), :],
            tab_rem.at[phase * 2 + which, pl.ds(0, rem), :],
            rem_sem.at[phase * 2 + which],
        )

    small = [
        pltpu.make_async_copy(gain1_hbm, gain1, in_sem.at[1]),
        pltpu.make_async_copy(bias1_hbm, bias1, in_sem.at[2]),
        pltpu.make_async_copy(gain2_hbm, gain2, in_sem.at[3]),
        pltpu.make_async_copy(bias2_hbm, bias2, in_sem.at[4]),
        pltpu.make_async_copy(tok_hbm, tok, in_sem.at[5]),
    ]

    picked[...] = jnp.zeros_like(picked)
    m_run[...] = jnp.full_like(m_run, LOWEST)
    s_run[...] = jnp.zeros_like(s_run)
    tab_rem[:, rem:, :] = jnp.zeros((4, rem_pad - rem, width), jnp.bfloat16)

    lane = lax.broadcasted_iota(jnp.int32, (rows, LANES), 1)

    def stat_row(x):
        s1 = jnp.sum(x, axis=1, keepdims=True)
        s2 = jnp.sum(x * x, axis=1, keepdims=True)
        return jnp.broadcast_to(jnp.concatenate([s1, s2], axis=0), (LANES, LANES)).T[0:1, :]

    def stat_copy(slots, send, recv, d):
        return pltpu.make_async_remote_copy(
            src_ref=slots.at[tp], dst_ref=slots.at[tp], send_sem=send.at[d - 1], recv_sem=recv.at[d - 1],
            device_id=peer_id(0, d), device_id_type=MESH,
        )

    def norm(x, slots, send, recv, gain, bias):
        for d in (1, 2, 3):
            stat_copy(slots, send, recv, d).wait_recv()
        total = (slots[0] + slots[1]) + (slots[2] + slots[3])
        full_width = 4.0 * width
        total = jnp.broadcast_to(total, (8, LANES)) / full_width
        mean = total
        var = pltpu.roll(total, rows, axis=1) - mean * mean
        inv = lax.rsqrt(var + NORM_EPS)
        row = lax.broadcasted_iota(jnp.int32, (8, LANES), 0)
        back = jnp.where(row == 0, mean, inv).T
        mean_c = back[:rows, 0:1]
        inv_c = back[:rows, 1:2]
        return (x - mean_c) * inv_c * gain + bias

    hid_copy.wait()
    x1 = hid[...].astype(jnp.float32)
    stat_slots[pl.ds(tp, 1)] = stat_row(x1)[None]
    pl.semaphore_wait(barrier, 3 + has_low + has_high)
    for d in (2, 3, 1):
        stat_copy(stat_slots, stat_send, stat_recv, d).start()
    for copy in small:
        copy.start()
    for which in range(2):
        rem_copy(0, which).start()
    for i in range(min(DEPTH - 1, 2 * n_full)):
        for which in range(2):
            tab_copy(i, which).start()
    for which in range(2):
        rem_copy(1, which).start()
    for copy in small:
        copy.wait()
    normed[...] = norm(
        x1, stat_slots, stat_send, stat_recv, gain1[...].reshape(1, width), bias1[...].reshape(1, width)
    ).astype(jnp.bfloat16)

    def tx_copy(e, cols=None):
        view = (lambda r: r.at[e]) if cols is None else (lambda r: r.at[e, :, pl.ds(0, cols)])
        return pltpu.make_async_remote_copy(
            src_ref=view(tx), dst_ref=view(rx), send_sem=tx_send.at[e], recv_sem=tx_recv.at[e],
            device_id={"tp": sibling}, device_id_type=MESH,
        )

    def y_copy(e):
        return pltpu.make_async_remote_copy(
            src_ref=acc.at[e], dst_ref=y_rx.at[e], send_sem=y_send.at[e], recv_sem=y_recv.at[e],
            device_id={"tp": across}, device_id_type=MESH,
        )

    half = LANES // 2
    whole = rem - half

    def y_tail_copy():
        return pltpu.make_async_remote_copy(
            src_ref=y_tail, dst_ref=y_tail_rx, send_sem=y_send.at[n_full], recv_sem=y_recv.at[n_full],
            device_id={"tp": across}, device_id_type=MESH,
        )

    def pack_tail(block):
        y_tail[0:rows, :] = block[:, 0:whole]
        low = block[0:rows // 2, whole:whole + LANES]
        high = pltpu.roll(block[rows // 2:rows, whole:whole + LANES], half, axis=1)
        both = jnp.where(lane[0:rows // 2] < half, low, high)
        y_tail[rows:rows + rows // 4, 0:LANES] = both[0:rows // 4]
        y_tail[rows:rows + rows // 4, LANES:2 * LANES] = both[rows // 4:rows // 2]

    def tail_block(b):
        if (b + 1) * LANES <= whole:
            return y_tail_rx[0:rows, b * LANES:(b + 1) * LANES]
        both = jnp.concatenate(
            [y_tail_rx[rows:rows + rows // 4, 0:LANES], y_tail_rx[rows:rows + rows // 4, LANES:2 * LANES]], axis=0
        )
        return jnp.concatenate([both, pltpu.roll(both, half, axis=1)], axis=0)

    def partial(block):
        return lax.dot_general(
            normed[...], block, (((1,), (1,)), ((), ())), preferred_element_type=jnp.float32
        )

    tok_col = jnp.broadcast_to(tok[...], (8, rows)).T[:, 0:1]
    tok_local = tok_col - vp * (4 * seg)

    def add_picked(block, start):
        n = block.shape[0]
        at = lax.broadcasted_iota(jnp.int32, (rows, n), 1)
        hot = jnp.where(at == tok_local - start, 1.0, 0.0).astype(jnp.bfloat16)
        picked[...] += lax.dot_general(
            hot, block, (((1,), (0,)), ((), ())), preferred_element_type=jnp.float32
        )

    def add_picked_rem(phase, which):
        at = lax.broadcasted_iota(jnp.int32, (rows, rem_pad), 1)
        hit = (at == tok_local - rem_start(phase, which)) & (at < rem)
        hot = jnp.where(hit, 1.0, 0.0).astype(jnp.bfloat16)
        picked[...] += lax.dot_general(
            hot, tab_rem[phase * 2 + which], (((1,), (0,)), ((), ())), preferred_element_type=jnp.float32
        )

    def run_phase(phase):
        base = phase * n_chunks

        last = base + n_full
        first = phase * n_full
        slot0 = first % DEPTH
        rem_copy(phase, 0).wait()
        tx[last, :, 0:rem_pad] = partial(tab_rem[phase * 2])
        tx_copy(last, rem_pad).start()
        tab_copy(first, 0).wait()
        tx[base] = partial(tab[slot0, 0])
        tx_copy(base).start()
        rem_copy(phase, 1).wait()
        mine = partial(tab_rem[phase * 2 + 1])
        acc[last, :, 0:rem_pad] = mine
        tab_copy(first, 1).wait()
        acc[base] = partial(tab[slot0, 1])
        tx_copy(last, rem_pad).wait_recv()
        if phase == 0:
            pack_tail(acc[last, :, 0:rem_pad] + rx[last, :, 0:rem_pad])
            y_tail_copy().start()
        else:
            acc[last, :, 0:rem_pad] = acc[last, :, 0:rem_pad] + rx[last, :, 0:rem_pad]

        def finish(e):
            tx_copy(e).wait_recv()
            acc[e] = acc[e] + rx[e]
            if phase == 0:
                y_copy(e).start()

        tab_copy(first + DEPTH - 1, 0).start()
        tab_copy(first + DEPTH - 1, 1).start()
        add_picked_rem(phase, 0)
        add_picked_rem(phase, 1)
        finish(base)
        add_picked(tab[slot0, 0], row_start(first, 0))
        add_picked(tab[slot0, 1], row_start(first, 1))

        def body(i, carry):
            k = i - phase * n_full
            e = base + k

            @pl.when(i + DEPTH - 1 < 2 * n_full)
            def _():
                tab_copy(i + DEPTH - 1, 0).start()
                tab_copy(i + DEPTH - 1, 1).start()

            slot = lax.rem(i, DEPTH)
            tab_copy(i, 0).wait()
            tx[e] = partial(tab[slot, 0])
            tx_copy(e).start()
            tab_copy(i, 1).wait()
            acc[e] = partial(tab[slot, 1])

            @pl.when(k > 1)
            def _():
                finish(e - 1)

            add_picked(tab[slot, 0], row_start(i, 0))
            add_picked(tab[slot, 1], row_start(i, 1))
            return carry

        lax.fori_loop(first + 1, first + n_full, body, 0)
        finish(last - 1)

    signal_vp(near_sem.at[0])
    run_phase(0)
    pl.semaphore_wait(near_sem.at[0], has_low + has_high)
    signal_vp(near_sem.at[1])
    run_phase(1)
    pl.semaphore_wait(near_sem.at[1], has_low + has_high)
    signal_tp(near_sem.at[2])

    def pick_copy(dz):
        return pltpu.make_async_remote_copy(
            src_ref=picked, dst_ref=picked_rx.at[vp], send_sem=pick_send.at[dz - 1], recv_sem=pick_recv.at[dz - 1],
            device_id=peer_id(dz, 0), device_id_type=MESH,
        )

    for dz in range(1, n_vp):
        pick_copy(dz).start()
    picked_rx[pl.ds(vp, 1)] = picked[...][None]
    for dz in range(1, n_vp):
        pick_copy(dz).wait_recv()
    x2 = picked_rx[0]
    for z in range(1, n_vp):
        x2 = x2 + picked_rx[z]
    stat2_slots[pl.ds(tp, 1)] = stat_row(x2)[None]
    for d in (2, 3, 1):
        stat_copy(stat2_slots, stat2_send, stat2_recv, d).start()
    next_out[...] = norm(
        x2, stat2_slots, stat2_send, stat2_recv, gain2[...].reshape(1, width), bias2[...].reshape(1, width)
    ).astype(jnp.bfloat16)

    def absorb(k, cols):
        e = n_chunks + k
        blocks = cols // LANES
        top = m_run[...]
        for b in range(blocks):
            sl = pl.ds(b * LANES, LANES)
            z = acc[e, :, sl] + (y_rx[k, :, sl] if cols == CHUNK else tail_block(b))
            logits[k, :, sl] = z
            if cols != CHUNK and (b + 1) * LANES > rem:
                z = jnp.where(lane < rem - b * LANES, z, -jnp.inf)
            top = jnp.maximum(top, z)
        total = s_run[...] * jnp.exp(m_run[...] - top)
        for b in range(blocks):
            z = logits[k, :, pl.ds(b * LANES, LANES)]
            if cols != CHUNK and (b + 1) * LANES > rem:
                z = jnp.where(lane < rem - b * LANES, z, -jnp.inf)
            total = total + jnp.exp(z - top)
        m_run[...] = top
        s_run[...] = total

    def absorb_body(k, carry):
        y_copy(k).wait_recv()
        absorb(k, CHUNK)
        return carry

    y_tail_copy().wait_recv()
    absorb(n_full, rem_pad)
    pl.semaphore_wait(near_sem.at[2], 3)
    lax.fori_loop(0, n_full, absorb_body, 0)

    m_t = m_run[...].T
    top = jnp.max(m_t, axis=0, keepdims=True)
    tot = jnp.sum(s_run[...].T * jnp.exp(m_t - top), axis=0, keepdims=True)
    lse_slots[pl.ds(my_rank, 1), :, 0:rows] = top[None]
    lse_slots[pl.ds(my_rank, 1), :, rows:LANES] = tot[None]

    def lse_copy(dz, dt, j):
        return pltpu.make_async_remote_copy(
            src_ref=lse_slots.at[my_rank], dst_ref=lse_slots.at[my_rank],
            send_sem=lse_send.at[j - 1], recv_sem=lse_recv.at[j - 1],
            device_id=peer_id(dz, dt), device_id_type=MESH,
        )

    for dz, dt, j in peers:
        lse_copy(dz, dt, j).start()

    def drain(e, carry):
        tx_copy(e).wait_send()
        tx_copy(n_chunks + e).wait_send()
        y_copy(e).wait_send()
        return carry

    lax.fori_loop(0, n_full, drain, 0)
    tx_copy(n_full, rem_pad).wait_send()
    tx_copy(n_chunks + n_full, rem_pad).wait_send()
    y_tail_copy().wait_send()
    for d in (1, 2, 3):
        stat_copy(stat_slots, stat_send, stat_recv, d).wait_send()
        stat_copy(stat2_slots, stat2_send, stat2_recv, d).wait_send()
    for dz in range(1, n_vp):
        pick_copy(dz).wait_send()

    for dz, dt, j in peers:
        lse_copy(dz, dt, j).wait_recv()
    pairs = lse_slots[:, 0, :]
    top = jnp.max(pairs, axis=0, keepdims=True)
    scaled = pltpu.roll(pairs, rows, axis=1) * jnp.exp(pairs - top)
    tot = jnp.sum(scaled, axis=0, keepdims=True)
    lse_out[...] = jnp.broadcast_to(top + jnp.log(tot), (8, LANES))
    for dz, dt, j in peers:
        lse_copy(dz, dt, j).wait_send()


def finish_kernel(n_full, rem, logits, lse, next_rows, out_hbm, sum_hbm, next_hbm, stage, sums, sem, small_sem):
    rows = stage.shape[0]
    next_copy = pltpu.make_async_copy(next_rows, next_hbm, small_sem.at[0])
    next_copy.start()
    sums[...] = lse[0:1, 0:rows]
    sum_copy = pltpu.make_async_copy(sums, sum_hbm, small_sem.at[1])
    sum_copy.start()
    log_sum = lse[...].T[:rows, 0:1]
    copies = []
    for r in range(rows // 8):
        here = slice(8 * r, 8 * r + 8)
        part = jnp.broadcast_to(log_sum[here], (8, LANES))
        for k in range(n_full + 1):
            cols = CHUNK if k < n_full else rem
            for b in range(0, cols, LANES):
                w = min(LANES, cols - b)
                at = k * CHUNK + b
                stage[here, at:at + w] = logits[k, here, b:b + w] - part[:, :w]
        copy = pltpu.make_async_copy(stage.at[here, :], out_hbm.at[here, :], sem.at[r])
        copy.start()
        copies.append(copy)
    for copy in [next_copy, sum_copy] + copies:
        copy.wait()


def solution(mesh):
    n_vp = mesh.shape["vp"]
    assert mesh.shape["tp"] == 4

    def per_device(hidden, lnf_gain, lnf_bias, emb_table, next_tok, eln_gain, eln_bias):
        rows, width = hidden.shape
        seg = emb_table.shape[0] // 4
        n_full, rem = divmod(seg, CHUNK)
        n_chunks = n_full + 1
        rem_pad = -(-rem // LANES) * LANES
        assert 2 * rows == LANES and n_vp == 4 and rem == 2 * LANES + LANES // 2 and n_full > DEPTH
        f32, bf16 = jnp.float32, jnp.bfloat16
        dma = pltpu.SemaphoreType.DMA
        hbm = pl.BlockSpec(memory_space=pltpu.HBM)
        vmem = pl.BlockSpec(memory_space=pltpu.VMEM)
        logits, lse, next_rows = pl.pallas_call(
            functools.partial(head_kernel, n_vp, n_full, rem, width),
            out_shape=(
                pltpu.VMEM((n_chunks, rows, CHUNK), f32),
                pltpu.VMEM((8, LANES), f32),
                pltpu.VMEM((rows, width), bf16),
            ),
            in_specs=[hbm] * 7,
            out_specs=(vmem, vmem, vmem),
            scratch_shapes=[
                pltpu.VMEM((rows, width), bf16),
                *[pltpu.VMEM((width,), f32)] * 4,
                pltpu.VMEM((1, rows), jnp.int32),
                pltpu.VMEM((DEPTH, 2, CHUNK, width), bf16),
                pltpu.VMEM((4, rem_pad, width), bf16),
                pltpu.VMEM((rows, width), bf16),
                pltpu.VMEM((rows, width), f32),
                pltpu.VMEM((n_vp, rows, width), f32),
                pltpu.VMEM((2 * n_chunks, rows, CHUNK), f32),
                pltpu.VMEM((2 * n_chunks, rows, CHUNK), f32),
                pltpu.VMEM((2 * n_chunks, rows, CHUNK), f32),
                pltpu.VMEM((n_chunks, rows, CHUNK), f32),
                pltpu.VMEM((rows, LANES), f32),
                pltpu.VMEM((rows, LANES), f32),
                pltpu.VMEM((4, 1, LANES), f32),
                pltpu.VMEM((4, 1, LANES), f32),
                pltpu.VMEM((n_vp * 4, 1, LANES), f32),
                dma((6,)), dma((DEPTH, 2)), dma((4,)),
                dma((3,)), dma((3,)), dma((3,)), dma((3,)),
                dma((2 * n_chunks,)), dma((2 * n_chunks,)),
                dma((n_chunks,)), dma((n_chunks,)),
                dma((n_vp - 1,)), dma((n_vp - 1,)),
                dma((n_vp * 4 - 1,)), dma((n_vp * 4 - 1,)),
                pltpu.SemaphoreType.REGULAR((3,)),
                pltpu.VMEM((rows + rows // 4, 2 * LANES), f32), pltpu.VMEM((rows + rows // 4, 2 * LANES), f32),
            ],
            compiler_params=pltpu.CompilerParams(
                collective_id=0, has_side_effects=True, vmem_limit_bytes=52 * 1024 * 1024
            ),
            name="head",
        )(
            *[
                pltpu.with_memory_space_constraint(a, pltpu.HBM)
                for a in (hidden, lnf_gain, lnf_bias, emb_table, next_tok.reshape(1, rows), eln_gain, eln_bias)
            ]
        )
        logprobs, log_sum, next_in = pl.pallas_call(
            functools.partial(finish_kernel, n_full, rem),
            out_shape=(
                jax.ShapeDtypeStruct((rows, seg), f32),
                jax.ShapeDtypeStruct((1, rows), f32),
                jax.ShapeDtypeStruct((rows, width), bf16),
            ),
            in_specs=[vmem, vmem, vmem],
            out_specs=(hbm, hbm, hbm),
            scratch_shapes=[pltpu.VMEM((rows, seg), f32), pltpu.VMEM((1, rows), f32), dma((rows // 8,)), dma((2,))],
            compiler_params=pltpu.CompilerParams(vmem_limit_bytes=24 * 1024 * 1024),
            name="finish",
        )(logits, lse, next_rows)
        return logprobs, log_sum.reshape(rows), next_in

    return jax.shard_map(
        per_device,
        mesh=mesh,
        in_specs=(P("dp", "tp"), P("tp"), P("tp"), P("vp", "tp"), P("dp"), P("tp"), P("tp")),
        out_specs=(P("dp", ("vp", "tp")), P("dp"), P("dp", "tp")),
        check_vma=False,
    )
```

```python
import functools

import jax
import jax.numpy as jnp
from jax import lax
from jax.experimental import pallas as pl
from jax.experimental.pallas import tpu as pltpu
from jax.sharding import PartitionSpec as P

NORM_EPS = 1e-5
CHUNK = 512
LANES = 128
DEPTH = 3
LOWEST = -3.0e38
MESH = pl.DeviceIdType.MESH


def head_kernel(
    n_vp, n_full, rem, width,
    hid_hbm, gain1_hbm, bias1_hbm, tab_hbm, tok_hbm, gain2_hbm, bias2_hbm,
    logits, lse_out, next_out,
    hid, gain1, bias1, gain2, bias2, tok, tab, tab_rem, normed, picked, picked_rx,
    tx, rx, acc, y_rx, m_run, s_run, stat_slots, stat2_slots, lse_slots,
    in_sem, tab_sem, rem_sem, stat_send, stat_recv, stat2_send, stat2_recv,
    tx_send, tx_recv, y_send, y_recv, pick_send, pick_recv, lse_send, lse_recv, near_sem, y_tail, y_tail_rx,
):
    rows = hid.shape[0]
    n_chunks = n_full + 1
    seg = n_full * CHUNK + rem
    rem_pad = tab_rem.shape[1]
    vp = lax.axis_index("vp")
    tp = lax.axis_index("tp")
    chip_y = tp // 2
    core = lax.rem(tp, 2)
    sibling = tp + 1 - 2 * core
    across = lax.rem(tp + 2, 4)
    my_rank = vp * 4 + tp

    peers = []
    for dz in reversed(range(n_vp)):
        for dt in reversed(range(4)):
            if dz or dt:
                peers.append((dz, dt, dz * 4 + dt))

    def peer_id(dz, dt):
        return {"vp": lax.rem(vp + dz, n_vp), "tp": lax.rem(tp + dt, 4)}

    hid_copy = pltpu.make_async_copy(hid_hbm, hid, in_sem.at[0])
    hid_copy.start()

    has_low = jnp.where(vp > 0, 1, 0)
    has_high = jnp.where(vp < n_vp - 1, 1, 0)

    def signal_vp(sem):
        @pl.when(vp > 0)
        def _():
            pl.semaphore_signal(sem, inc=1, device_id={"vp": vp - 1}, device_id_type=MESH)

        @pl.when(vp < n_vp - 1)
        def _():
            pl.semaphore_signal(sem, inc=1, device_id={"vp": vp + 1}, device_id_type=MESH)

    def signal_tp(sem):
        for dt in (2, 3, 1):
            pl.semaphore_signal(sem, inc=1, device_id=peer_id(0, dt), device_id_type=MESH)

    barrier = pltpu.get_barrier_semaphore()
    signal_tp(barrier)
    signal_vp(barrier)

    def seg_start(phase, which):
        y = chip_y + (1 - phase) * (1 - 2 * chip_y)
        c = core + (1 - which) * (1 - 2 * core)
        return (y * 2 + c) * seg

    def row_start(i, which):
        phase = jnp.where(i >= n_full, 1, 0)
        k = i - phase * n_full
        return pl.multiple_of(seg_start(phase, which) + k * CHUNK, 64)

    def tab_copy(i, which):
        slot = lax.rem(i, DEPTH)
        return pltpu.make_async_copy(
            tab_hbm.at[pl.ds(row_start(i, which), CHUNK), :], tab.at[slot, which], tab_sem.at[slot, which]
        )

    def rem_start(phase, which):
        return pl.multiple_of(seg_start(phase, which) + n_full * CHUNK, 64)

    def rem_copy(phase, which):
        return pltpu.make_async_copy(
            tab_hbm.at[pl.ds(rem_start(phase, which), rem), :],
            tab_rem.at[phase * 2 + which, pl.ds(0, rem), :],
            rem_sem.at[phase * 2 + which],
        )

    small = [
        pltpu.make_async_copy(gain1_hbm, gain1, in_sem.at[1]),
        pltpu.make_async_copy(bias1_hbm, bias1, in_sem.at[2]),
        pltpu.make_async_copy(gain2_hbm, gain2, in_sem.at[3]),
        pltpu.make_async_copy(bias2_hbm, bias2, in_sem.at[4]),
        pltpu.make_async_copy(tok_hbm, tok, in_sem.at[5]),
    ]

    picked[...] = jnp.zeros_like(picked)
    m_run[...] = jnp.full_like(m_run, LOWEST)
    s_run[...] = jnp.zeros_like(s_run)
    tab_rem[:, rem:, :] = jnp.zeros((4, rem_pad - rem, width), jnp.bfloat16)

    lane = lax.broadcasted_iota(jnp.int32, (rows, LANES), 1)

    def stat_row(x):
        s1 = jnp.sum(x, axis=1, keepdims=True)
        s2 = jnp.sum(x * x, axis=1, keepdims=True)
        return jnp.broadcast_to(jnp.concatenate([s1, s2], axis=0), (LANES, LANES)).T[0:1, :]

    def stat_copy(slots, send, recv, d):
        return pltpu.make_async_remote_copy(
            src_ref=slots.at[tp], dst_ref=slots.at[tp], send_sem=send.at[d - 1], recv_sem=recv.at[d - 1],
            device_id=peer_id(0, d), device_id_type=MESH,
        )

    def norm(x, slots, send, recv, gain, bias):
        for d in (1, 2, 3):
            stat_copy(slots, send, recv, d).wait_recv()
        total = (slots[0] + slots[1]) + (slots[2] + slots[3])
        full_width = 4.0 * width
        total = jnp.broadcast_to(total, (8, LANES)) / full_width
        mean = total
        var = pltpu.roll(total, rows, axis=1) - mean * mean
        inv = lax.rsqrt(var + NORM_EPS)
        row = lax.broadcasted_iota(jnp.int32, (8, LANES), 0)
        back = jnp.where(row == 0, mean, inv).T
        mean_c = back[:rows, 0:1]
        inv_c = back[:rows, 1:2]
        return (x - mean_c) * inv_c * gain + bias

    hid_copy.wait()
    x1 = hid[...].astype(jnp.float32)
    stat_slots[pl.ds(tp, 1)] = stat_row(x1)[None]
    pl.semaphore_wait(barrier, 3 + has_low + has_high)
    for d in (2, 3, 1):
        stat_copy(stat_slots, stat_send, stat_recv, d).start()
    for copy in small:
        copy.start()
    for which in range(2):
        rem_copy(0, which).start()
    for i in range(min(DEPTH - 1, 2 * n_full)):
        for which in range(2):
            tab_copy(i, which).start()
    for which in range(2):
        rem_copy(1, which).start()
    for copy in small:
        copy.wait()
    normed[...] = norm(
        x1, stat_slots, stat_send, stat_recv, gain1[...].reshape(1, width), bias1[...].reshape(1, width)
    ).astype(jnp.bfloat16)

    def tx_copy(e, cols=None):
        view = (lambda r: r.at[e]) if cols is None else (lambda r: r.at[e, :, pl.ds(0, cols)])
        return pltpu.make_async_remote_copy(
            src_ref=view(tx), dst_ref=view(rx), send_sem=tx_send.at[e], recv_sem=tx_recv.at[e],
            device_id={"tp": sibling}, device_id_type=MESH,
        )

    def y_copy(e):
        return pltpu.make_async_remote_copy(
            src_ref=acc.at[e], dst_ref=y_rx.at[e], send_sem=y_send.at[e], recv_sem=y_recv.at[e],
            device_id={"tp": across}, device_id_type=MESH,
        )

    half = LANES // 2
    whole = rem - half

    def y_tail_copy():
        return pltpu.make_async_remote_copy(
            src_ref=y_tail, dst_ref=y_tail_rx, send_sem=y_send.at[n_full], recv_sem=y_recv.at[n_full],
            device_id={"tp": across}, device_id_type=MESH,
        )

    def pack_tail(block):
        y_tail[0:rows, :] = block[:, 0:whole]
        low = block[0:rows // 2, whole:whole + LANES]
        high = pltpu.roll(block[rows // 2:rows, whole:whole + LANES], half, axis=1)
        both = jnp.where(lane[0:rows // 2] < half, low, high)
        y_tail[rows:rows + rows // 4, 0:LANES] = both[0:rows // 4]
        y_tail[rows:rows + rows // 4, LANES:2 * LANES] = both[rows // 4:rows // 2]

    def tail_block(b):
        if (b + 1) * LANES <= whole:
            return y_tail_rx[0:rows, b * LANES:(b + 1) * LANES]
        both = jnp.concatenate(
            [y_tail_rx[rows:rows + rows // 4, 0:LANES], y_tail_rx[rows:rows + rows // 4, LANES:2 * LANES]], axis=0
        )
        return jnp.concatenate([both, pltpu.roll(both, half, axis=1)], axis=0)

    def partial(block):
        return lax.dot_general(
            normed[...], block, (((1,), (1,)), ((), ())), preferred_element_type=jnp.float32
        )

    tok_col = jnp.broadcast_to(tok[...], (8, rows)).T[:, 0:1]
    tok_local = tok_col - vp * (4 * seg)

    def add_picked(block, start):
        n = block.shape[0]
        at = lax.broadcasted_iota(jnp.int32, (rows, n), 1)
        hot = jnp.where(at == tok_local - start, 1.0, 0.0).astype(jnp.bfloat16)
        picked[...] += lax.dot_general(
            hot, block, (((1,), (0,)), ((), ())), preferred_element_type=jnp.float32
        )

    def add_picked_rem(phase, which):
        at = lax.broadcasted_iota(jnp.int32, (rows, rem_pad), 1)
        hit = (at == tok_local - rem_start(phase, which)) & (at < rem)
        hot = jnp.where(hit, 1.0, 0.0).astype(jnp.bfloat16)
        picked[...] += lax.dot_general(
            hot, tab_rem[phase * 2 + which], (((1,), (0,)), ((), ())), preferred_element_type=jnp.float32
        )

    def run_phase(phase):
        base = phase * n_chunks

        last = base + n_full
        first = phase * n_full
        slot0 = first % DEPTH
        rem_copy(phase, 0).wait()
        tx[last, :, 0:rem_pad] = partial(tab_rem[phase * 2])
        tx_copy(last, rem_pad).start()
        tab_copy(first, 0).wait()
        tx[base] = partial(tab[slot0, 0])
        tx_copy(base).start()
        rem_copy(phase, 1).wait()
        mine = partial(tab_rem[phase * 2 + 1])
        acc[last, :, 0:rem_pad] = mine
        tab_copy(first, 1).wait()
        acc[base] = partial(tab[slot0, 1])
        tx_copy(last, rem_pad).wait_recv()
        if phase == 0:
            pack_tail(acc[last, :, 0:rem_pad] + rx[last, :, 0:rem_pad])
            y_tail_copy().start()
        else:
            acc[last, :, 0:rem_pad] = acc[last, :, 0:rem_pad] + rx[last, :, 0:rem_pad]

        def finish(e):
            tx_copy(e).wait_recv()
            acc[e] = acc[e] + rx[e]
            if phase == 0:
                y_copy(e).start()

        tab_copy(first + DEPTH - 1, 0).start()
        tab_copy(first + DEPTH - 1, 1).start()
        add_picked_rem(phase, 0)
        add_picked_rem(phase, 1)
        finish(base)
        add_picked(tab[slot0, 0], row_start(first, 0))
        add_picked(tab[slot0, 1], row_start(first, 1))

        def body(i, carry):
            k = i - phase * n_full
            e = base + k

            @pl.when(i + DEPTH - 1 < 2 * n_full)
            def _():
                tab_copy(i + DEPTH - 1, 0).start()
                tab_copy(i + DEPTH - 1, 1).start()

            slot = lax.rem(i, DEPTH)
            tab_copy(i, 0).wait()
            tx[e] = partial(tab[slot, 0])
            tx_copy(e).start()
            tab_copy(i, 1).wait()
            acc[e] = partial(tab[slot, 1])

            @pl.when(k > 1)
            def _():
                finish(e - 1)

            add_picked(tab[slot, 0], row_start(i, 0))
            add_picked(tab[slot, 1], row_start(i, 1))
            return carry

        lax.fori_loop(first + 1, first + n_full, body, 0)
        finish(last - 1)

    signal_vp(near_sem.at[0])
    run_phase(0)
    pl.semaphore_wait(near_sem.at[0], has_low + has_high)
    signal_vp(near_sem.at[1])
    run_phase(1)
    pl.semaphore_wait(near_sem.at[1], has_low + has_high)
    signal_tp(near_sem.at[2])

    def pick_copy(dz):
        return pltpu.make_async_remote_copy(
            src_ref=picked, dst_ref=picked_rx.at[vp], send_sem=pick_send.at[dz - 1], recv_sem=pick_recv.at[dz - 1],
            device_id=peer_id(dz, 0), device_id_type=MESH,
        )

    for dz in range(1, n_vp):
        pick_copy(dz).start()
    picked_rx[pl.ds(vp, 1)] = picked[...][None]
    for dz in range(1, n_vp):
        pick_copy(dz).wait_recv()
    x2 = picked_rx[0]
    for z in range(1, n_vp):
        x2 = x2 + picked_rx[z]
    stat2_slots[pl.ds(tp, 1)] = stat_row(x2)[None]
    for d in (2, 3, 1):
        stat_copy(stat2_slots, stat2_send, stat2_recv, d).start()
    next_out[...] = norm(
        x2, stat2_slots, stat2_send, stat2_recv, gain2[...].reshape(1, width), bias2[...].reshape(1, width)
    ).astype(jnp.bfloat16)

    def absorb(k, cols):
        e = n_chunks + k
        blocks = cols // LANES
        top = m_run[...]
        for b in range(blocks):
            sl = pl.ds(b * LANES, LANES)
            z = acc[e, :, sl] + (y_rx[k, :, sl] if cols == CHUNK else tail_block(b))
            logits[k, :, sl] = z
            if cols != CHUNK and (b + 1) * LANES > rem:
                z = jnp.where(lane < rem - b * LANES, z, -jnp.inf)
            top = jnp.maximum(top, z)
        total = s_run[...] * jnp.exp(m_run[...] - top)
        for b in range(blocks):
            z = logits[k, :, pl.ds(b * LANES, LANES)]
            if cols != CHUNK and (b + 1) * LANES > rem:
                z = jnp.where(lane < rem - b * LANES, z, -jnp.inf)
            total = total + jnp.exp(z - top)
        m_run[...] = top
        s_run[...] = total

    def absorb_body(k, carry):
        y_copy(k).wait_recv()
        absorb(k, CHUNK)
        return carry

    y_tail_copy().wait_recv()
    absorb(n_full, rem_pad)
    pl.semaphore_wait(near_sem.at[2], 3)
    lax.fori_loop(0, n_full, absorb_body, 0)

    m_t = m_run[...].T
    top = jnp.max(m_t, axis=0, keepdims=True)
    tot = jnp.sum(s_run[...].T * jnp.exp(m_t - top), axis=0, keepdims=True)
    lse_slots[pl.ds(my_rank, 1), :, 0:rows] = top[None]
    lse_slots[pl.ds(my_rank, 1), :, rows:LANES] = tot[None]

    def lse_copy(dz, dt, j):
        return pltpu.make_async_remote_copy(
            src_ref=lse_slots.at[my_rank], dst_ref=lse_slots.at[my_rank],
            send_sem=lse_send.at[j - 1], recv_sem=lse_recv.at[j - 1],
            device_id=peer_id(dz, dt), device_id_type=MESH,
        )

    for dz, dt, j in peers:
        lse_copy(dz, dt, j).start()

    def drain(e, carry):
        tx_copy(e).wait_send()
        tx_copy(n_chunks + e).wait_send()
        y_copy(e).wait_send()
        return carry

    lax.fori_loop(0, n_full, drain, 0)
    tx_copy(n_full, rem_pad).wait_send()
    tx_copy(n_chunks + n_full, rem_pad).wait_send()
    y_tail_copy().wait_send()
    for d in (1, 2, 3):
        stat_copy(stat_slots, stat_send, stat_recv, d).wait_send()
        stat_copy(stat2_slots, stat2_send, stat2_recv, d).wait_send()
    for dz in range(1, n_vp):
        pick_copy(dz).wait_send()

    for dz, dt, j in peers:
        lse_copy(dz, dt, j).wait_recv()
    pairs = lse_slots[:, 0, :]
    top = jnp.max(pairs, axis=0, keepdims=True)
    scaled = pltpu.roll(pairs, rows, axis=1) * jnp.exp(pairs - top)
    tot = jnp.sum(scaled, axis=0, keepdims=True)
    lse_out[...] = jnp.broadcast_to(top + jnp.log(tot), (8, LANES))
    for dz, dt, j in peers:
        lse_copy(dz, dt, j).wait_send()


def finish_kernel(n_full, rem, logits, lse, next_rows, out_hbm, sum_hbm, next_hbm, stage, sums, sem, small_sem):
    rows = stage.shape[0]
    next_copy = pltpu.make_async_copy(next_rows, next_hbm, small_sem.at[0])
    next_copy.start()
    sums[...] = lse[0:1, 0:rows]
    sum_copy = pltpu.make_async_copy(sums, sum_hbm, small_sem.at[1])
    sum_copy.start()
    log_sum = lse[...].T[:rows, 0:1]
    copies = []
    for r in range(rows // 8):
        here = slice(8 * r, 8 * r + 8)
        part = jnp.broadcast_to(log_sum[here], (8, LANES))
        for k in range(n_full + 1):
            cols = CHUNK if k < n_full else rem
            for b in range(0, cols, LANES):
                w = min(LANES, cols - b)
                at = k * CHUNK + b
                stage[here, at:at + w] = logits[k, here, b:b + w] - part[:, :w]
        copy = pltpu.make_async_copy(stage.at[here, :], out_hbm.at[here, :], sem.at[r])
        copy.start()
        copies.append(copy)
    for copy in [next_copy, sum_copy] + copies:
        copy.wait()


def solution(mesh):
    n_vp = mesh.shape["vp"]
    assert mesh.shape["tp"] == 4

    def per_device(hidden, lnf_gain, lnf_bias, emb_table, next_tok, eln_gain, eln_bias):
        rows, width = hidden.shape
        seg = emb_table.shape[0] // 4
        n_full, rem = divmod(seg, CHUNK)
        n_chunks = n_full + 1
        rem_pad = -(-rem // LANES) * LANES
        assert 2 * rows == LANES and n_vp == 4 and rem == 2 * LANES + LANES // 2 and n_full > DEPTH
        f32, bf16 = jnp.float32, jnp.bfloat16
        dma = pltpu.SemaphoreType.DMA
        hbm = pl.BlockSpec(memory_space=pltpu.HBM)
        vmem = pl.BlockSpec(memory_space=pltpu.VMEM)
        logits, lse, next_rows = pl.pallas_call(
            functools.partial(head_kernel, n_vp, n_full, rem, width),
            out_shape=(
                pltpu.VMEM((n_chunks, rows, CHUNK), f32),
                pltpu.VMEM((8, LANES), f32),
                pltpu.VMEM((rows, width), bf16),
            ),
            in_specs=[hbm] * 7,
            out_specs=(vmem, vmem, vmem),
            scratch_shapes=[
                pltpu.VMEM((rows, width), bf16),
                *[pltpu.VMEM((width,), f32)] * 4,
                pltpu.VMEM((1, rows), jnp.int32),
                pltpu.VMEM((DEPTH, 2, CHUNK, width), bf16),
                pltpu.VMEM((4, rem_pad, width), bf16),
                pltpu.VMEM((rows, width), bf16),
                pltpu.VMEM((rows, width), f32),
                pltpu.VMEM((n_vp, rows, width), f32),
                pltpu.VMEM((2 * n_chunks, rows, CHUNK), f32),
                pltpu.VMEM((2 * n_chunks, rows, CHUNK), f32),
                pltpu.VMEM((2 * n_chunks, rows, CHUNK), f32),
                pltpu.VMEM((n_chunks, rows, CHUNK), f32),
                pltpu.VMEM((rows, LANES), f32),
                pltpu.VMEM((rows, LANES), f32),
                pltpu.VMEM((4, 1, LANES), f32),
                pltpu.VMEM((4, 1, LANES), f32),
                pltpu.VMEM((n_vp * 4, 1, LANES), f32),
                dma((6,)), dma((DEPTH, 2)), dma((4,)),
                dma((3,)), dma((3,)), dma((3,)), dma((3,)),
                dma((2 * n_chunks,)), dma((2 * n_chunks,)),
                dma((n_chunks,)), dma((n_chunks,)),
                dma((n_vp - 1,)), dma((n_vp - 1,)),
                dma((n_vp * 4 - 1,)), dma((n_vp * 4 - 1,)),
                pltpu.SemaphoreType.REGULAR((3,)),
                pltpu.VMEM((rows + rows // 4, 2 * LANES), f32), pltpu.VMEM((rows + rows // 4, 2 * LANES), f32),
            ],
            compiler_params=pltpu.CompilerParams(
                collective_id=0, has_side_effects=True, vmem_limit_bytes=52 * 1024 * 1024
            ),
            name="head",
        )(
            *[
                pltpu.with_memory_space_constraint(a, pltpu.HBM)
                for a in (hidden, lnf_gain, lnf_bias, emb_table, next_tok.reshape(1, rows), eln_gain, eln_bias)
            ]
        )
        logprobs, log_sum, next_in = pl.pallas_call(
            functools.partial(finish_kernel, n_full, rem),
            out_shape=(
                jax.ShapeDtypeStruct((rows, seg), f32),
                jax.ShapeDtypeStruct((1, rows), f32),
                jax.ShapeDtypeStruct((rows, width), bf16),
            ),
            in_specs=[vmem, vmem, vmem],
            out_specs=(hbm, hbm, hbm),
            scratch_shapes=[pltpu.VMEM((rows, seg), f32), pltpu.VMEM((1, rows), f32), dma((rows // 8,)), dma((2,))],
            compiler_params=pltpu.CompilerParams(vmem_limit_bytes=24 * 1024 * 1024),
            name="finish",
        )(logits, lse, next_rows)
        return logprobs, log_sum.reshape(rows), next_in

    return jax.shard_map(
        per_device,
        mesh=mesh,
        in_specs=(P("dp", "tp"), P("tp"), P("tp"), P("vp", "tp"), P("dp"), P("tp"), P("tp")),
        out_specs=(P("dp", ("vp", "tp")), P("dp"), P("dp", "tp")),
        check_vma=False,
    )
```

```python
import functools

import jax
import jax.numpy as jnp
from jax import lax
from jax.experimental import pallas as pl
from jax.experimental.pallas import tpu as pltpu
from jax.sharding import PartitionSpec as P

NORM_EPS = 1e-5
CHUNK = 768
LANES = 128
DEPTH = 3
LOWEST = -3.0e38
MESH = pl.DeviceIdType.MESH


def head_kernel(
    n_vp, n_full, rem, width,
    hid_hbm, gain1_hbm, bias1_hbm, tab_hbm, tok_hbm, gain2_hbm, bias2_hbm,
    logits, lse_out, next_out,
    hid, gain1, bias1, gain2, bias2, tok, tab, tab_rem, normed, picked, picked_rx,
    tx, rx, acc, y_rx, m_run, s_run, stat_slots, stat2_slots, lse_slots,
    in_sem, tab_sem, rem_sem, stat_send, stat_recv, stat2_send, stat2_recv,
    tx_send, tx_recv, y_send, y_recv, pick_send, pick_recv, lse_send, lse_recv, near_sem, y_tail, y_tail_rx,
):
    rows = hid.shape[0]
    n_chunks = n_full + 1
    seg = n_full * CHUNK + rem
    rem_pad = tab_rem.shape[1]
    vp = lax.axis_index("vp")
    tp = lax.axis_index("tp")
    chip_y = tp // 2
    core = lax.rem(tp, 2)
    sibling = tp + 1 - 2 * core
    across = lax.rem(tp + 2, 4)
    my_rank = vp * 4 + tp

    peers = []
    for dz in reversed(range(n_vp)):
        for dt in reversed(range(4)):
            if dz or dt:
                peers.append((dz, dt, dz * 4 + dt))

    def peer_id(dz, dt):
        return {"vp": lax.rem(vp + dz, n_vp), "tp": lax.rem(tp + dt, 4)}

    hid_copy = pltpu.make_async_copy(hid_hbm, hid, in_sem.at[0])
    hid_copy.start()

    has_low = jnp.where(vp > 0, 1, 0)
    has_high = jnp.where(vp < n_vp - 1, 1, 0)

    def signal_vp(sem):
        @pl.when(vp > 0)
        def _():
            pl.semaphore_signal(sem, inc=1, device_id={"vp": vp - 1}, device_id_type=MESH)

        @pl.when(vp < n_vp - 1)
        def _():
            pl.semaphore_signal(sem, inc=1, device_id={"vp": vp + 1}, device_id_type=MESH)

    def signal_tp(sem):
        for dt in (2, 3, 1):
            pl.semaphore_signal(sem, inc=1, device_id=peer_id(0, dt), device_id_type=MESH)

    barrier = pltpu.get_barrier_semaphore()
    signal_tp(barrier)
    signal_vp(barrier)

    def seg_start(phase, which):
        y = chip_y + (1 - phase) * (1 - 2 * chip_y)
        c = core + (1 - which) * (1 - 2 * core)
        return (y * 2 + c) * seg

    def row_start(i, which):
        phase = jnp.where(i >= n_full, 1, 0)
        k = i - phase * n_full
        return pl.multiple_of(seg_start(phase, which) + k * CHUNK, 64)

    def tab_copy(i, which):
        slot = lax.rem(i, DEPTH)
        return pltpu.make_async_copy(
            tab_hbm.at[pl.ds(row_start(i, which), CHUNK), :], tab.at[slot, which], tab_sem.at[slot, which]
        )

    def rem_start(phase, which):
        return pl.multiple_of(seg_start(phase, which) + n_full * CHUNK, 64)

    def rem_copy(phase, which):
        return pltpu.make_async_copy(
            tab_hbm.at[pl.ds(rem_start(phase, which), rem), :],
            tab_rem.at[phase * 2 + which, pl.ds(0, rem), :],
            rem_sem.at[phase * 2 + which],
        )

    small = [
        pltpu.make_async_copy(gain1_hbm, gain1, in_sem.at[1]),
        pltpu.make_async_copy(bias1_hbm, bias1, in_sem.at[2]),
        pltpu.make_async_copy(gain2_hbm, gain2, in_sem.at[3]),
        pltpu.make_async_copy(bias2_hbm, bias2, in_sem.at[4]),
        pltpu.make_async_copy(tok_hbm, tok, in_sem.at[5]),
    ]

    picked[...] = jnp.zeros_like(picked)
    m_run[...] = jnp.full_like(m_run, LOWEST)
    s_run[...] = jnp.zeros_like(s_run)
    tab_rem[:, rem:, :] = jnp.zeros((4, rem_pad - rem, width), jnp.bfloat16)

    lane = lax.broadcasted_iota(jnp.int32, (rows, LANES), 1)

    def stat_row(x):
        s1 = jnp.sum(x, axis=1, keepdims=True)
        s2 = jnp.sum(x * x, axis=1, keepdims=True)
        return jnp.broadcast_to(jnp.concatenate([s1, s2], axis=0), (LANES, LANES)).T[0:1, :]

    def stat_copy(slots, send, recv, d):
        return pltpu.make_async_remote_copy(
            src_ref=slots.at[tp], dst_ref=slots.at[tp], send_sem=send.at[d - 1], recv_sem=recv.at[d - 1],
            device_id=peer_id(0, d), device_id_type=MESH,
        )

    def norm(x, slots, send, recv, gain, bias):
        for d in (1, 2, 3):
            stat_copy(slots, send, recv, d).wait_recv()
        total = (slots[0] + slots[1]) + (slots[2] + slots[3])
        full_width = 4.0 * width
        total = jnp.broadcast_to(total, (8, LANES)) / full_width
        mean = total
        var = pltpu.roll(total, rows, axis=1) - mean * mean
        inv = lax.rsqrt(var + NORM_EPS)
        row = lax.broadcasted_iota(jnp.int32, (8, LANES), 0)
        back = jnp.where(row == 0, mean, inv).T
        mean_c = back[:rows, 0:1]
        inv_c = back[:rows, 1:2]
        return (x - mean_c) * inv_c * gain + bias

    hid_copy.wait()
    x1 = hid[...].astype(jnp.float32)
    stat_slots[pl.ds(tp, 1)] = stat_row(x1)[None]
    pl.semaphore_wait(barrier, 3 + has_low + has_high)
    for d in (2, 3, 1):
        stat_copy(stat_slots, stat_send, stat_recv, d).start()
    for copy in small:
        copy.start()
    for which in range(2):
        rem_copy(0, which).start()
    for i in range(min(DEPTH - 1, 2 * n_full)):
        for which in range(2):
            tab_copy(i, which).start()
    for which in range(2):
        rem_copy(1, which).start()
    for copy in small:
        copy.wait()
    normed[...] = norm(
        x1, stat_slots, stat_send, stat_recv, gain1[...].reshape(1, width), bias1[...].reshape(1, width)
    ).astype(jnp.bfloat16)

    def tx_copy(e, cols=None):
        view = (lambda r: r.at[e]) if cols is None else (lambda r: r.at[e, :, pl.ds(0, cols)])
        return pltpu.make_async_remote_copy(
            src_ref=view(tx), dst_ref=view(rx), send_sem=tx_send.at[e], recv_sem=tx_recv.at[e],
            device_id={"tp": sibling}, device_id_type=MESH,
        )

    def y_copy(e):
        return pltpu.make_async_remote_copy(
            src_ref=acc.at[e], dst_ref=y_rx.at[e], send_sem=y_send.at[e], recv_sem=y_recv.at[e],
            device_id={"tp": across}, device_id_type=MESH,
        )

    def y_pair(e):
        return pltpu.make_async_remote_copy(
            src_ref=acc.at[pl.ds(e, 2)], dst_ref=y_rx.at[pl.ds(e, 2)],
            send_sem=y_send.at[e + 1], recv_sem=y_recv.at[e + 1],
            device_id={"tp": across}, device_id_type=MESH,
        )

    def opens_pair(k):
        return (lax.rem(k + core, 2) == 0) & (k < n_full - 1)

    def closes_pair(k):
        return (lax.rem(k + core, 2) == 1) & (k > 0)

    def is_single(k):
        return (core == 1) & ((k == 0) | (k == n_full - 1))

    half = LANES // 2
    whole = rem - half

    def y_tail_copy():
        return pltpu.make_async_remote_copy(
            src_ref=y_tail, dst_ref=y_tail_rx, send_sem=y_send.at[n_full], recv_sem=y_recv.at[n_full],
            device_id={"tp": across}, device_id_type=MESH,
        )

    def pack_tail(block):
        y_tail[0:rows, :] = block[:, 0:whole]
        low = block[0:rows // 2, whole:whole + LANES]
        high = pltpu.roll(block[rows // 2:rows, whole:whole + LANES], half, axis=1)
        both = jnp.where(lane[0:rows // 2] < half, low, high)
        y_tail[rows:rows + rows // 4, 0:LANES] = both[0:rows // 4]
        y_tail[rows:rows + rows // 4, LANES:2 * LANES] = both[rows // 4:rows // 2]

    def tail_block(b):
        if (b + 1) * LANES <= whole:
            return y_tail_rx[0:rows, b * LANES:(b + 1) * LANES]
        both = jnp.concatenate(
            [y_tail_rx[rows:rows + rows // 4, 0:LANES], y_tail_rx[rows:rows + rows // 4, LANES:2 * LANES]], axis=0
        )
        return jnp.concatenate([both, pltpu.roll(both, half, axis=1)], axis=0)

    def partial(block):
        return lax.dot_general(
            normed[...], block, (((1,), (1,)), ((), ())), preferred_element_type=jnp.float32
        )

    tok_col = jnp.broadcast_to(tok[...], (8, rows)).T[:, 0:1]
    tok_local = tok_col - vp * (4 * seg)

    def add_picked(block, start):
        n = block.shape[0]
        at = lax.broadcasted_iota(jnp.int32, (rows, n), 1)
        hot = jnp.where(at == tok_local - start, 1.0, 0.0).astype(jnp.bfloat16)
        picked[...] += lax.dot_general(
            hot, block, (((1,), (0,)), ((), ())), preferred_element_type=jnp.float32
        )

    def add_picked_rem(phase, which):
        at = lax.broadcasted_iota(jnp.int32, (rows, rem_pad), 1)
        hit = (at == tok_local - rem_start(phase, which)) & (at < rem)
        hot = jnp.where(hit, 1.0, 0.0).astype(jnp.bfloat16)
        picked[...] += lax.dot_general(
            hot, tab_rem[phase * 2 + which], (((1,), (0,)), ((), ())), preferred_element_type=jnp.float32
        )

    def run_phase(phase):
        base = phase * n_chunks

        last = base + n_full
        first = phase * n_full
        slot0 = first % DEPTH
        rem_copy(phase, 0).wait()
        tx[last, :, 0:rem_pad] = partial(tab_rem[phase * 2])
        tx_copy(last, rem_pad).start()
        tab_copy(first, 0).wait()
        tx[base] = partial(tab[slot0, 0])
        tx_copy(base).start()
        rem_copy(phase, 1).wait()
        mine = partial(tab_rem[phase * 2 + 1])
        acc[last, :, 0:rem_pad] = mine
        tab_copy(first, 1).wait()
        acc[base] = partial(tab[slot0, 1])
        tx_copy(last, rem_pad).wait_recv()
        if phase == 0:
            pack_tail(acc[last, :, 0:rem_pad] + rx[last, :, 0:rem_pad])
            y_tail_copy().start()
        else:
            acc[last, :, 0:rem_pad] = acc[last, :, 0:rem_pad] + rx[last, :, 0:rem_pad]

        def finish(e):
            tx_copy(e).wait_recv()
            acc[e] = acc[e] + rx[e]
            if phase == 0:
                @pl.when(closes_pair(e))
                def _():
                    y_pair(e - 1).start()

                @pl.when(is_single(e))
                def _():
                    y_copy(e).start()

        tab_copy(first + DEPTH - 1, 0).start()
        tab_copy(first + DEPTH - 1, 1).start()
        add_picked_rem(phase, 0)
        add_picked_rem(phase, 1)
        finish(base)
        add_picked(tab[slot0, 0], row_start(first, 0))
        add_picked(tab[slot0, 1], row_start(first, 1))

        def body(i, carry):
            k = i - phase * n_full
            e = base + k

            @pl.when(i + DEPTH - 1 < 2 * n_full)
            def _():
                tab_copy(i + DEPTH - 1, 0).start()
                tab_copy(i + DEPTH - 1, 1).start()

            slot = lax.rem(i, DEPTH)
            tab_copy(i, 0).wait()
            tx[e] = partial(tab[slot, 0])
            tx_copy(e).start()
            tab_copy(i, 1).wait()
            acc[e] = partial(tab[slot, 1])

            @pl.when(k > 1)
            def _():
                finish(e - 1)

            add_picked(tab[slot, 0], row_start(i, 0))
            add_picked(tab[slot, 1], row_start(i, 1))
            return carry

        lax.fori_loop(first + 1, first + n_full, body, 0)
        finish(last - 1)

    signal_vp(near_sem.at[0])
    run_phase(0)
    pl.semaphore_wait(near_sem.at[0], has_low + has_high)
    signal_vp(near_sem.at[1])
    run_phase(1)
    pl.semaphore_wait(near_sem.at[1], has_low + has_high)
    signal_tp(near_sem.at[2])

    def pick_copy(dz):
        return pltpu.make_async_remote_copy(
            src_ref=picked, dst_ref=picked_rx.at[vp], send_sem=pick_send.at[dz - 1], recv_sem=pick_recv.at[dz - 1],
            device_id=peer_id(dz, 0), device_id_type=MESH,
        )

    for dz in range(1, n_vp):
        pick_copy(dz).start()
    picked_rx[pl.ds(vp, 1)] = picked[...][None]
    for dz in range(1, n_vp):
        pick_copy(dz).wait_recv()
    x2 = picked_rx[0]
    for z in range(1, n_vp):
        x2 = x2 + picked_rx[z]
    stat2_slots[pl.ds(tp, 1)] = stat_row(x2)[None]
    for d in (2, 3, 1):
        stat_copy(stat2_slots, stat2_send, stat2_recv, d).start()
    next_out[...] = norm(
        x2, stat2_slots, stat2_send, stat2_recv, gain2[...].reshape(1, width), bias2[...].reshape(1, width)
    ).astype(jnp.bfloat16)

    def absorb(k, cols):
        e = n_chunks + k
        blocks = cols // LANES
        top = m_run[...]
        for b in range(blocks):
            sl = pl.ds(b * LANES, LANES)
            z = acc[e, :, sl] + (y_rx[k, :, sl] if cols == CHUNK else tail_block(b))
            logits[k, :, sl] = z
            if cols != CHUNK and (b + 1) * LANES > rem:
                z = jnp.where(lane < rem - b * LANES, z, -jnp.inf)
            top = jnp.maximum(top, z)
        total = s_run[...] * jnp.exp(m_run[...] - top)
        for b in range(blocks):
            z = logits[k, :, pl.ds(b * LANES, LANES)]
            if cols != CHUNK and (b + 1) * LANES > rem:
                z = jnp.where(lane < rem - b * LANES, z, -jnp.inf)
            total = total + jnp.exp(z - top)
        m_run[...] = top
        s_run[...] = total

    def absorb_body(k, carry):
        @pl.when(opens_pair(k))
        def _():
            y_pair(k).wait_recv()

        @pl.when(is_single(k))
        def _():
            y_copy(k).wait_recv()

        absorb(k, CHUNK)
        return carry

    y_tail_copy().wait_recv()
    absorb(n_full, rem_pad)
    pl.semaphore_wait(near_sem.at[2], 3)
    lax.fori_loop(0, n_full, absorb_body, 0)

    m_t = m_run[...].T
    top = jnp.max(m_t, axis=0, keepdims=True)
    tot = jnp.sum(s_run[...].T * jnp.exp(m_t - top), axis=0, keepdims=True)
    lse_slots[pl.ds(my_rank, 1), :, 0:rows] = top[None]
    lse_slots[pl.ds(my_rank, 1), :, rows:LANES] = tot[None]

    def lse_copy(dz, dt, j):
        return pltpu.make_async_remote_copy(
            src_ref=lse_slots.at[my_rank], dst_ref=lse_slots.at[my_rank],
            send_sem=lse_send.at[j - 1], recv_sem=lse_recv.at[j - 1],
            device_id=peer_id(dz, dt), device_id_type=MESH,
        )

    for dz, dt, j in peers:
        lse_copy(dz, dt, j).start()

    def drain(e, carry):
        tx_copy(e).wait_send()
        tx_copy(n_chunks + e).wait_send()

        @pl.when(opens_pair(e))
        def _():
            y_pair(e).wait_send()

        @pl.when(is_single(e))
        def _():
            y_copy(e).wait_send()

        return carry

    lax.fori_loop(0, n_full, drain, 0)
    tx_copy(n_full, rem_pad).wait_send()
    tx_copy(n_chunks + n_full, rem_pad).wait_send()
    y_tail_copy().wait_send()
    for d in (1, 2, 3):
        stat_copy(stat_slots, stat_send, stat_recv, d).wait_send()
        stat_copy(stat2_slots, stat2_send, stat2_recv, d).wait_send()
    for dz in range(1, n_vp):
        pick_copy(dz).wait_send()

    for dz, dt, j in peers:
        lse_copy(dz, dt, j).wait_recv()
    pairs = lse_slots[:, 0, :]
    top = jnp.max(pairs, axis=0, keepdims=True)
    scaled = pltpu.roll(pairs, rows, axis=1) * jnp.exp(pairs - top)
    tot = jnp.sum(scaled, axis=0, keepdims=True)
    lse_out[...] = jnp.broadcast_to(top + jnp.log(tot), (8, LANES))
    for dz, dt, j in peers:
        lse_copy(dz, dt, j).wait_send()


def finish_kernel(n_full, rem, logits, lse, next_rows, out_hbm, sum_hbm, next_hbm, stage, sums, sem, small_sem):
    rows = stage.shape[0]
    next_copy = pltpu.make_async_copy(next_rows, next_hbm, small_sem.at[0])
    next_copy.start()
    sums[...] = lse[0:1, 0:rows]
    sum_copy = pltpu.make_async_copy(sums, sum_hbm, small_sem.at[1])
    sum_copy.start()
    log_sum = lse[...].T[:rows, 0:1]
    copies = []
    for r in range(rows // 8):
        here = slice(8 * r, 8 * r + 8)
        part = jnp.broadcast_to(log_sum[here], (8, LANES))
        for k in range(n_full + 1):
            cols = CHUNK if k < n_full else rem
            for b in range(0, cols, LANES):
                w = min(LANES, cols - b)
                at = k * CHUNK + b
                stage[here, at:at + w] = logits[k, here, b:b + w] - part[:, :w]
        copy = pltpu.make_async_copy(stage.at[here, :], out_hbm.at[here, :], sem.at[r])
        copy.start()
        copies.append(copy)
    for copy in [next_copy, sum_copy] + copies:
        copy.wait()


def solution(mesh):
    n_vp = mesh.shape["vp"]
    assert mesh.shape["tp"] == 4

    def per_device(hidden, lnf_gain, lnf_bias, emb_table, next_tok, eln_gain, eln_bias):
        rows, width = hidden.shape
        seg = emb_table.shape[0] // 4
        n_full, rem = divmod(seg, CHUNK)
        n_chunks = n_full + 1
        rem_pad = -(-rem // LANES) * LANES
        assert 2 * rows == LANES and n_vp == 4 and rem == 2 * LANES + LANES // 2 and n_full > DEPTH and n_full % 2 == 0
        f32, bf16 = jnp.float32, jnp.bfloat16
        dma = pltpu.SemaphoreType.DMA
        hbm = pl.BlockSpec(memory_space=pltpu.HBM)
        vmem = pl.BlockSpec(memory_space=pltpu.VMEM)
        logits, lse, next_rows = pl.pallas_call(
            functools.partial(head_kernel, n_vp, n_full, rem, width),
            out_shape=(
                pltpu.VMEM((n_chunks, rows, CHUNK), f32),
                pltpu.VMEM((8, LANES), f32),
                pltpu.VMEM((rows, width), bf16),
            ),
            in_specs=[hbm] * 7,
            out_specs=(vmem, vmem, vmem),
            scratch_shapes=[
                pltpu.VMEM((rows, width), bf16),
                *[pltpu.VMEM((width,), f32)] * 4,
                pltpu.VMEM((1, rows), jnp.int32),
                pltpu.VMEM((DEPTH, 2, CHUNK, width), bf16),
                pltpu.VMEM((4, rem_pad, width), bf16),
                pltpu.VMEM((rows, width), bf16),
                pltpu.VMEM((rows, width), f32),
                pltpu.VMEM((n_vp, rows, width), f32),
                pltpu.VMEM((2 * n_chunks, rows, CHUNK), f32),
                pltpu.VMEM((2 * n_chunks, rows, CHUNK), f32),
                pltpu.VMEM((2 * n_chunks, rows, CHUNK), f32),
                pltpu.VMEM((n_chunks, rows, CHUNK), f32),
                pltpu.VMEM((rows, LANES), f32),
                pltpu.VMEM((rows, LANES), f32),
                pltpu.VMEM((4, 1, LANES), f32),
                pltpu.VMEM((4, 1, LANES), f32),
                pltpu.VMEM((n_vp * 4, 1, LANES), f32),
                dma((6,)), dma((DEPTH, 2)), dma((4,)),
                dma((3,)), dma((3,)), dma((3,)), dma((3,)),
                dma((2 * n_chunks,)), dma((2 * n_chunks,)),
                dma((n_chunks,)), dma((n_chunks,)),
                dma((n_vp - 1,)), dma((n_vp - 1,)),
                dma((n_vp * 4 - 1,)), dma((n_vp * 4 - 1,)),
                pltpu.SemaphoreType.REGULAR((3,)),
                pltpu.VMEM((rows + rows // 4, 2 * LANES), f32), pltpu.VMEM((rows + rows // 4, 2 * LANES), f32),
            ],
            compiler_params=pltpu.CompilerParams(
                collective_id=0, has_side_effects=True, vmem_limit_bytes=52 * 1024 * 1024
            ),
            name="head",
        )(
            *[
                pltpu.with_memory_space_constraint(a, pltpu.HBM)
                for a in (hidden, lnf_gain, lnf_bias, emb_table, next_tok.reshape(1, rows), eln_gain, eln_bias)
            ]
        )
        logprobs, log_sum, next_in = pl.pallas_call(
            functools.partial(finish_kernel, n_full, rem),
            out_shape=(
                jax.ShapeDtypeStruct((rows, seg), f32),
                jax.ShapeDtypeStruct((1, rows), f32),
                jax.ShapeDtypeStruct((rows, width), bf16),
            ),
            in_specs=[vmem, vmem, vmem],
            out_specs=(hbm, hbm, hbm),
            scratch_shapes=[pltpu.VMEM((rows, seg), f32), pltpu.VMEM((1, rows), f32), dma((rows // 8,)), dma((2,))],
            compiler_params=pltpu.CompilerParams(vmem_limit_bytes=24 * 1024 * 1024),
            name="finish",
        )(logits, lse, next_rows)
        return logprobs, log_sum.reshape(rows), next_in

    return jax.shard_map(
        per_device,
        mesh=mesh,
        in_specs=(P("dp", "tp"), P("tp"), P("tp"), P("vp", "tp"), P("dp"), P("tp"), P("tp")),
        out_specs=(P("dp", ("vp", "tp")), P("dp"), P("dp", "tp")),
        check_vma=False,
    )
```

```python
import functools

import jax
import jax.numpy as jnp
from jax import lax
from jax.experimental import pallas as pl
from jax.experimental.pallas import tpu as pltpu
from jax.sharding import PartitionSpec as P

NORM_EPS = 1e-5
CHUNK = 768
LANES = 128
DEPTH = 3
LOWEST = -3.0e38
MESH = pl.DeviceIdType.MESH


def head_kernel(
    n_vp, n_full, rem, width,
    hid_hbm, gain1_hbm, bias1_hbm, tab_hbm, tok_hbm, gain2_hbm, bias2_hbm,
    logits, lse_out, next_out,
    hid, gain1, bias1, gain2, bias2, tok, tab, tab_rem, normed, picked, picked_rx,
    tx, rx, acc, y_rx, m_run, s_run, stat_slots, stat2_slots, lse_slots,
    in_sem, tab_sem, rem_sem, stat_send, stat_recv, stat2_send, stat2_recv,
    tx_send, tx_recv, y_send, y_recv, pick_send, pick_recv, lse_send, lse_recv, near_sem, y_tail, y_tail_rx,
):
    rows = hid.shape[0]
    n_chunks = n_full + 1
    seg = n_full * CHUNK + rem
    rem_pad = tab_rem.shape[1]
    vp = lax.axis_index("vp")
    tp = lax.axis_index("tp")
    chip_y = tp // 2
    core = lax.rem(tp, 2)
    sibling = tp + 1 - 2 * core
    across = lax.rem(tp + 2, 4)
    my_rank = vp * 4 + tp

    peers = []
    for dz in reversed(range(n_vp)):
        for dt in reversed(range(4)):
            if dz or dt:
                peers.append((dz, dt, dz * 4 + dt))

    def peer_id(dz, dt):
        return {"vp": lax.rem(vp + dz, n_vp), "tp": lax.rem(tp + dt, 4)}

    hid_copy = pltpu.make_async_copy(hid_hbm, hid, in_sem.at[0])
    hid_copy.start()

    has_low = jnp.where(vp > 0, 1, 0)
    has_high = jnp.where(vp < n_vp - 1, 1, 0)

    def signal_vp(sem):
        @pl.when(vp > 0)
        def _():
            pl.semaphore_signal(sem, inc=1, device_id={"vp": vp - 1}, device_id_type=MESH)

        @pl.when(vp < n_vp - 1)
        def _():
            pl.semaphore_signal(sem, inc=1, device_id={"vp": vp + 1}, device_id_type=MESH)

    def signal_tp(sem):
        for dt in (2, 3, 1):
            pl.semaphore_signal(sem, inc=1, device_id=peer_id(0, dt), device_id_type=MESH)

    barrier = pltpu.get_barrier_semaphore()
    signal_tp(barrier)
    signal_vp(barrier)

    def seg_start(phase, which):
        y = chip_y + (1 - phase) * (1 - 2 * chip_y)
        c = core + (1 - which) * (1 - 2 * core)
        return (y * 2 + c) * seg

    def row_start(i, which):
        phase = jnp.where(i >= n_full, 1, 0)
        k = i - phase * n_full
        return pl.multiple_of(seg_start(phase, which) + k * CHUNK, 64)

    def tab_copy(i, which):
        slot = lax.rem(i, DEPTH)
        return pltpu.make_async_copy(
            tab_hbm.at[pl.ds(row_start(i, which), CHUNK), :], tab.at[slot, which], tab_sem.at[slot, which]
        )

    def rem_start(phase, which):
        return pl.multiple_of(seg_start(phase, which) + n_full * CHUNK, 64)

    def rem_copy(phase, which):
        return pltpu.make_async_copy(
            tab_hbm.at[pl.ds(rem_start(phase, which), rem), :],
            tab_rem.at[phase * 2 + which, pl.ds(0, rem), :],
            rem_sem.at[phase * 2 + which],
        )

    small = [
        pltpu.make_async_copy(gain1_hbm, gain1, in_sem.at[1]),
        pltpu.make_async_copy(bias1_hbm, bias1, in_sem.at[2]),
        pltpu.make_async_copy(gain2_hbm, gain2, in_sem.at[3]),
        pltpu.make_async_copy(bias2_hbm, bias2, in_sem.at[4]),
        pltpu.make_async_copy(tok_hbm, tok, in_sem.at[5]),
    ]

    picked[...] = jnp.zeros_like(picked)
    m_run[...] = jnp.full_like(m_run, LOWEST)
    s_run[...] = jnp.zeros_like(s_run)
    tab_rem[:, rem:, :] = jnp.zeros((4, rem_pad - rem, width), jnp.bfloat16)

    lane = lax.broadcasted_iota(jnp.int32, (rows, LANES), 1)

    def stat_row(x):
        s1 = jnp.sum(x, axis=1, keepdims=True)
        s2 = jnp.sum(x * x, axis=1, keepdims=True)
        return jnp.broadcast_to(jnp.concatenate([s1, s2], axis=0), (LANES, LANES)).T[0:1, :]

    def stat_copy(slots, send, recv, d):
        return pltpu.make_async_remote_copy(
            src_ref=slots.at[tp], dst_ref=slots.at[tp], send_sem=send.at[0], recv_sem=recv.at[0],
            device_id=peer_id(0, d), device_id_type=MESH,
        )

    def all_of(slots, sem, count):
        return pltpu.make_async_copy(slots.at[pl.ds(0, count)], slots.at[pl.ds(0, count)], sem.at[0])

    def norm(x, slots, send, recv, gain, bias):
        all_of(slots, recv, 3).wait()
        total = (slots[0] + slots[1]) + (slots[2] + slots[3])
        full_width = 4.0 * width
        total = jnp.broadcast_to(total, (8, LANES)) / full_width
        mean = total
        var = pltpu.roll(total, rows, axis=1) - mean * mean
        inv = lax.rsqrt(var + NORM_EPS)
        row = lax.broadcasted_iota(jnp.int32, (8, LANES), 0)
        back = jnp.where(row == 0, mean, inv).T
        mean_c = back[:rows, 0:1]
        inv_c = back[:rows, 1:2]
        return (x - mean_c) * inv_c * gain + bias

    hid_copy.wait()
    x1 = hid[...].astype(jnp.float32)
    stat_slots[pl.ds(tp, 1)] = stat_row(x1)[None]
    pl.semaphore_wait(barrier, 3 + has_low + has_high)
    for d in (2, 3, 1):
        stat_copy(stat_slots, stat_send, stat_recv, d).start()
    for copy in small:
        copy.start()
    for which in range(2):
        rem_copy(0, which).start()
    for i in range(min(DEPTH - 1, 2 * n_full)):
        for which in range(2):
            tab_copy(i, which).start()
    for which in range(2):
        rem_copy(1, which).start()
    for copy in small:
        copy.wait()
    normed[...] = norm(
        x1, stat_slots, stat_send, stat_recv, gain1[...].reshape(1, width), bias1[...].reshape(1, width)
    ).astype(jnp.bfloat16)

    def tx_copy(e, cols=None):
        view = (lambda r: r.at[e]) if cols is None else (lambda r: r.at[e, :, pl.ds(0, cols)])
        return pltpu.make_async_remote_copy(
            src_ref=view(tx), dst_ref=view(rx), send_sem=tx_send.at[e], recv_sem=tx_recv.at[e],
            device_id={"tp": sibling}, device_id_type=MESH,
        )

    def y_copy(e):
        return pltpu.make_async_remote_copy(
            src_ref=acc.at[e], dst_ref=y_rx.at[e], send_sem=y_send.at[e], recv_sem=y_recv.at[e],
            device_id={"tp": across}, device_id_type=MESH,
        )

    half = LANES // 2
    whole = rem - half

    def y_tail_copy():
        return pltpu.make_async_remote_copy(
            src_ref=y_tail, dst_ref=y_tail_rx, send_sem=y_send.at[n_full], recv_sem=y_recv.at[n_full],
            device_id={"tp": across}, device_id_type=MESH,
        )

    def pack_tail(block):
        y_tail[0:rows, :] = block[:, 0:whole]
        low = block[0:rows // 2, whole:whole + LANES]
        high = pltpu.roll(block[rows // 2:rows, whole:whole + LANES], half, axis=1)
        both = jnp.where(lane[0:rows // 2] < half, low, high)
        y_tail[rows:rows + rows // 4, 0:LANES] = both[0:rows // 4]
        y_tail[rows:rows + rows // 4, LANES:2 * LANES] = both[rows // 4:rows // 2]

    def tail_block(b):
        if (b + 1) * LANES <= whole:
            return y_tail_rx[0:rows, b * LANES:(b + 1) * LANES]
        both = jnp.concatenate(
            [y_tail_rx[rows:rows + rows // 4, 0:LANES], y_tail_rx[rows:rows + rows // 4, LANES:2 * LANES]], axis=0
        )
        return jnp.concatenate([both, pltpu.roll(both, half, axis=1)], axis=0)

    def partial(block):
        return lax.dot_general(
            normed[...], block, (((1,), (1,)), ((), ())), preferred_element_type=jnp.float32
        )

    tok_col = jnp.broadcast_to(tok[...], (8, rows)).T[:, 0:1]
    tok_local = tok_col - vp * (4 * seg)

    def add_picked(block, start):
        n = block.shape[0]
        at = lax.broadcasted_iota(jnp.int32, (rows, n), 1)
        hot = jnp.where(at == tok_local - start, 1.0, 0.0).astype(jnp.bfloat16)
        picked[...] += lax.dot_general(
            hot, block, (((1,), (0,)), ((), ())), preferred_element_type=jnp.float32
        )

    def add_picked_rem(phase, which):
        at = lax.broadcasted_iota(jnp.int32, (rows, rem_pad), 1)
        hit = (at == tok_local - rem_start(phase, which)) & (at < rem)
        hot = jnp.where(hit, 1.0, 0.0).astype(jnp.bfloat16)
        picked[...] += lax.dot_general(
            hot, tab_rem[phase * 2 + which], (((1,), (0,)), ((), ())), preferred_element_type=jnp.float32
        )

    def run_phase(phase):
        base = phase * n_chunks

        last = base + n_full
        first = phase * n_full
        slot0 = first % DEPTH
        rem_copy(phase, 0).wait()
        tx[last, :, 0:rem_pad] = partial(tab_rem[phase * 2])
        tx_copy(last, rem_pad).start()
        tab_copy(first, 0).wait()
        tx[base] = partial(tab[slot0, 0])
        tx_copy(base).start()
        rem_copy(phase, 1).wait()
        mine = partial(tab_rem[phase * 2 + 1])
        acc[last, :, 0:rem_pad] = mine
        tab_copy(first, 1).wait()
        acc[base] = partial(tab[slot0, 1])
        tx_copy(last, rem_pad).wait_recv()
        if phase == 0:
            pack_tail(acc[last, :, 0:rem_pad] + rx[last, :, 0:rem_pad])
            y_tail_copy().start()
        else:
            acc[last, :, 0:rem_pad] = acc[last, :, 0:rem_pad] + rx[last, :, 0:rem_pad]

        def finish(e):
            tx_copy(e).wait_recv()
            acc[e] = acc[e] + rx[e]
            if phase == 0:
                y_copy(e).start()

        tab_copy(first + DEPTH - 1, 0).start()
        tab_copy(first + DEPTH - 1, 1).start()
        add_picked_rem(phase, 0)
        add_picked_rem(phase, 1)
        finish(base)
        add_picked(tab[slot0, 0], row_start(first, 0))
        add_picked(tab[slot0, 1], row_start(first, 1))

        def body(i, carry):
            k = i - phase * n_full
            e = base + k

            @pl.when(i + DEPTH - 1 < 2 * n_full)
            def _():
                tab_copy(i + DEPTH - 1, 0).start()
                tab_copy(i + DEPTH - 1, 1).start()

            slot = lax.rem(i, DEPTH)
            tab_copy(i, 0).wait()
            tx[e] = partial(tab[slot, 0])
            tx_copy(e).start()
            tab_copy(i, 1).wait()
            acc[e] = partial(tab[slot, 1])

            @pl.when(k > 1)
            def _():
                finish(e - 1)

            add_picked(tab[slot, 0], row_start(i, 0))
            add_picked(tab[slot, 1], row_start(i, 1))
            return carry

        lax.fori_loop(first + 1, first + n_full, body, 0)
        finish(last - 1)

    signal_vp(near_sem.at[0])
    run_phase(0)
    pl.semaphore_wait(near_sem.at[0], has_low + has_high)
    signal_vp(near_sem.at[1])
    run_phase(1)
    pl.semaphore_wait(near_sem.at[1], has_low + has_high)
    signal_tp(near_sem.at[2])

    def pick_copy(dz):
        return pltpu.make_async_remote_copy(
            src_ref=picked, dst_ref=picked_rx.at[vp], send_sem=pick_send.at[dz - 1], recv_sem=pick_recv.at[dz - 1],
            device_id=peer_id(dz, 0), device_id_type=MESH,
        )

    for dz in range(1, n_vp):
        pick_copy(dz).start()
    picked_rx[pl.ds(vp, 1)] = picked[...][None]
    for dz in range(1, n_vp):
        pick_copy(dz).wait_recv()
    x2 = picked_rx[0]
    for z in range(1, n_vp):
        x2 = x2 + picked_rx[z]
    stat2_slots[pl.ds(tp, 1)] = stat_row(x2)[None]
    for d in (2, 3, 1):
        stat_copy(stat2_slots, stat2_send, stat2_recv, d).start()
    next_out[...] = norm(
        x2, stat2_slots, stat2_send, stat2_recv, gain2[...].reshape(1, width), bias2[...].reshape(1, width)
    ).astype(jnp.bfloat16)

    def absorb(k, cols):
        e = n_chunks + k
        blocks = cols // LANES
        top = m_run[...]
        for b in range(blocks):
            sl = pl.ds(b * LANES, LANES)
            z = acc[e, :, sl] + (y_rx[k, :, sl] if cols == CHUNK else tail_block(b))
            logits[k, :, sl] = z
            if cols != CHUNK and (b + 1) * LANES > rem:
                z = jnp.where(lane < rem - b * LANES, z, -jnp.inf)
            top = jnp.maximum(top, z)
        total = s_run[...] * jnp.exp(m_run[...] - top)
        for b in range(blocks):
            z = logits[k, :, pl.ds(b * LANES, LANES)]
            if cols != CHUNK and (b + 1) * LANES > rem:
                z = jnp.where(lane < rem - b * LANES, z, -jnp.inf)
            total = total + jnp.exp(z - top)
        m_run[...] = top
        s_run[...] = total

    def absorb_body(k, carry):
        y_copy(k).wait_recv()
        absorb(k, CHUNK)
        tx_copy(k).wait_send()
        tx_copy(n_chunks + k).wait_send()

        @pl.when(k > 0)
        def _():
            y_copy(k - 1).wait_send()

        return carry

    y_tail_copy().wait_recv()
    absorb(n_full, rem_pad)
    pl.semaphore_wait(near_sem.at[2], 3)
    tx_copy(n_full, rem_pad).wait_send()
    tx_copy(n_chunks + n_full, rem_pad).wait_send()
    y_tail_copy().wait_send()
    all_of(stat_slots, stat_send, 3).wait()
    all_of(stat2_slots, stat2_send, 3).wait()
    for dz in range(1, n_vp):
        pick_copy(dz).wait_send()
    lax.fori_loop(0, n_full, absorb_body, 0)

    m_t = m_run[...].T
    top = jnp.max(m_t, axis=0, keepdims=True)
    tot = jnp.sum(s_run[...].T * jnp.exp(m_t - top), axis=0, keepdims=True)
    lse_slots[pl.ds(my_rank, 1), :, 0:rows] = top[None]
    lse_slots[pl.ds(my_rank, 1), :, rows:LANES] = tot[None]

    def lse_copy(dz, dt, j):
        return pltpu.make_async_remote_copy(
            src_ref=lse_slots.at[my_rank], dst_ref=lse_slots.at[my_rank],
            send_sem=lse_send.at[0], recv_sem=lse_recv.at[0],
            device_id=peer_id(dz, dt), device_id_type=MESH,
        )

    for dz, dt, j in peers:
        lse_copy(dz, dt, j).start()

    y_copy(n_full - 1).wait_send()
    all_of(lse_slots, lse_recv, len(peers)).wait()
    pairs = lse_slots[:, 0, :]
    top = jnp.max(pairs, axis=0, keepdims=True)
    scaled = pltpu.roll(pairs, rows, axis=1) * jnp.exp(pairs - top)
    tot = jnp.sum(scaled, axis=0, keepdims=True)
    lse_out[...] = jnp.broadcast_to(top + jnp.log(tot), (8, LANES))
    all_of(lse_slots, lse_send, len(peers)).wait()


def finish_kernel(n_full, rem, logits, lse, next_rows, out_hbm, sum_hbm, next_hbm, stage, sums, sem, small_sem):
    rows = stage.shape[0]
    next_copy = pltpu.make_async_copy(next_rows, next_hbm, small_sem.at[0])
    next_copy.start()
    sums[...] = lse[0:1, 0:rows]
    sum_copy = pltpu.make_async_copy(sums, sum_hbm, small_sem.at[1])
    sum_copy.start()
    log_sum = lse[...].T[:rows, 0:1]
    copies = []
    for r in range(rows // 8):
        here = slice(8 * r, 8 * r + 8)
        part = jnp.broadcast_to(log_sum[here], (8, LANES))
        for k in range(n_full + 1):
            cols = CHUNK if k < n_full else rem
            for b in range(0, cols, LANES):
                w = min(LANES, cols - b)
                at = k * CHUNK + b
                stage[here, at:at + w] = logits[k, here, b:b + w] - part[:, :w]
        copy = pltpu.make_async_copy(stage.at[here, :], out_hbm.at[here, :], sem.at[r])
        copy.start()
        copies.append(copy)
    for copy in [next_copy, sum_copy] + copies:
        copy.wait()


def solution(mesh):
    n_vp = mesh.shape["vp"]
    assert mesh.shape["tp"] == 4

    def per_device(hidden, lnf_gain, lnf_bias, emb_table, next_tok, eln_gain, eln_bias):
        rows, width = hidden.shape
        seg = emb_table.shape[0] // 4
        n_full, rem = divmod(seg, CHUNK)
        n_chunks = n_full + 1
        rem_pad = -(-rem // LANES) * LANES
        assert 2 * rows == LANES and n_vp == 4 and rem == 2 * LANES + LANES // 2 and n_full > DEPTH
        f32, bf16 = jnp.float32, jnp.bfloat16
        dma = pltpu.SemaphoreType.DMA
        hbm = pl.BlockSpec(memory_space=pltpu.HBM)
        vmem = pl.BlockSpec(memory_space=pltpu.VMEM)
        logits, lse, next_rows = pl.pallas_call(
            functools.partial(head_kernel, n_vp, n_full, rem, width),
            out_shape=(
                pltpu.VMEM((n_chunks, rows, CHUNK), f32),
                pltpu.VMEM((8, LANES), f32),
                pltpu.VMEM((rows, width), bf16),
            ),
            in_specs=[hbm] * 7,
            out_specs=(vmem, vmem, vmem),
            scratch_shapes=[
                pltpu.VMEM((rows, width), bf16),
                *[pltpu.VMEM((width,), f32)] * 4,
                pltpu.VMEM((1, rows), jnp.int32),
                pltpu.VMEM((DEPTH, 2, CHUNK, width), bf16),
                pltpu.VMEM((4, rem_pad, width), bf16),
                pltpu.VMEM((rows, width), bf16),
                pltpu.VMEM((rows, width), f32),
                pltpu.VMEM((n_vp, rows, width), f32),
                pltpu.VMEM((2 * n_chunks, rows, CHUNK), f32),
                pltpu.VMEM((2 * n_chunks, rows, CHUNK), f32),
                pltpu.VMEM((2 * n_chunks, rows, CHUNK), f32),
                pltpu.VMEM((n_chunks, rows, CHUNK), f32),
                pltpu.VMEM((rows, LANES), f32),
                pltpu.VMEM((rows, LANES), f32),
                pltpu.VMEM((4, 1, LANES), f32),
                pltpu.VMEM((4, 1, LANES), f32),
                pltpu.VMEM((n_vp * 4, 1, LANES), f32),
                dma((6,)), dma((DEPTH, 2)), dma((4,)),
                dma((1,)), dma((1,)), dma((1,)), dma((1,)),
                dma((2 * n_chunks,)), dma((2 * n_chunks,)),
                dma((n_chunks,)), dma((n_chunks,)),
                dma((n_vp - 1,)), dma((n_vp - 1,)),
                dma((1,)), dma((1,)),
                pltpu.SemaphoreType.REGULAR((3,)),
                pltpu.VMEM((rows + rows // 4, 2 * LANES), f32), pltpu.VMEM((rows + rows // 4, 2 * LANES), f32),
            ],
            compiler_params=pltpu.CompilerParams(
                collective_id=0, has_side_effects=True, vmem_limit_bytes=52 * 1024 * 1024
            ),
            name="head",
        )(
            *[
                pltpu.with_memory_space_constraint(a, pltpu.HBM)
                for a in (hidden, lnf_gain, lnf_bias, emb_table, next_tok.reshape(1, rows), eln_gain, eln_bias)
            ]
        )
        logprobs, log_sum, next_in = pl.pallas_call(
            functools.partial(finish_kernel, n_full, rem),
            out_shape=(
                jax.ShapeDtypeStruct((rows, seg), f32),
                jax.ShapeDtypeStruct((1, rows), f32),
                jax.ShapeDtypeStruct((rows, width), bf16),
            ),
            in_specs=[vmem, vmem, vmem],
            out_specs=(hbm, hbm, hbm),
            scratch_shapes=[pltpu.VMEM((rows, seg), f32), pltpu.VMEM((1, rows), f32), dma((rows // 8,)), dma((2,))],
            compiler_params=pltpu.CompilerParams(vmem_limit_bytes=24 * 1024 * 1024),
            name="finish",
        )(logits, lse, next_rows)
        return logprobs, log_sum.reshape(rows), next_in

    return jax.shard_map(
        per_device,
        mesh=mesh,
        in_specs=(P("dp", "tp"), P("tp"), P("tp"), P("vp", "tp"), P("dp"), P("tp"), P("tp")),
        out_specs=(P("dp", ("vp", "tp")), P("dp"), P("dp", "tp")),
        check_vma=False,
    )
```

```python
import functools

import jax
import jax.numpy as jnp
from jax import lax
from jax.experimental import pallas as pl
from jax.experimental.pallas import tpu as pltpu
from jax.sharding import PartitionSpec as P

NORM_EPS = 1e-5
CHUNK = 768
LANES = 128
DEPTH = 3
LOWEST = -3.0e38
MESH = pl.DeviceIdType.MESH


def head_kernel(
    n_vp, n_full, rem, width,
    hid_hbm, gain1_hbm, bias1_hbm, tab_hbm, tok_hbm, gain2_hbm, bias2_hbm,
    logits, lse_out, next_out,
    hid, gain1, bias1, gain2, bias2, tok, tab, tab_rem, normed, picked, picked_rx,
    tx, rx, acc, y_rx, m_run, s_run, stat_slots, stat2_slots, lse_slots,
    in_sem, tab_sem, rem_sem, stat_send, stat_recv, stat2_send, stat2_recv,
    tx_send, tx_recv, y_send, y_recv, pick_send, pick_recv, lse_send, lse_recv, near_sem, y_tail, y_tail_rx,
):
    rows = hid.shape[0]
    n_chunks = n_full + 1
    seg = n_full * CHUNK + rem
    rem_pad = tab_rem.shape[1]
    vp = lax.axis_index("vp")
    tp = lax.axis_index("tp")
    chip_y = tp // 2
    core = lax.rem(tp, 2)
    sibling = tp + 1 - 2 * core
    across = lax.rem(tp + 2, 4)
    my_rank = vp * 4 + tp

    peers = []
    for dz in reversed(range(n_vp)):
        for dt in reversed(range(4)):
            if dz or dt:
                peers.append((dz, dt, dz * 4 + dt))

    def peer_id(dz, dt):
        return {"vp": lax.rem(vp + dz, n_vp), "tp": lax.rem(tp + dt, 4)}

    hid_copy = pltpu.make_async_copy(hid_hbm, hid, in_sem.at[0])
    hid_copy.start()

    has_low = jnp.where(vp > 0, 1, 0)
    has_high = jnp.where(vp < n_vp - 1, 1, 0)

    def signal_vp(sem):
        @pl.when(vp > 0)
        def _():
            pl.semaphore_signal(sem, inc=1, device_id={"vp": vp - 1}, device_id_type=MESH)

        @pl.when(vp < n_vp - 1)
        def _():
            pl.semaphore_signal(sem, inc=1, device_id={"vp": vp + 1}, device_id_type=MESH)

    def signal_tp(sem):
        for dt in (2, 3, 1):
            pl.semaphore_signal(sem, inc=1, device_id=peer_id(0, dt), device_id_type=MESH)

    barrier = pltpu.get_barrier_semaphore()
    signal_tp(barrier)
    signal_vp(barrier)

    def seg_start(phase, which):
        y = chip_y + (1 - phase) * (1 - 2 * chip_y)
        c = core + (1 - which) * (1 - 2 * core)
        return (y * 2 + c) * seg

    def row_start(i, which):
        phase = jnp.where(i >= n_full, 1, 0)
        k = i - phase * n_full
        return pl.multiple_of(seg_start(phase, which) + k * CHUNK, 64)

    def tab_copy(i, which):
        slot = lax.rem(i, DEPTH)
        return pltpu.make_async_copy(
            tab_hbm.at[pl.ds(row_start(i, which), CHUNK), :], tab.at[slot, which], tab_sem.at[slot, which]
        )

    def rem_start(phase, which):
        return pl.multiple_of(seg_start(phase, which) + n_full * CHUNK, 64)

    def rem_copy(phase, which):
        return pltpu.make_async_copy(
            tab_hbm.at[pl.ds(rem_start(phase, which), rem), :],
            tab_rem.at[phase * 2 + which, pl.ds(0, rem), :],
            rem_sem.at[phase * 2 + which],
        )

    small = [
        pltpu.make_async_copy(gain1_hbm, gain1, in_sem.at[1]),
        pltpu.make_async_copy(bias1_hbm, bias1, in_sem.at[2]),
        pltpu.make_async_copy(gain2_hbm, gain2, in_sem.at[3]),
        pltpu.make_async_copy(bias2_hbm, bias2, in_sem.at[4]),
        pltpu.make_async_copy(tok_hbm, tok, in_sem.at[5]),
    ]

    picked[...] = jnp.zeros_like(picked)
    m_run[...] = jnp.full_like(m_run, LOWEST)
    s_run[...] = jnp.zeros_like(s_run)
    tab_rem[:, rem:, :] = jnp.zeros((4, rem_pad - rem, width), jnp.bfloat16)

    lane = lax.broadcasted_iota(jnp.int32, (rows, LANES), 1)

    def stat_row(x):
        s1 = jnp.sum(x, axis=1, keepdims=True)
        s2 = jnp.sum(x * x, axis=1, keepdims=True)
        return jnp.broadcast_to(jnp.concatenate([s1, s2], axis=0), (LANES, LANES)).T[0:1, :]

    def stat_copy(slots, send, recv, d):
        return pltpu.make_async_remote_copy(
            src_ref=slots.at[tp], dst_ref=slots.at[tp], send_sem=send.at[0], recv_sem=recv.at[0],
            device_id=peer_id(0, d), device_id_type=MESH,
        )

    def all_of(slots, sem, count):
        return pltpu.make_async_copy(slots.at[pl.ds(0, count)], slots.at[pl.ds(0, count)], sem.at[0])

    def norm(x, slots, send, recv, gain, bias):
        all_of(slots, recv, 3).wait()
        total = (slots[0] + slots[1]) + (slots[2] + slots[3])
        full_width = 4.0 * width
        total = jnp.broadcast_to(total, (8, LANES)) / full_width
        mean = total
        var = pltpu.roll(total, rows, axis=1) - mean * mean
        inv = lax.rsqrt(var + NORM_EPS)
        row = lax.broadcasted_iota(jnp.int32, (8, LANES), 0)
        back = jnp.where(row == 0, mean, inv).T
        mean_c = back[:rows, 0:1]
        inv_c = back[:rows, 1:2]
        return (x - mean_c) * inv_c * gain + bias

    hid_copy.wait()
    x1 = hid[...].astype(jnp.float32)
    stat_slots[pl.ds(tp, 1)] = stat_row(x1)[None]
    pl.semaphore_wait(barrier, 3 + has_low + has_high)
    for d in (2, 3, 1):
        stat_copy(stat_slots, stat_send, stat_recv, d).start()
    for copy in small:
        copy.start()
    for which in range(2):
        rem_copy(0, which).start()
    for i in range(min(DEPTH - 1, 2 * n_full)):
        for which in range(2):
            tab_copy(i, which).start()
    for which in range(2):
        rem_copy(1, which).start()
    for copy in small:
        copy.wait()
    normed[...] = norm(
        x1, stat_slots, stat_send, stat_recv, gain1[...].reshape(1, width), bias1[...].reshape(1, width)
    ).astype(jnp.bfloat16)

    def tx_copy(e, cols=None):
        view = (lambda r: r.at[e]) if cols is None else (lambda r: r.at[e, :, pl.ds(0, cols)])
        return pltpu.make_async_remote_copy(
            src_ref=view(tx), dst_ref=view(rx), send_sem=tx_send.at[e], recv_sem=tx_recv.at[e],
            device_id={"tp": sibling}, device_id_type=MESH,
        )

    middle = n_full - 8
    sizes = [1, 1, 2] + [4] * (middle // 4) + [middle % 4] * (middle % 4 > 0) + [2, 1, 1]
    groups = [(sum(sizes[:g]), n) for g, n in enumerate(sizes)]

    def y_copy(e, n):
        return pltpu.make_async_remote_copy(
            src_ref=acc.at[pl.ds(e, n)], dst_ref=y_rx.at[pl.ds(e, n)],
            send_sem=y_send.at[e], recv_sem=y_recv.at[e],
            device_id={"tp": across}, device_id_type=MESH,
        )

    half = LANES // 2
    whole = rem - half

    def y_tail_copy():
        return pltpu.make_async_remote_copy(
            src_ref=y_tail, dst_ref=y_tail_rx, send_sem=y_send.at[n_full], recv_sem=y_recv.at[n_full],
            device_id={"tp": across}, device_id_type=MESH,
        )

    def pack_tail(block):
        y_tail[0:rows, :] = block[:, 0:whole]
        low = block[0:rows // 2, whole:whole + LANES]
        high = pltpu.roll(block[rows // 2:rows, whole:whole + LANES], half, axis=1)
        both = jnp.where(lane[0:rows // 2] < half, low, high)
        y_tail[rows:rows + rows // 4, 0:LANES] = both[0:rows // 4]
        y_tail[rows:rows + rows // 4, LANES:2 * LANES] = both[rows // 4:rows // 2]

    def tail_block(b):
        if (b + 1) * LANES <= whole:
            return y_tail_rx[0:rows, b * LANES:(b + 1) * LANES]
        both = jnp.concatenate(
            [y_tail_rx[rows:rows + rows // 4, 0:LANES], y_tail_rx[rows:rows + rows // 4, LANES:2 * LANES]], axis=0
        )
        return jnp.concatenate([both, pltpu.roll(both, half, axis=1)], axis=0)

    def partial(block):
        return lax.dot_general(
            normed[...], block, (((1,), (1,)), ((), ())), preferred_element_type=jnp.float32
        )

    tok_col = jnp.broadcast_to(tok[...], (8, rows)).T[:, 0:1]
    tok_local = tok_col - vp * (4 * seg)

    def add_picked(block, start):
        n = block.shape[0]
        at = lax.broadcasted_iota(jnp.int32, (rows, n), 1)
        hot = jnp.where(at == tok_local - start, 1.0, 0.0).astype(jnp.bfloat16)
        picked[...] += lax.dot_general(
            hot, block, (((1,), (0,)), ((), ())), preferred_element_type=jnp.float32
        )

    def add_picked_rem(phase, which):
        at = lax.broadcasted_iota(jnp.int32, (rows, rem_pad), 1)
        hit = (at == tok_local - rem_start(phase, which)) & (at < rem)
        hot = jnp.where(hit, 1.0, 0.0).astype(jnp.bfloat16)
        picked[...] += lax.dot_general(
            hot, tab_rem[phase * 2 + which], (((1,), (0,)), ((), ())), preferred_element_type=jnp.float32
        )

    def run_phase(phase):
        base = phase * n_chunks

        last = base + n_full
        first = phase * n_full
        slot0 = first % DEPTH
        rem_copy(phase, 0).wait()
        tx[last, :, 0:rem_pad] = partial(tab_rem[phase * 2])
        tx_copy(last, rem_pad).start()
        tab_copy(first, 0).wait()
        tx[base] = partial(tab[slot0, 0])
        tx_copy(base).start()
        rem_copy(phase, 1).wait()
        mine = partial(tab_rem[phase * 2 + 1])
        acc[last, :, 0:rem_pad] = mine
        tab_copy(first, 1).wait()
        acc[base] = partial(tab[slot0, 1])
        tx_copy(last, rem_pad).wait_recv()
        if phase == 0:
            pack_tail(acc[last, :, 0:rem_pad] + rx[last, :, 0:rem_pad])
            y_tail_copy().start()
        else:
            acc[last, :, 0:rem_pad] = acc[last, :, 0:rem_pad] + rx[last, :, 0:rem_pad]

        def finish(e):
            tx_copy(e).wait_recv()
            acc[e] = acc[e] + rx[e]
            if phase == 0:
                for g, n in groups:
                    @pl.when(e == g + n - 1)
                    def _(g=g, n=n):
                        y_copy(g, n).start()

        tab_copy(first + DEPTH - 1, 0).start()
        tab_copy(first + DEPTH - 1, 1).start()
        add_picked_rem(phase, 0)
        add_picked_rem(phase, 1)
        finish(base)
        add_picked(tab[slot0, 0], row_start(first, 0))
        add_picked(tab[slot0, 1], row_start(first, 1))

        def body(i, carry):
            k = i - phase * n_full
            e = base + k

            @pl.when(i + DEPTH - 1 < 2 * n_full)
            def _():
                tab_copy(i + DEPTH - 1, 0).start()
                tab_copy(i + DEPTH - 1, 1).start()

            slot = lax.rem(i, DEPTH)
            tab_copy(i, 0).wait()
            tx[e] = partial(tab[slot, 0])
            tx_copy(e).start()
            tab_copy(i, 1).wait()
            acc[e] = partial(tab[slot, 1])

            @pl.when(k > 1)
            def _():
                finish(e - 1)

            add_picked(tab[slot, 0], row_start(i, 0))
            add_picked(tab[slot, 1], row_start(i, 1))
            return carry

        lax.fori_loop(first + 1, first + n_full, body, 0)
        finish(last - 1)

    signal_vp(near_sem.at[0])
    run_phase(0)
    pl.semaphore_wait(near_sem.at[0], has_low + has_high)
    signal_vp(near_sem.at[1])
    run_phase(1)
    pl.semaphore_wait(near_sem.at[1], has_low + has_high)
    signal_tp(near_sem.at[2])

    def pick_copy(dz):
        return pltpu.make_async_remote_copy(
            src_ref=picked, dst_ref=picked_rx.at[vp], send_sem=pick_send.at[dz - 1], recv_sem=pick_recv.at[dz - 1],
            device_id=peer_id(dz, 0), device_id_type=MESH,
        )

    for dz in range(1, n_vp):
        pick_copy(dz).start()
    picked_rx[pl.ds(vp, 1)] = picked[...][None]
    for dz in range(1, n_vp):
        pick_copy(dz).wait_recv()
    x2 = picked_rx[0]
    for z in range(1, n_vp):
        x2 = x2 + picked_rx[z]
    stat2_slots[pl.ds(tp, 1)] = stat_row(x2)[None]
    for d in (2, 3, 1):
        stat_copy(stat2_slots, stat2_send, stat2_recv, d).start()
    next_out[...] = norm(
        x2, stat2_slots, stat2_send, stat2_recv, gain2[...].reshape(1, width), bias2[...].reshape(1, width)
    ).astype(jnp.bfloat16)

    def absorb(k, cols):
        e = n_chunks + k
        blocks = cols // LANES
        top = m_run[...]
        for b in range(blocks):
            sl = pl.ds(b * LANES, LANES)
            z = acc[e, :, sl] + (y_rx[k, :, sl] if cols == CHUNK else tail_block(b))
            logits[k, :, sl] = z
            if cols != CHUNK and (b + 1) * LANES > rem:
                z = jnp.where(lane < rem - b * LANES, z, -jnp.inf)
            top = jnp.maximum(top, z)
        total = s_run[...] * jnp.exp(m_run[...] - top)
        for b in range(blocks):
            z = logits[k, :, pl.ds(b * LANES, LANES)]
            if cols != CHUNK and (b + 1) * LANES > rem:
                z = jnp.where(lane < rem - b * LANES, z, -jnp.inf)
            total = total + jnp.exp(z - top)
        m_run[...] = top
        s_run[...] = total

    def absorb_body(k, carry):
        absorb(k, CHUNK)
        tx_copy(k).wait_send()
        tx_copy(n_chunks + k).wait_send()
        return carry

    y_tail_copy().wait_recv()
    absorb(n_full, rem_pad)
    pl.semaphore_wait(near_sem.at[2], 3)
    tx_copy(n_full, rem_pad).wait_send()
    tx_copy(n_chunks + n_full, rem_pad).wait_send()
    y_tail_copy().wait_send()
    all_of(stat_slots, stat_send, 3).wait()
    all_of(stat2_slots, stat2_send, 3).wait()
    for dz in range(1, n_vp):
        pick_copy(dz).wait_send()
    for g, n in groups:
        y_copy(g, n).wait_recv()
        lax.fori_loop(g, g + n, absorb_body, 0)

    m_t = m_run[...].T
    top = jnp.max(m_t, axis=0, keepdims=True)
    tot = jnp.sum(s_run[...].T * jnp.exp(m_t - top), axis=0, keepdims=True)
    lse_slots[pl.ds(my_rank, 1), :, 0:rows] = top[None]
    lse_slots[pl.ds(my_rank, 1), :, rows:LANES] = tot[None]

    def lse_copy(dz, dt, j):
        return pltpu.make_async_remote_copy(
            src_ref=lse_slots.at[my_rank], dst_ref=lse_slots.at[my_rank],
            send_sem=lse_send.at[0], recv_sem=lse_recv.at[0],
            device_id=peer_id(dz, dt), device_id_type=MESH,
        )

    for dz, dt, j in peers:
        lse_copy(dz, dt, j).start()

    for g, n in groups:
        y_copy(g, n).wait_send()
    all_of(lse_slots, lse_recv, len(peers)).wait()
    pairs = lse_slots[:, 0, :]
    top = jnp.max(pairs, axis=0, keepdims=True)
    scaled = pltpu.roll(pairs, rows, axis=1) * jnp.exp(pairs - top)
    tot = jnp.sum(scaled, axis=0, keepdims=True)
    lse_out[...] = jnp.broadcast_to(top + jnp.log(tot), (8, LANES))
    all_of(lse_slots, lse_send, len(peers)).wait()


def finish_kernel(n_full, rem, logits, lse, next_rows, out_hbm, sum_hbm, next_hbm, stage, sums, sem, small_sem):
    rows = stage.shape[0]
    next_copy = pltpu.make_async_copy(next_rows, next_hbm, small_sem.at[0])
    next_copy.start()
    sums[...] = lse[0:1, 0:rows]
    sum_copy = pltpu.make_async_copy(sums, sum_hbm, small_sem.at[1])
    sum_copy.start()
    log_sum = lse[...].T[:rows, 0:1]
    copies = []
    for r in range(rows // 8):
        here = slice(8 * r, 8 * r + 8)
        part = jnp.broadcast_to(log_sum[here], (8, LANES))
        for k in range(n_full + 1):
            cols = CHUNK if k < n_full else rem
            for b in range(0, cols, LANES):
                w = min(LANES, cols - b)
                at = k * CHUNK + b
                stage[here, at:at + w] = logits[k, here, b:b + w] - part[:, :w]
        copy = pltpu.make_async_copy(stage.at[here, :], out_hbm.at[here, :], sem.at[r])
        copy.start()
        copies.append(copy)
    for copy in [next_copy, sum_copy] + copies:
        copy.wait()


def solution(mesh):
    n_vp = mesh.shape["vp"]
    assert mesh.shape["tp"] == 4

    def per_device(hidden, lnf_gain, lnf_bias, emb_table, next_tok, eln_gain, eln_bias):
        rows, width = hidden.shape
        seg = emb_table.shape[0] // 4
        n_full, rem = divmod(seg, CHUNK)
        n_chunks = n_full + 1
        rem_pad = -(-rem // LANES) * LANES
        assert 2 * rows == LANES and n_vp == 4 and rem == 2 * LANES + LANES // 2 and n_full >= 8
        f32, bf16 = jnp.float32, jnp.bfloat16
        dma = pltpu.SemaphoreType.DMA
        hbm = pl.BlockSpec(memory_space=pltpu.HBM)
        vmem = pl.BlockSpec(memory_space=pltpu.VMEM)
        logits, lse, next_rows = pl.pallas_call(
            functools.partial(head_kernel, n_vp, n_full, rem, width),
            out_shape=(
                pltpu.VMEM((n_chunks, rows, CHUNK), f32),
                pltpu.VMEM((8, LANES), f32),
                pltpu.VMEM((rows, width), bf16),
            ),
            in_specs=[hbm] * 7,
            out_specs=(vmem, vmem, vmem),
            scratch_shapes=[
                pltpu.VMEM((rows, width), bf16),
                *[pltpu.VMEM((width,), f32)] * 4,
                pltpu.VMEM((1, rows), jnp.int32),
                pltpu.VMEM((DEPTH, 2, CHUNK, width), bf16),
                pltpu.VMEM((4, rem_pad, width), bf16),
                pltpu.VMEM((rows, width), bf16),
                pltpu.VMEM((rows, width), f32),
                pltpu.VMEM((n_vp, rows, width), f32),
                pltpu.VMEM((2 * n_chunks, rows, CHUNK), f32),
                pltpu.VMEM((2 * n_chunks, rows, CHUNK), f32),
                pltpu.VMEM((2 * n_chunks, rows, CHUNK), f32),
                pltpu.VMEM((n_chunks, rows, CHUNK), f32),
                pltpu.VMEM((rows, LANES), f32),
                pltpu.VMEM((rows, LANES), f32),
                pltpu.VMEM((4, 1, LANES), f32),
                pltpu.VMEM((4, 1, LANES), f32),
                pltpu.VMEM((n_vp * 4, 1, LANES), f32),
                dma((6,)), dma((DEPTH, 2)), dma((4,)),
                dma((1,)), dma((1,)), dma((1,)), dma((1,)),
                dma((2 * n_chunks,)), dma((2 * n_chunks,)),
                dma((n_chunks,)), dma((n_chunks,)),
                dma((n_vp - 1,)), dma((n_vp - 1,)),
                dma((1,)), dma((1,)),
                pltpu.SemaphoreType.REGULAR((3,)),
                pltpu.VMEM((rows + rows // 4, 2 * LANES), f32), pltpu.VMEM((rows + rows // 4, 2 * LANES), f32),
            ],
            compiler_params=pltpu.CompilerParams(
                collective_id=0, has_side_effects=True, vmem_limit_bytes=52 * 1024 * 1024
            ),
            name="head",
        )(
            *[
                pltpu.with_memory_space_constraint(a, pltpu.HBM)
                for a in (hidden, lnf_gain, lnf_bias, emb_table, next_tok.reshape(1, rows), eln_gain, eln_bias)
            ]
        )
        logprobs, log_sum, next_in = pl.pallas_call(
            functools.partial(finish_kernel, n_full, rem),
            out_shape=(
                jax.ShapeDtypeStruct((rows, seg), f32),
                jax.ShapeDtypeStruct((1, rows), f32),
                jax.ShapeDtypeStruct((rows, width), bf16),
            ),
            in_specs=[vmem, vmem, vmem],
            out_specs=(hbm, hbm, hbm),
            scratch_shapes=[pltpu.VMEM((rows, seg), f32), pltpu.VMEM((1, rows), f32), dma((rows // 8,)), dma((2,))],
            compiler_params=pltpu.CompilerParams(vmem_limit_bytes=24 * 1024 * 1024),
            name="finish",
        )(logits, lse, next_rows)
        return logprobs, log_sum.reshape(rows), next_in

    return jax.shard_map(
        per_device,
        mesh=mesh,
        in_specs=(P("dp", "tp"), P("tp"), P("tp"), P("vp", "tp"), P("dp"), P("tp"), P("tp")),
        out_specs=(P("dp", ("vp", "tp")), P("dp"), P("dp", "tp")),
        check_vma=False,
    )
```

```python
import functools

import jax
import jax.numpy as jnp
from jax import lax
from jax.experimental import pallas as pl
from jax.experimental.pallas import tpu as pltpu
from jax.sharding import PartitionSpec as P

NORM_EPS = 1e-5
CHUNK = 1536
LANES = 128
DEPTH = 3
LOWEST = -3.0e38
MESH = pl.DeviceIdType.MESH


def head_kernel(
    n_vp, n_full, rem, width,
    hid_hbm, gain1_hbm, bias1_hbm, tab_hbm, tok_hbm, gain2_hbm, bias2_hbm,
    logits, lse_out, next_out,
    hid, gain1, bias1, gain2, bias2, tok, tab, tab_rem, normed, picked, picked_rx,
    tx, rx, acc, y_rx, m_run, s_run, stat_slots, stat2_slots, lse_slots,
    in_sem, tab_sem, rem_sem, stat_send, stat_recv, stat2_send, stat2_recv,
    tx_send, tx_recv, y_send, y_recv, pick_send, pick_recv, lse_send, lse_recv, near_sem, y_tail, y_tail_rx,
):
    rows = hid.shape[0]
    n_chunks = n_full + 1
    seg = n_full * CHUNK + rem
    rem_pad = tab_rem.shape[1]
    vp = lax.axis_index("vp")
    tp = lax.axis_index("tp")
    chip_y = tp // 2
    core = lax.rem(tp, 2)
    sibling = tp + 1 - 2 * core
    across = lax.rem(tp + 2, 4)
    my_rank = vp * 4 + tp

    peers = []
    for dz in reversed(range(n_vp)):
        for dt in reversed(range(4)):
            if dz or dt:
                peers.append((dz, dt, dz * 4 + dt))

    def peer_id(dz, dt):
        return {"vp": lax.rem(vp + dz, n_vp), "tp": lax.rem(tp + dt, 4)}

    hid_copy = pltpu.make_async_copy(hid_hbm, hid, in_sem.at[0])
    hid_copy.start()

    has_low = jnp.where(vp > 0, 1, 0)
    has_high = jnp.where(vp < n_vp - 1, 1, 0)

    def signal_vp(sem):
        @pl.when(vp > 0)
        def _():
            pl.semaphore_signal(sem, inc=1, device_id={"vp": vp - 1}, device_id_type=MESH)

        @pl.when(vp < n_vp - 1)
        def _():
            pl.semaphore_signal(sem, inc=1, device_id={"vp": vp + 1}, device_id_type=MESH)

    def signal_tp(sem):
        for dt in (2, 3, 1):
            pl.semaphore_signal(sem, inc=1, device_id=peer_id(0, dt), device_id_type=MESH)

    barrier = pltpu.get_barrier_semaphore()
    signal_tp(barrier)
    signal_vp(barrier)

    def seg_start(phase, which):
        y = chip_y + (1 - phase) * (1 - 2 * chip_y)
        c = core + (1 - which) * (1 - 2 * core)
        return (y * 2 + c) * seg

    def row_start(i, which):
        phase = jnp.where(i >= n_full, 1, 0)
        k = i - phase * n_full
        return pl.multiple_of(seg_start(phase, which) + k * CHUNK, 64)

    def tab_copy(i, which):
        slot = lax.rem(i, DEPTH)
        return pltpu.make_async_copy(
            tab_hbm.at[pl.ds(row_start(i, which), CHUNK), :], tab.at[slot, which], tab_sem.at[slot, which]
        )

    def rem_start(phase, which):
        return pl.multiple_of(seg_start(phase, which) + n_full * CHUNK, 64)

    def rem_copy(phase, which):
        return pltpu.make_async_copy(
            tab_hbm.at[pl.ds(rem_start(phase, which), rem), :],
            tab_rem.at[phase * 2 + which, pl.ds(0, rem), :],
            rem_sem.at[phase * 2 + which],
        )

    small = [
        pltpu.make_async_copy(gain1_hbm, gain1, in_sem.at[1]),
        pltpu.make_async_copy(bias1_hbm, bias1, in_sem.at[2]),
        pltpu.make_async_copy(gain2_hbm, gain2, in_sem.at[3]),
        pltpu.make_async_copy(bias2_hbm, bias2, in_sem.at[4]),
        pltpu.make_async_copy(tok_hbm, tok, in_sem.at[5]),
    ]

    picked[...] = jnp.zeros_like(picked)
    m_run[...] = jnp.full_like(m_run, LOWEST)
    s_run[...] = jnp.zeros_like(s_run)
    tab_rem[:, rem:, :] = jnp.zeros((4, rem_pad - rem, width), jnp.bfloat16)

    lane = lax.broadcasted_iota(jnp.int32, (rows, LANES), 1)

    def stat_row(x):
        s1 = jnp.sum(x, axis=1, keepdims=True)
        s2 = jnp.sum(x * x, axis=1, keepdims=True)
        return jnp.broadcast_to(jnp.concatenate([s1, s2], axis=0), (LANES, LANES)).T[0:1, :]

    def stat_copy(slots, send, recv, d):
        return pltpu.make_async_remote_copy(
            src_ref=slots.at[tp], dst_ref=slots.at[tp], send_sem=send.at[0], recv_sem=recv.at[0],
            device_id=peer_id(0, d), device_id_type=MESH,
        )

    def all_of(slots, sem, count):
        return pltpu.make_async_copy(slots.at[pl.ds(0, count)], slots.at[pl.ds(0, count)], sem.at[0])

    def norm(x, slots, send, recv, gain, bias):
        all_of(slots, recv, 3).wait()
        total = (slots[0] + slots[1]) + (slots[2] + slots[3])
        full_width = 4.0 * width
        total = jnp.broadcast_to(total, (8, LANES)) / full_width
        mean = total
        var = pltpu.roll(total, rows, axis=1) - mean * mean
        inv = lax.rsqrt(var + NORM_EPS)
        row = lax.broadcasted_iota(jnp.int32, (8, LANES), 0)
        back = jnp.where(row == 0, mean, inv).T
        mean_c = back[:rows, 0:1]
        inv_c = back[:rows, 1:2]
        return (x - mean_c) * inv_c * gain + bias

    hid_copy.wait()
    x1 = hid[...].astype(jnp.float32)
    stat_slots[pl.ds(tp, 1)] = stat_row(x1)[None]
    pl.semaphore_wait(barrier, 3 + has_low + has_high)
    for d in (2, 3, 1):
        stat_copy(stat_slots, stat_send, stat_recv, d).start()
    for copy in small:
        copy.start()
    for which in range(2):
        rem_copy(0, which).start()
    for i in range(min(DEPTH - 1, 2 * n_full)):
        for which in range(2):
            tab_copy(i, which).start()
    for which in range(2):
        rem_copy(1, which).start()
    for copy in small:
        copy.wait()
    normed[...] = norm(
        x1, stat_slots, stat_send, stat_recv, gain1[...].reshape(1, width), bias1[...].reshape(1, width)
    ).astype(jnp.bfloat16)

    def tx_copy(e, cols=None):
        view = (lambda r: r.at[e]) if cols is None else (lambda r: r.at[e, :, pl.ds(0, cols)])
        return pltpu.make_async_remote_copy(
            src_ref=view(tx), dst_ref=view(rx), send_sem=tx_send.at[e], recv_sem=tx_recv.at[e],
            device_id={"tp": sibling}, device_id_type=MESH,
        )

    middle = n_full - 8
    sizes = [1, 1, 2] + [4] * (middle // 4) + [middle % 4] * (middle % 4 > 0) + [2, 1, 1]
    groups = [(sum(sizes[:g]), n) for g, n in enumerate(sizes)]

    def y_copy(e, n):
        return pltpu.make_async_remote_copy(
            src_ref=acc.at[pl.ds(e, n)], dst_ref=y_rx.at[pl.ds(e, n)],
            send_sem=y_send.at[e], recv_sem=y_recv.at[e],
            device_id={"tp": across}, device_id_type=MESH,
        )

    half = LANES // 2
    whole = rem - half

    def y_tail_copy():
        return pltpu.make_async_remote_copy(
            src_ref=y_tail, dst_ref=y_tail_rx, send_sem=y_send.at[n_full], recv_sem=y_recv.at[n_full],
            device_id={"tp": across}, device_id_type=MESH,
        )

    def pack_tail(block):
        y_tail[0:rows, :] = block[:, 0:whole]
        low = block[0:rows // 2, whole:whole + LANES]
        high = pltpu.roll(block[rows // 2:rows, whole:whole + LANES], half, axis=1)
        both = jnp.where(lane[0:rows // 2] < half, low, high)
        y_tail[rows:rows + rows // 4, 0:LANES] = both[0:rows // 4]
        y_tail[rows:rows + rows // 4, LANES:2 * LANES] = both[rows // 4:rows // 2]

    def tail_block(b):
        if (b + 1) * LANES <= whole:
            return y_tail_rx[0:rows, b * LANES:(b + 1) * LANES]
        both = jnp.concatenate(
            [y_tail_rx[rows:rows + rows // 4, 0:LANES], y_tail_rx[rows:rows + rows // 4, LANES:2 * LANES]], axis=0
        )
        return jnp.concatenate([both, pltpu.roll(both, half, axis=1)], axis=0)

    def partial(block):
        return lax.dot_general(
            normed[...], block, (((1,), (1,)), ((), ())), preferred_element_type=jnp.float32
        )

    tok_col = jnp.broadcast_to(tok[...], (8, rows)).T[:, 0:1]
    tok_local = tok_col - vp * (4 * seg)

    def add_picked(block, start):
        n = block.shape[0]
        at = lax.broadcasted_iota(jnp.int32, (rows, n), 1)
        hot = jnp.where(at == tok_local - start, 1.0, 0.0).astype(jnp.bfloat16)
        picked[...] += lax.dot_general(
            hot, block, (((1,), (0,)), ((), ())), preferred_element_type=jnp.float32
        )

    def add_picked_rem(phase, which):
        at = lax.broadcasted_iota(jnp.int32, (rows, rem_pad), 1)
        hit = (at == tok_local - rem_start(phase, which)) & (at < rem)
        hot = jnp.where(hit, 1.0, 0.0).astype(jnp.bfloat16)
        picked[...] += lax.dot_general(
            hot, tab_rem[phase * 2 + which], (((1,), (0,)), ((), ())), preferred_element_type=jnp.float32
        )

    def run_phase(phase):
        base = phase * n_chunks

        last = base + n_full
        first = phase * n_full
        slot0 = first % DEPTH
        rem_copy(phase, 0).wait()
        tx[last, :, 0:rem_pad] = partial(tab_rem[phase * 2])
        tx_copy(last, rem_pad).start()
        tab_copy(first, 0).wait()
        tx[base] = partial(tab[slot0, 0])
        tx_copy(base).start()
        rem_copy(phase, 1).wait()
        mine = partial(tab_rem[phase * 2 + 1])
        acc[last, :, 0:rem_pad] = mine
        tab_copy(first, 1).wait()
        acc[base] = partial(tab[slot0, 1])
        tx_copy(last, rem_pad).wait_recv()
        if phase == 0:
            pack_tail(acc[last, :, 0:rem_pad] + rx[last, :, 0:rem_pad])
            y_tail_copy().start()
        else:
            acc[last, :, 0:rem_pad] = acc[last, :, 0:rem_pad] + rx[last, :, 0:rem_pad]

        def finish(e):
            tx_copy(e).wait_recv()
            acc[e] = acc[e] + rx[e]
            if phase == 0:
                for g, n in groups:
                    @pl.when(e == g + n - 1)
                    def _(g=g, n=n):
                        y_copy(g, n).start()

        tab_copy(first + DEPTH - 1, 0).start()
        tab_copy(first + DEPTH - 1, 1).start()
        add_picked_rem(phase, 0)
        add_picked_rem(phase, 1)
        finish(base)
        add_picked(tab[slot0, 0], row_start(first, 0))
        add_picked(tab[slot0, 1], row_start(first, 1))

        def body(i, carry):
            k = i - phase * n_full
            e = base + k

            @pl.when(i + DEPTH - 1 < 2 * n_full)
            def _():
                tab_copy(i + DEPTH - 1, 0).start()
                tab_copy(i + DEPTH - 1, 1).start()

            slot = lax.rem(i, DEPTH)
            tab_copy(i, 0).wait()
            tx[e] = partial(tab[slot, 0])
            tx_copy(e).start()
            tab_copy(i, 1).wait()
            acc[e] = partial(tab[slot, 1])

            @pl.when(k > 1)
            def _():
                finish(e - 1)

            add_picked(tab[slot, 0], row_start(i, 0))
            add_picked(tab[slot, 1], row_start(i, 1))
            return carry

        lax.fori_loop(first + 1, first + n_full, body, 0)
        finish(last - 1)

    signal_vp(near_sem.at[0])
    run_phase(0)
    pl.semaphore_wait(near_sem.at[0], has_low + has_high)
    signal_vp(near_sem.at[1])
    run_phase(1)
    pl.semaphore_wait(near_sem.at[1], has_low + has_high)
    signal_tp(near_sem.at[2])

    def pick_copy(dz):
        return pltpu.make_async_remote_copy(
            src_ref=picked, dst_ref=picked_rx.at[vp], send_sem=pick_send.at[dz - 1], recv_sem=pick_recv.at[dz - 1],
            device_id=peer_id(dz, 0), device_id_type=MESH,
        )

    for dz in range(1, n_vp):
        pick_copy(dz).start()
    picked_rx[pl.ds(vp, 1)] = picked[...][None]
    for dz in range(1, n_vp):
        pick_copy(dz).wait_recv()
    x2 = picked_rx[0]
    for z in range(1, n_vp):
        x2 = x2 + picked_rx[z]
    stat2_slots[pl.ds(tp, 1)] = stat_row(x2)[None]
    for d in (2, 3, 1):
        stat_copy(stat2_slots, stat2_send, stat2_recv, d).start()
    next_out[...] = norm(
        x2, stat2_slots, stat2_send, stat2_recv, gain2[...].reshape(1, width), bias2[...].reshape(1, width)
    ).astype(jnp.bfloat16)

    def absorb(k, cols):
        e = n_chunks + k
        blocks = cols // LANES
        top = m_run[...]
        for b in range(blocks):
            sl = pl.ds(b * LANES, LANES)
            z = acc[e, :, sl] + (y_rx[k, :, sl] if cols == CHUNK else tail_block(b))
            logits[k, :, sl] = z
            if cols != CHUNK and (b + 1) * LANES > rem:
                z = jnp.where(lane < rem - b * LANES, z, -jnp.inf)
            top = jnp.maximum(top, z)
        total = s_run[...] * jnp.exp(m_run[...] - top)
        for b in range(blocks):
            z = logits[k, :, pl.ds(b * LANES, LANES)]
            if cols != CHUNK and (b + 1) * LANES > rem:
                z = jnp.where(lane < rem - b * LANES, z, -jnp.inf)
            total = total + jnp.exp(z - top)
        m_run[...] = top
        s_run[...] = total

    def absorb_body(k, carry):
        absorb(k, CHUNK)
        tx_copy(k).wait_send()
        tx_copy(n_chunks + k).wait_send()
        return carry

    y_tail_copy().wait_recv()
    absorb(n_full, rem_pad)
    pl.semaphore_wait(near_sem.at[2], 3)
    tx_copy(n_full, rem_pad).wait_send()
    tx_copy(n_chunks + n_full, rem_pad).wait_send()
    y_tail_copy().wait_send()
    all_of(stat_slots, stat_send, 3).wait()
    all_of(stat2_slots, stat2_send, 3).wait()
    for dz in range(1, n_vp):
        pick_copy(dz).wait_send()
    for g, n in groups:
        y_copy(g, n).wait_recv()
        lax.fori_loop(g, g + n, absorb_body, 0)

    m_t = m_run[...].T
    top = jnp.max(m_t, axis=0, keepdims=True)
    tot = jnp.sum(s_run[...].T * jnp.exp(m_t - top), axis=0, keepdims=True)
    lse_slots[pl.ds(my_rank, 1), :, 0:rows] = top[None]
    lse_slots[pl.ds(my_rank, 1), :, rows:LANES] = tot[None]

    def lse_copy(dz, dt, j):
        return pltpu.make_async_remote_copy(
            src_ref=lse_slots.at[my_rank], dst_ref=lse_slots.at[my_rank],
            send_sem=lse_send.at[0], recv_sem=lse_recv.at[0],
            device_id=peer_id(dz, dt), device_id_type=MESH,
        )

    for dz, dt, j in peers:
        lse_copy(dz, dt, j).start()

    for g, n in groups:
        y_copy(g, n).wait_send()
    all_of(lse_slots, lse_recv, len(peers)).wait()
    pairs = lse_slots[:, 0, :]
    top = jnp.max(pairs, axis=0, keepdims=True)
    scaled = pltpu.roll(pairs, rows, axis=1) * jnp.exp(pairs - top)
    tot = jnp.sum(scaled, axis=0, keepdims=True)
    lse_out[...] = jnp.broadcast_to(top + jnp.log(tot), (8, LANES))
    all_of(lse_slots, lse_send, len(peers)).wait()


def finish_kernel(n_full, rem, logits, lse, next_rows, out_hbm, sum_hbm, next_hbm, stage, sums, sem, small_sem):
    rows = stage.shape[0]
    next_copy = pltpu.make_async_copy(next_rows, next_hbm, small_sem.at[0])
    next_copy.start()
    sums[...] = lse[0:1, 0:rows]
    sum_copy = pltpu.make_async_copy(sums, sum_hbm, small_sem.at[1])
    sum_copy.start()
    log_sum = lse[...].T[:rows, 0:1]
    copies = []
    for r in range(rows // 8):
        here = slice(8 * r, 8 * r + 8)
        part = jnp.broadcast_to(log_sum[here], (8, LANES))
        for k in range(n_full + 1):
            cols = CHUNK if k < n_full else rem
            for b in range(0, cols, LANES):
                w = min(LANES, cols - b)
                at = k * CHUNK + b
                stage[here, at:at + w] = logits[k, here, b:b + w] - part[:, :w]
        copy = pltpu.make_async_copy(stage.at[here, :], out_hbm.at[here, :], sem.at[r])
        copy.start()
        copies.append(copy)
    for copy in [next_copy, sum_copy] + copies:
        copy.wait()


def solution(mesh):
    n_vp = mesh.shape["vp"]
    assert mesh.shape["tp"] == 4

    def per_device(hidden, lnf_gain, lnf_bias, emb_table, next_tok, eln_gain, eln_bias):
        rows, width = hidden.shape
        seg = emb_table.shape[0] // 4
        n_full, rem = divmod(seg, CHUNK)
        n_chunks = n_full + 1
        rem_pad = -(-rem // LANES) * LANES
        assert 2 * rows == LANES and n_vp == 4 and rem == 2 * LANES + LANES // 2 and n_full >= 8
        f32, bf16 = jnp.float32, jnp.bfloat16
        dma = pltpu.SemaphoreType.DMA
        hbm = pl.BlockSpec(memory_space=pltpu.HBM)
        vmem = pl.BlockSpec(memory_space=pltpu.VMEM)
        logits, lse, next_rows = pl.pallas_call(
            functools.partial(head_kernel, n_vp, n_full, rem, width),
            out_shape=(
                pltpu.VMEM((n_chunks, rows, CHUNK), f32),
                pltpu.VMEM((8, LANES), f32),
                pltpu.VMEM((rows, width), bf16),
            ),
            in_specs=[hbm] * 7,
            out_specs=(vmem, vmem, vmem),
            scratch_shapes=[
                pltpu.VMEM((rows, width), bf16),
                *[pltpu.VMEM((width,), f32)] * 4,
                pltpu.VMEM((1, rows), jnp.int32),
                pltpu.VMEM((DEPTH, 2, CHUNK, width), bf16),
                pltpu.VMEM((4, rem_pad, width), bf16),
                pltpu.VMEM((rows, width), bf16),
                pltpu.VMEM((rows, width), f32),
                pltpu.VMEM((n_vp, rows, width), f32),
                pltpu.VMEM((2 * n_chunks, rows, CHUNK), f32),
                pltpu.VMEM((2 * n_chunks, rows, CHUNK), f32),
                pltpu.VMEM((2 * n_chunks, rows, CHUNK), f32),
                pltpu.VMEM((n_chunks, rows, CHUNK), f32),
                pltpu.VMEM((rows, LANES), f32),
                pltpu.VMEM((rows, LANES), f32),
                pltpu.VMEM((4, 1, LANES), f32),
                pltpu.VMEM((4, 1, LANES), f32),
                pltpu.VMEM((n_vp * 4, 1, LANES), f32),
                dma((6,)), dma((DEPTH, 2)), dma((4,)),
                dma((1,)), dma((1,)), dma((1,)), dma((1,)),
                dma((2 * n_chunks,)), dma((2 * n_chunks,)),
                dma((n_chunks,)), dma((n_chunks,)),
                dma((n_vp - 1,)), dma((n_vp - 1,)),
                dma((1,)), dma((1,)),
                pltpu.SemaphoreType.REGULAR((3,)),
                pltpu.VMEM((rows + rows // 4, 2 * LANES), f32), pltpu.VMEM((rows + rows // 4, 2 * LANES), f32),
            ],
            compiler_params=pltpu.CompilerParams(
                collective_id=0, has_side_effects=True, vmem_limit_bytes=52 * 1024 * 1024
            ),
            name="head",
        )(
            *[
                pltpu.with_memory_space_constraint(a, pltpu.HBM)
                for a in (hidden, lnf_gain, lnf_bias, emb_table, next_tok.reshape(1, rows), eln_gain, eln_bias)
            ]
        )
        logprobs, log_sum, next_in = pl.pallas_call(
            functools.partial(finish_kernel, n_full, rem),
            out_shape=(
                jax.ShapeDtypeStruct((rows, seg), f32),
                jax.ShapeDtypeStruct((1, rows), f32),
                jax.ShapeDtypeStruct((rows, width), bf16),
            ),
            in_specs=[vmem, vmem, vmem],
            out_specs=(hbm, hbm, hbm),
            scratch_shapes=[pltpu.VMEM((rows, seg), f32), pltpu.VMEM((1, rows), f32), dma((rows // 8,)), dma((2,))],
            compiler_params=pltpu.CompilerParams(vmem_limit_bytes=24 * 1024 * 1024),
            name="finish",
        )(logits, lse, next_rows)
        return logprobs, log_sum.reshape(rows), next_in

    return jax.shard_map(
        per_device,
        mesh=mesh,
        in_specs=(P("dp", "tp"), P("tp"), P("tp"), P("vp", "tp"), P("dp"), P("tp"), P("tp")),
        out_specs=(P("dp", ("vp", "tp")), P("dp"), P("dp", "tp")),
        check_vma=False,
    )
```

```python
import functools

import jax
import jax.numpy as jnp
from jax import lax
from jax.experimental import pallas as pl
from jax.experimental.pallas import tpu as pltpu
from jax.sharding import PartitionSpec as P

NORM_EPS = 1e-5
CHUNK = 2560
LANES = 128
DEPTH = 3
LOWEST = -3.0e38
MESH = pl.DeviceIdType.MESH


def head_kernel(
    n_vp, n_full, rem, width,
    hid_hbm, gain1_hbm, bias1_hbm, tab_hbm, tok_hbm, gain2_hbm, bias2_hbm,
    logits, lse_out, next_out,
    hid, gain1, bias1, gain2, bias2, tok, tab, tab_rem, normed, picked, picked_rx,
    tx, rx, acc, y_rx, m_run, s_run, stat_slots, stat2_slots, lse_slots,
    in_sem, tab_sem, rem_sem, stat_send, stat_recv, stat2_send, stat2_recv,
    tx_send, tx_recv, y_send, y_recv, pick_send, pick_recv, lse_send, lse_recv, near_sem, y_tail, y_tail_rx,
):
    rows = hid.shape[0]
    n_chunks = n_full + 1
    seg = n_full * CHUNK + rem
    rem_pad = tab_rem.shape[1]
    vp = lax.axis_index("vp")
    tp = lax.axis_index("tp")
    chip_y = tp // 2
    core = lax.rem(tp, 2)
    sibling = tp + 1 - 2 * core
    across = lax.rem(tp + 2, 4)
    my_rank = vp * 4 + tp

    peers = []
    for dz in reversed(range(n_vp)):
        for dt in reversed(range(4)):
            if dz or dt:
                peers.append((dz, dt, dz * 4 + dt))

    def peer_id(dz, dt):
        return {"vp": lax.rem(vp + dz, n_vp), "tp": lax.rem(tp + dt, 4)}

    hid_copy = pltpu.make_async_copy(hid_hbm, hid, in_sem.at[0])
    hid_copy.start()

    has_low = jnp.where(vp > 0, 1, 0)
    has_high = jnp.where(vp < n_vp - 1, 1, 0)

    def signal_vp(sem):
        @pl.when(vp > 0)
        def _():
            pl.semaphore_signal(sem, inc=1, device_id={"vp": vp - 1}, device_id_type=MESH)

        @pl.when(vp < n_vp - 1)
        def _():
            pl.semaphore_signal(sem, inc=1, device_id={"vp": vp + 1}, device_id_type=MESH)

    def signal_tp(sem):
        for dt in (2, 3, 1):
            pl.semaphore_signal(sem, inc=1, device_id=peer_id(0, dt), device_id_type=MESH)

    barrier = pltpu.get_barrier_semaphore()
    signal_tp(barrier)
    signal_vp(barrier)

    def seg_start(phase, which):
        y = chip_y + (1 - phase) * (1 - 2 * chip_y)
        c = core + (1 - which) * (1 - 2 * core)
        return (y * 2 + c) * seg

    def row_start(i, which):
        phase = jnp.where(i >= n_full, 1, 0)
        k = i - phase * n_full
        return pl.multiple_of(seg_start(phase, which) + k * CHUNK, 64)

    def tab_copy(i, which):
        slot = lax.rem(i, DEPTH)
        return pltpu.make_async_copy(
            tab_hbm.at[pl.ds(row_start(i, which), CHUNK), :], tab.at[slot, which], tab_sem.at[slot, which]
        )

    def rem_start(phase, which):
        return pl.multiple_of(seg_start(phase, which) + n_full * CHUNK, 64)

    def rem_copy(phase, which):
        return pltpu.make_async_copy(
            tab_hbm.at[pl.ds(rem_start(phase, which), rem), :],
            tab_rem.at[phase * 2 + which, pl.ds(0, rem), :],
            rem_sem.at[phase * 2 + which],
        )

    small = [
        pltpu.make_async_copy(gain1_hbm, gain1, in_sem.at[1]),
        pltpu.make_async_copy(bias1_hbm, bias1, in_sem.at[2]),
        pltpu.make_async_copy(gain2_hbm, gain2, in_sem.at[3]),
        pltpu.make_async_copy(bias2_hbm, bias2, in_sem.at[4]),
        pltpu.make_async_copy(tok_hbm, tok, in_sem.at[5]),
    ]

    picked[...] = jnp.zeros_like(picked)
    m_run[...] = jnp.full_like(m_run, LOWEST)
    s_run[...] = jnp.zeros_like(s_run)
    tab_rem[:, rem:, :] = jnp.zeros((4, rem_pad - rem, width), jnp.bfloat16)

    lane = lax.broadcasted_iota(jnp.int32, (rows, LANES), 1)

    def stat_row(x):
        s1 = jnp.sum(x, axis=1, keepdims=True)
        s2 = jnp.sum(x * x, axis=1, keepdims=True)
        return jnp.broadcast_to(jnp.concatenate([s1, s2], axis=0), (LANES, LANES)).T[0:1, :]

    def stat_copy(slots, send, recv, d):
        return pltpu.make_async_remote_copy(
            src_ref=slots.at[tp], dst_ref=slots.at[tp], send_sem=send.at[0], recv_sem=recv.at[0],
            device_id=peer_id(0, d), device_id_type=MESH,
        )

    def all_of(slots, sem, count):
        return pltpu.make_async_copy(slots.at[pl.ds(0, count)], slots.at[pl.ds(0, count)], sem.at[0])

    def norm(x, slots, send, recv, gain, bias):
        all_of(slots, recv, 3).wait()
        total = (slots[0] + slots[1]) + (slots[2] + slots[3])
        full_width = 4.0 * width
        total = jnp.broadcast_to(total, (8, LANES)) / full_width
        mean = total
        var = pltpu.roll(total, rows, axis=1) - mean * mean
        inv = lax.rsqrt(var + NORM_EPS)
        row = lax.broadcasted_iota(jnp.int32, (8, LANES), 0)
        back = jnp.where(row == 0, mean, inv).T
        mean_c = back[:rows, 0:1]
        inv_c = back[:rows, 1:2]
        return (x - mean_c) * inv_c * gain + bias

    hid_copy.wait()
    x1 = hid[...].astype(jnp.float32)
    stat_slots[pl.ds(tp, 1)] = stat_row(x1)[None]
    pl.semaphore_wait(barrier, 3 + has_low + has_high)
    for d in (2, 3, 1):
        stat_copy(stat_slots, stat_send, stat_recv, d).start()
    for copy in small:
        copy.start()
    for which in range(2):
        rem_copy(0, which).start()
    for i in range(min(DEPTH - 1, 2 * n_full)):
        for which in range(2):
            tab_copy(i, which).start()
    for which in range(2):
        rem_copy(1, which).start()
    for copy in small:
        copy.wait()
    normed[...] = norm(
        x1, stat_slots, stat_send, stat_recv, gain1[...].reshape(1, width), bias1[...].reshape(1, width)
    ).astype(jnp.bfloat16)

    def tx_copy(e, cols=None):
        view = (lambda r: r.at[e]) if cols is None else (lambda r: r.at[e, :, pl.ds(0, cols)])
        return pltpu.make_async_remote_copy(
            src_ref=view(tx), dst_ref=view(rx), send_sem=tx_send.at[e], recv_sem=tx_recv.at[e],
            device_id={"tp": sibling}, device_id_type=MESH,
        )

    cut = CHUNK // 4 * 3

    def y_copy(e):
        return pltpu.make_async_remote_copy(
            src_ref=acc.at[e], dst_ref=y_rx.at[e], send_sem=y_send.at[e], recv_sem=y_recv.at[e],
            device_id={"tp": across}, device_id_type=MESH,
        )

    def y_last(part):
        at = pl.ds(0, cut) if part == 0 else pl.ds(cut, CHUNK - cut)
        sem = (n_full - 1) if part == 0 else n_chunks
        return pltpu.make_async_remote_copy(
            src_ref=acc.at[n_full - 1, :, at], dst_ref=y_rx.at[n_full - 1, :, at],
            send_sem=y_send.at[sem], recv_sem=y_recv.at[sem],
            device_id={"tp": across}, device_id_type=MESH,
        )

    half = LANES // 2
    whole = rem - half

    def y_tail_copy():
        return pltpu.make_async_remote_copy(
            src_ref=y_tail, dst_ref=y_tail_rx, send_sem=y_send.at[n_full], recv_sem=y_recv.at[n_full],
            device_id={"tp": across}, device_id_type=MESH,
        )

    def pack_tail(block):
        y_tail[0:rows, :] = block[:, 0:whole]
        low = block[0:rows // 2, whole:whole + LANES]
        high = pltpu.roll(block[rows // 2:rows, whole:whole + LANES], half, axis=1)
        both = jnp.where(lane[0:rows // 2] < half, low, high)
        y_tail[rows:rows + rows // 4, 0:LANES] = both[0:rows // 4]
        y_tail[rows:rows + rows // 4, LANES:2 * LANES] = both[rows // 4:rows // 2]

    def tail_block(b):
        if (b + 1) * LANES <= whole:
            return y_tail_rx[0:rows, b * LANES:(b + 1) * LANES]
        both = jnp.concatenate(
            [y_tail_rx[rows:rows + rows // 4, 0:LANES], y_tail_rx[rows:rows + rows // 4, LANES:2 * LANES]], axis=0
        )
        return jnp.concatenate([both, pltpu.roll(both, half, axis=1)], axis=0)

    def partial(block):
        return lax.dot_general(
            normed[...], block, (((1,), (1,)), ((), ())), preferred_element_type=jnp.float32
        )

    tok_col = jnp.broadcast_to(tok[...], (8, rows)).T[:, 0:1]
    tok_local = tok_col - vp * (4 * seg)

    def add_picked(block, start):
        n = block.shape[0]
        at = lax.broadcasted_iota(jnp.int32, (rows, n), 1)
        hot = jnp.where(at == tok_local - start, 1.0, 0.0).astype(jnp.bfloat16)
        picked[...] += lax.dot_general(
            hot, block, (((1,), (0,)), ((), ())), preferred_element_type=jnp.float32
        )

    def add_picked_rem(phase, which):
        at = lax.broadcasted_iota(jnp.int32, (rows, rem_pad), 1)
        hit = (at == tok_local - rem_start(phase, which)) & (at < rem)
        hot = jnp.where(hit, 1.0, 0.0).astype(jnp.bfloat16)
        picked[...] += lax.dot_general(
            hot, tab_rem[phase * 2 + which], (((1,), (0,)), ((), ())), preferred_element_type=jnp.float32
        )

    def run_phase(phase):
        base = phase * n_chunks

        last = base + n_full
        first = phase * n_full
        slot0 = first % DEPTH
        rem_copy(phase, 0).wait()
        tx[last, :, 0:rem_pad] = partial(tab_rem[phase * 2])
        tx_copy(last, rem_pad).start()
        tab_copy(first, 0).wait()
        tx[base] = partial(tab[slot0, 0])
        tx_copy(base).start()
        rem_copy(phase, 1).wait()
        mine = partial(tab_rem[phase * 2 + 1])
        acc[last, :, 0:rem_pad] = mine
        tab_copy(first, 1).wait()
        acc[base] = partial(tab[slot0, 1])
        tx_copy(last, rem_pad).wait_recv()
        if phase == 0:
            pack_tail(acc[last, :, 0:rem_pad] + rx[last, :, 0:rem_pad])
            y_tail_copy().start()
        else:
            acc[last, :, 0:rem_pad] = acc[last, :, 0:rem_pad] + rx[last, :, 0:rem_pad]

        def finish(e, end=False):
            tx_copy(e).wait_recv()
            acc[e] = acc[e] + rx[e]
            if phase == 0 and not end:
                y_copy(e).start()
            elif phase == 0:
                y_last(0).start()
                y_last(1).start()

        tab_copy(first + DEPTH - 1, 0).start()
        tab_copy(first + DEPTH - 1, 1).start()
        add_picked_rem(phase, 0)
        add_picked_rem(phase, 1)
        finish(base)
        add_picked(tab[slot0, 0], row_start(first, 0))
        add_picked(tab[slot0, 1], row_start(first, 1))

        def body(i, carry):
            k = i - phase * n_full
            e = base + k

            @pl.when(i + DEPTH - 1 < 2 * n_full)
            def _():
                tab_copy(i + DEPTH - 1, 0).start()
                tab_copy(i + DEPTH - 1, 1).start()

            slot = lax.rem(i, DEPTH)
            tab_copy(i, 0).wait()
            tx[e] = partial(tab[slot, 0])
            tx_copy(e).start()
            tab_copy(i, 1).wait()
            acc[e] = partial(tab[slot, 1])

            @pl.when(k > 1)
            def _():
                finish(e - 1)

            add_picked(tab[slot, 0], row_start(i, 0))
            add_picked(tab[slot, 1], row_start(i, 1))
            return carry

        lax.fori_loop(first + 1, first + n_full, body, 0)
        finish(last - 1, end=True)

    signal_vp(near_sem.at[0])
    run_phase(0)
    pl.semaphore_wait(near_sem.at[0], has_low + has_high)
    signal_vp(near_sem.at[1])
    run_phase(1)
    pl.semaphore_wait(near_sem.at[1], has_low + has_high)
    signal_tp(near_sem.at[2])

    def pick_copy(dz):
        return pltpu.make_async_remote_copy(
            src_ref=picked, dst_ref=picked_rx.at[vp], send_sem=pick_send.at[dz - 1], recv_sem=pick_recv.at[dz - 1],
            device_id=peer_id(dz, 0), device_id_type=MESH,
        )

    for dz in range(1, n_vp):
        pick_copy(dz).start()
    picked_rx[pl.ds(vp, 1)] = picked[...][None]
    for dz in range(1, n_vp):
        pick_copy(dz).wait_recv()
    x2 = picked_rx[0]
    for z in range(1, n_vp):
        x2 = x2 + picked_rx[z]
    stat2_slots[pl.ds(tp, 1)] = stat_row(x2)[None]
    for d in (2, 3, 1):
        stat_copy(stat2_slots, stat2_send, stat2_recv, d).start()
    next_out[...] = norm(
        x2, stat2_slots, stat2_send, stat2_recv, gain2[...].reshape(1, width), bias2[...].reshape(1, width)
    ).astype(jnp.bfloat16)

    def absorb(k, cols, skip=0):
        e = n_chunks + k
        blocks = range(skip // LANES, cols // LANES)
        top = m_run[...]
        for b in blocks:
            sl = pl.ds(b * LANES, LANES)
            z = acc[e, :, sl] + (tail_block(b) if k is n_full else y_rx[k, :, sl])
            logits[k, :, sl] = z
            if k is n_full and (b + 1) * LANES > rem:
                z = jnp.where(lane < rem - b * LANES, z, -jnp.inf)
            top = jnp.maximum(top, z)
        total = s_run[...] * jnp.exp(m_run[...] - top)
        for b in blocks:
            z = logits[k, :, pl.ds(b * LANES, LANES)]
            if k is n_full and (b + 1) * LANES > rem:
                z = jnp.where(lane < rem - b * LANES, z, -jnp.inf)
            total = total + jnp.exp(z - top)
        m_run[...] = top
        s_run[...] = total

    def absorb_body(k, carry):
        y_copy(k).wait_recv()
        absorb(k, CHUNK)
        tx_copy(k).wait_send()
        tx_copy(n_chunks + k).wait_send()
        return carry

    y_tail_copy().wait_recv()
    absorb(n_full, rem_pad)
    pl.semaphore_wait(near_sem.at[2], 3)
    tx_copy(n_full, rem_pad).wait_send()
    tx_copy(n_chunks + n_full, rem_pad).wait_send()
    y_tail_copy().wait_send()
    all_of(stat_slots, stat_send, 3).wait()
    all_of(stat2_slots, stat2_send, 3).wait()
    for dz in range(1, n_vp):
        pick_copy(dz).wait_send()
    lax.fori_loop(0, n_full - 1, absorb_body, 0)
    tx_copy(n_full - 1).wait_send()
    tx_copy(n_chunks + n_full - 1).wait_send()
    y_last(0).wait_recv()
    absorb(n_full - 1, cut)
    y_last(1).wait_recv()
    absorb(n_full - 1, CHUNK, cut)

    m_t = m_run[...].T
    top = jnp.max(m_t, axis=0, keepdims=True)
    tot = jnp.sum(s_run[...].T * jnp.exp(m_t - top), axis=0, keepdims=True)
    lse_slots[pl.ds(my_rank, 1), :, 0:rows] = top[None]
    lse_slots[pl.ds(my_rank, 1), :, rows:LANES] = tot[None]

    def lse_copy(dz, dt, j):
        return pltpu.make_async_remote_copy(
            src_ref=lse_slots.at[my_rank], dst_ref=lse_slots.at[my_rank],
            send_sem=lse_send.at[0], recv_sem=lse_recv.at[0],
            device_id=peer_id(dz, dt), device_id_type=MESH,
        )

    for dz, dt, j in peers:
        lse_copy(dz, dt, j).start()

    for e in range(n_full - 1):
        y_copy(e).wait_send()
    y_last(0).wait_send()
    y_last(1).wait_send()
    all_of(lse_slots, lse_recv, len(peers)).wait()
    pairs = lse_slots[:, 0, :]
    top = jnp.max(pairs, axis=0, keepdims=True)
    scaled = pltpu.roll(pairs, rows, axis=1) * jnp.exp(pairs - top)
    tot = jnp.sum(scaled, axis=0, keepdims=True)
    lse_out[...] = jnp.broadcast_to(top + jnp.log(tot), (8, LANES))
    all_of(lse_slots, lse_send, len(peers)).wait()


def finish_kernel(n_full, rem, logits, lse, next_rows, out_hbm, sum_hbm, next_hbm, stage, sums, sem, small_sem):
    rows = stage.shape[0]
    next_copy = pltpu.make_async_copy(next_rows, next_hbm, small_sem.at[0])
    next_copy.start()
    sums[...] = lse[0:1, 0:rows]
    sum_copy = pltpu.make_async_copy(sums, sum_hbm, small_sem.at[1])
    sum_copy.start()
    log_sum = lse[...].T[:rows, 0:1]
    copies = []
    for r in range(rows // 8):
        here = slice(8 * r, 8 * r + 8)
        part = jnp.broadcast_to(log_sum[here], (8, LANES))
        for k in range(n_full + 1):
            cols = CHUNK if k < n_full else rem
            for b in range(0, cols, LANES):
                w = min(LANES, cols - b)
                at = k * CHUNK + b
                stage[here, at:at + w] = logits[k, here, b:b + w] - part[:, :w]
        copy = pltpu.make_async_copy(stage.at[here, :], out_hbm.at[here, :], sem.at[r])
        copy.start()
        copies.append(copy)
    for copy in [next_copy, sum_copy] + copies:
        copy.wait()


def solution(mesh):
    n_vp = mesh.shape["vp"]
    assert mesh.shape["tp"] == 4

    def per_device(hidden, lnf_gain, lnf_bias, emb_table, next_tok, eln_gain, eln_bias):
        rows, width = hidden.shape
        seg = emb_table.shape[0] // 4
        n_full, rem = divmod(seg, CHUNK)
        n_chunks = n_full + 1
        rem_pad = -(-rem // LANES) * LANES
        assert 2 * rows == LANES and n_vp == 4 and rem == 2 * LANES + LANES // 2 and n_full > DEPTH
        f32, bf16 = jnp.float32, jnp.bfloat16
        dma = pltpu.SemaphoreType.DMA
        hbm = pl.BlockSpec(memory_space=pltpu.HBM)
        vmem = pl.BlockSpec(memory_space=pltpu.VMEM)
        logits, lse, next_rows = pl.pallas_call(
            functools.partial(head_kernel, n_vp, n_full, rem, width),
            out_shape=(
                pltpu.VMEM((n_chunks, rows, CHUNK), f32),
                pltpu.VMEM((8, LANES), f32),
                pltpu.VMEM((rows, width), bf16),
            ),
            in_specs=[hbm] * 7,
            out_specs=(vmem, vmem, vmem),
            scratch_shapes=[
                pltpu.VMEM((rows, width), bf16),
                *[pltpu.VMEM((width,), f32)] * 4,
                pltpu.VMEM((1, rows), jnp.int32),
                pltpu.VMEM((DEPTH, 2, CHUNK, width), bf16),
                pltpu.VMEM((4, rem_pad, width), bf16),
                pltpu.VMEM((rows, width), bf16),
                pltpu.VMEM((rows, width), f32),
                pltpu.VMEM((n_vp, rows, width), f32),
                pltpu.VMEM((2 * n_chunks, rows, CHUNK), f32),
                pltpu.VMEM((2 * n_chunks, rows, CHUNK), f32),
                pltpu.VMEM((2 * n_chunks, rows, CHUNK), f32),
                pltpu.VMEM((n_chunks, rows, CHUNK), f32),
                pltpu.VMEM((rows, LANES), f32),
                pltpu.VMEM((rows, LANES), f32),
                pltpu.VMEM((4, 1, LANES), f32),
                pltpu.VMEM((4, 1, LANES), f32),
                pltpu.VMEM((n_vp * 4, 1, LANES), f32),
                dma((6,)), dma((DEPTH, 2)), dma((4,)),
                dma((1,)), dma((1,)), dma((1,)), dma((1,)),
                dma((2 * n_chunks,)), dma((2 * n_chunks,)),
                dma((n_chunks + 1,)), dma((n_chunks + 1,)),
                dma((n_vp - 1,)), dma((n_vp - 1,)),
                dma((1,)), dma((1,)),
                pltpu.SemaphoreType.REGULAR((3,)),
                pltpu.VMEM((rows + rows // 4, 2 * LANES), f32), pltpu.VMEM((rows + rows // 4, 2 * LANES), f32),
            ],
            compiler_params=pltpu.CompilerParams(
                collective_id=0, has_side_effects=True, vmem_limit_bytes=52 * 1024 * 1024
            ),
            name="head",
        )(
            *[
                pltpu.with_memory_space_constraint(a, pltpu.HBM)
                for a in (hidden, lnf_gain, lnf_bias, emb_table, next_tok.reshape(1, rows), eln_gain, eln_bias)
            ]
        )
        logprobs, log_sum, next_in = pl.pallas_call(
            functools.partial(finish_kernel, n_full, rem),
            out_shape=(
                jax.ShapeDtypeStruct((rows, seg), f32),
                jax.ShapeDtypeStruct((1, rows), f32),
                jax.ShapeDtypeStruct((rows, width), bf16),
            ),
            in_specs=[vmem, vmem, vmem],
            out_specs=(hbm, hbm, hbm),
            scratch_shapes=[pltpu.VMEM((rows, seg), f32), pltpu.VMEM((1, rows), f32), dma((rows // 8,)), dma((2,))],
            compiler_params=pltpu.CompilerParams(vmem_limit_bytes=24 * 1024 * 1024),
            name="finish",
        )(logits, lse, next_rows)
        return logprobs, log_sum.reshape(rows), next_in

    return jax.shard_map(
        per_device,
        mesh=mesh,
        in_specs=(P("dp", "tp"), P("tp"), P("tp"), P("vp", "tp"), P("dp"), P("tp"), P("tp")),
        out_specs=(P("dp", ("vp", "tp")), P("dp"), P("dp", "tp")),
        check_vma=False,
    )
```

```python
import functools

import jax
import jax.numpy as jnp
from jax import lax
from jax.experimental import pallas as pl
from jax.experimental.pallas import tpu as pltpu
from jax.sharding import PartitionSpec as P

NORM_EPS = 1e-5
CHUNK = 1536
LANES = 128
DEPTH = 3
LOWEST = -3.0e38
MESH = pl.DeviceIdType.MESH


def head_kernel(
    n_vp, n_full, rem, width,
    hid_hbm, gain1_hbm, bias1_hbm, tab_hbm, tok_hbm, gain2_hbm, bias2_hbm,
    logits, lse_out, next_out,
    hid, gain1, bias1, gain2, bias2, tok, tab, tab_rem, normed, picked, picked_rx,
    tx, rx, acc, y_rx, m_run, s_run, stat_slots, stat2_slots, lse_slots,
    in_sem, tab_sem, rem_sem, stat_send, stat_recv, stat2_send, stat2_recv,
    tx_send, tx_recv, y_send, y_recv, pick_send, pick_recv, lse_send, lse_recv, near_sem, y_tail, y_tail_rx,
):
    rows = hid.shape[0]
    n_chunks = n_full + 1
    seg = n_full * CHUNK + rem
    rem_pad = tab_rem.shape[1]
    vp = lax.axis_index("vp")
    tp = lax.axis_index("tp")
    chip_y = tp // 2
    core = lax.rem(tp, 2)
    sibling = tp + 1 - 2 * core
    across = lax.rem(tp + 2, 4)
    my_rank = vp * 4 + tp

    peers = []
    for dz in reversed(range(n_vp)):
        for dt in reversed(range(4)):
            if dz or dt:
                peers.append((dz, dt, dz * 4 + dt))

    def peer_id(dz, dt):
        return {"vp": lax.rem(vp + dz, n_vp), "tp": lax.rem(tp + dt, 4)}

    hid_copy = pltpu.make_async_copy(hid_hbm, hid, in_sem.at[0])
    hid_copy.start()

    has_low = jnp.where(vp > 0, 1, 0)
    has_high = jnp.where(vp < n_vp - 1, 1, 0)

    def signal_vp(sem):
        @pl.when(vp > 0)
        def _():
            pl.semaphore_signal(sem, inc=1, device_id={"vp": vp - 1}, device_id_type=MESH)

        @pl.when(vp < n_vp - 1)
        def _():
            pl.semaphore_signal(sem, inc=1, device_id={"vp": vp + 1}, device_id_type=MESH)

    def signal_tp(sem):
        for dt in (2, 3, 1):
            pl.semaphore_signal(sem, inc=1, device_id=peer_id(0, dt), device_id_type=MESH)

    barrier = pltpu.get_barrier_semaphore()
    signal_tp(barrier)
    signal_vp(barrier)

    def seg_start(phase, which):
        y = chip_y + (1 - phase) * (1 - 2 * chip_y)
        c = core + (1 - which) * (1 - 2 * core)
        return (y * 2 + c) * seg

    def row_start(i, which):
        phase = jnp.where(i >= n_full, 1, 0)
        k = i - phase * n_full
        return pl.multiple_of(seg_start(phase, which) + k * CHUNK, 64)

    def tab_copy(i, which):
        slot = lax.rem(i, DEPTH)
        return pltpu.make_async_copy(
            tab_hbm.at[pl.ds(row_start(i, which), CHUNK), :], tab.at[slot, which], tab_sem.at[slot, which]
        )

    def rem_start(phase, which):
        return pl.multiple_of(seg_start(phase, which) + n_full * CHUNK, 64)

    def rem_copy(phase, which):
        return pltpu.make_async_copy(
            tab_hbm.at[pl.ds(rem_start(phase, which), rem), :],
            tab_rem.at[phase * 2 + which, pl.ds(0, rem), :],
            rem_sem.at[phase * 2 + which],
        )

    small = [
        pltpu.make_async_copy(gain1_hbm, gain1, in_sem.at[1]),
        pltpu.make_async_copy(bias1_hbm, bias1, in_sem.at[2]),
        pltpu.make_async_copy(gain2_hbm, gain2, in_sem.at[3]),
        pltpu.make_async_copy(bias2_hbm, bias2, in_sem.at[4]),
        pltpu.make_async_copy(tok_hbm, tok, in_sem.at[5]),
    ]

    picked[...] = jnp.zeros_like(picked)
    m_run[...] = jnp.full_like(m_run, LOWEST)
    s_run[...] = jnp.zeros_like(s_run)
    tab_rem[:, rem:, :] = jnp.zeros((4, rem_pad - rem, width), jnp.bfloat16)

    lane = lax.broadcasted_iota(jnp.int32, (rows, LANES), 1)

    def stat_row(x):
        s1 = jnp.sum(x, axis=1, keepdims=True)
        s2 = jnp.sum(x * x, axis=1, keepdims=True)
        return jnp.broadcast_to(jnp.concatenate([s1, s2], axis=0), (LANES, LANES)).T[0:1, :]

    def stat_copy(slots, send, recv, d):
        return pltpu.make_async_remote_copy(
            src_ref=slots.at[tp], dst_ref=slots.at[tp], send_sem=send.at[0], recv_sem=recv.at[0],
            device_id=peer_id(0, d), device_id_type=MESH,
        )

    def all_of(slots, sem, count):
        return pltpu.make_async_copy(slots.at[pl.ds(0, count)], slots.at[pl.ds(0, count)], sem.at[0])

    def norm(x, slots, send, recv, gain, bias):
        all_of(slots, recv, 3).wait()
        total = (slots[0] + slots[1]) + (slots[2] + slots[3])
        full_width = 4.0 * width
        total = jnp.broadcast_to(total, (8, LANES)) / full_width
        mean = total
        var = pltpu.roll(total, rows, axis=1) - mean * mean
        inv = lax.rsqrt(var + NORM_EPS)
        row = lax.broadcasted_iota(jnp.int32, (8, LANES), 0)
        back = jnp.where(row == 0, mean, inv).T
        mean_c = back[:rows, 0:1]
        inv_c = back[:rows, 1:2]
        return (x - mean_c) * inv_c * gain + bias

    hid_copy.wait()
    x1 = hid[...].astype(jnp.float32)
    stat_slots[pl.ds(tp, 1)] = stat_row(x1)[None]
    pl.semaphore_wait(barrier, 3 + has_low + has_high)
    for d in (2, 3, 1):
        stat_copy(stat_slots, stat_send, stat_recv, d).start()
    for copy in small:
        copy.start()
    for which in range(2):
        rem_copy(0, which).start()
    for i in range(min(DEPTH - 1, 2 * n_full)):
        for which in range(2):
            tab_copy(i, which).start()
    for which in range(2):
        rem_copy(1, which).start()
    for copy in small:
        copy.wait()
    normed[...] = norm(
        x1, stat_slots, stat_send, stat_recv, gain1[...].reshape(1, width), bias1[...].reshape(1, width)
    ).astype(jnp.bfloat16)

    def tx_copy(e, cols=None):
        view = (lambda r: r.at[e]) if cols is None else (lambda r: r.at[e, :, pl.ds(0, cols)])
        return pltpu.make_async_remote_copy(
            src_ref=view(tx), dst_ref=view(rx), send_sem=tx_send.at[e], recv_sem=tx_recv.at[e],
            device_id={"tp": sibling}, device_id_type=MESH,
        )

    cut = CHUNK // 4 * 3

    def y_copy(e):
        return pltpu.make_async_remote_copy(
            src_ref=acc.at[e], dst_ref=y_rx.at[e], send_sem=y_send.at[e], recv_sem=y_recv.at[e],
            device_id={"tp": across}, device_id_type=MESH,
        )

    def y_last(part):
        at = pl.ds(0, cut) if part == 0 else pl.ds(cut, CHUNK - cut)
        sem = (n_full - 1) if part == 0 else n_chunks
        return pltpu.make_async_remote_copy(
            src_ref=acc.at[n_full - 1, :, at], dst_ref=y_rx.at[n_full - 1, :, at],
            send_sem=y_send.at[sem], recv_sem=y_recv.at[sem],
            device_id={"tp": across}, device_id_type=MESH,
        )

    half = LANES // 2
    whole = rem - half

    def y_tail_copy():
        return pltpu.make_async_remote_copy(
            src_ref=y_tail, dst_ref=y_tail_rx, send_sem=y_send.at[n_full], recv_sem=y_recv.at[n_full],
            device_id={"tp": across}, device_id_type=MESH,
        )

    def pack_tail(block):
        y_tail[0:rows, :] = block[:, 0:whole]
        low = block[0:rows // 2, whole:whole + LANES]
        high = pltpu.roll(block[rows // 2:rows, whole:whole + LANES], half, axis=1)
        both = jnp.where(lane[0:rows // 2] < half, low, high)
        y_tail[rows:rows + rows // 4, 0:LANES] = both[0:rows // 4]
        y_tail[rows:rows + rows // 4, LANES:2 * LANES] = both[rows // 4:rows // 2]

    def tail_block(b):
        if (b + 1) * LANES <= whole:
            return y_tail_rx[0:rows, b * LANES:(b + 1) * LANES]
        both = jnp.concatenate(
            [y_tail_rx[rows:rows + rows // 4, 0:LANES], y_tail_rx[rows:rows + rows // 4, LANES:2 * LANES]], axis=0
        )
        return jnp.concatenate([both, pltpu.roll(both, half, axis=1)], axis=0)

    def partial(block):
        return lax.dot_general(
            normed[...], block, (((1,), (1,)), ((), ())), preferred_element_type=jnp.float32
        )

    tok_col = jnp.broadcast_to(tok[...], (8, rows)).T[:, 0:1]
    tok_local = tok_col - vp * (4 * seg)

    def add_picked(block, start):
        n = block.shape[0]
        at = lax.broadcasted_iota(jnp.int32, (rows, n), 1)
        hot = jnp.where(at == tok_local - start, 1.0, 0.0).astype(jnp.bfloat16)
        picked[...] += lax.dot_general(
            hot, block, (((1,), (0,)), ((), ())), preferred_element_type=jnp.float32
        )

    def add_picked_rem(phase, which):
        at = lax.broadcasted_iota(jnp.int32, (rows, rem_pad), 1)
        hit = (at == tok_local - rem_start(phase, which)) & (at < rem)
        hot = jnp.where(hit, 1.0, 0.0).astype(jnp.bfloat16)
        picked[...] += lax.dot_general(
            hot, tab_rem[phase * 2 + which], (((1,), (0,)), ((), ())), preferred_element_type=jnp.float32
        )

    def run_phase(phase):
        base = phase * n_chunks

        last = base + n_full
        first = phase * n_full
        slot0 = first % DEPTH
        rem_copy(phase, 0).wait()
        tx[last, :, 0:rem_pad] = partial(tab_rem[phase * 2])
        tx_copy(last, rem_pad).start()
        tab_copy(first, 0).wait()
        tx[base] = partial(tab[slot0, 0])
        tx_copy(base).start()
        rem_copy(phase, 1).wait()
        mine = partial(tab_rem[phase * 2 + 1])
        acc[last, :, 0:rem_pad] = mine
        tab_copy(first, 1).wait()
        acc[base] = partial(tab[slot0, 1])
        tx_copy(last, rem_pad).wait_recv()
        if phase == 0:
            pack_tail(acc[last, :, 0:rem_pad] + rx[last, :, 0:rem_pad])
            y_tail_copy().start()
        else:
            acc[last, :, 0:rem_pad] = acc[last, :, 0:rem_pad] + rx[last, :, 0:rem_pad]

        def finish(e, end=False):
            tx_copy(e).wait_recv()
            acc[e] = acc[e] + rx[e]
            if phase == 0 and not end:
                y_copy(e).start()
            elif phase == 0:
                y_last(0).start()
                y_last(1).start()

        tab_copy(first + DEPTH - 1, 0).start()
        tab_copy(first + DEPTH - 1, 1).start()
        add_picked_rem(phase, 0)
        add_picked_rem(phase, 1)
        finish(base)
        add_picked(tab[slot0, 0], row_start(first, 0))
        add_picked(tab[slot0, 1], row_start(first, 1))

        def body(i, carry):
            k = i - phase * n_full
            e = base + k

            @pl.when(i + DEPTH - 1 < 2 * n_full)
            def _():
                tab_copy(i + DEPTH - 1, 0).start()
                tab_copy(i + DEPTH - 1, 1).start()

            slot = lax.rem(i, DEPTH)
            tab_copy(i, 0).wait()
            tx[e] = partial(tab[slot, 0])
            tx_copy(e).start()
            tab_copy(i, 1).wait()
            acc[e] = partial(tab[slot, 1])

            @pl.when(k > 1)
            def _():
                finish(e - 1)

            add_picked(tab[slot, 0], row_start(i, 0))
            add_picked(tab[slot, 1], row_start(i, 1))
            return carry

        lax.fori_loop(first + 1, first + n_full, body, 0)
        finish(last - 1, end=True)

    signal_vp(near_sem.at[0])
    run_phase(0)
    pl.semaphore_wait(near_sem.at[0], has_low + has_high)
    signal_vp(near_sem.at[1])
    run_phase(1)
    pl.semaphore_wait(near_sem.at[1], has_low + has_high)
    signal_tp(near_sem.at[2])

    def pick_copy(dz):
        return pltpu.make_async_remote_copy(
            src_ref=picked, dst_ref=picked_rx.at[vp], send_sem=pick_send.at[dz - 1], recv_sem=pick_recv.at[dz - 1],
            device_id=peer_id(dz, 0), device_id_type=MESH,
        )

    for dz in range(1, n_vp):
        pick_copy(dz).start()
    picked_rx[pl.ds(vp, 1)] = picked[...][None]
    for dz in range(1, n_vp):
        pick_copy(dz).wait_recv()
    x2 = picked_rx[0]
    for z in range(1, n_vp):
        x2 = x2 + picked_rx[z]
    stat2_slots[pl.ds(tp, 1)] = stat_row(x2)[None]
    for d in (2, 3, 1):
        stat_copy(stat2_slots, stat2_send, stat2_recv, d).start()
    next_out[...] = norm(
        x2, stat2_slots, stat2_send, stat2_recv, gain2[...].reshape(1, width), bias2[...].reshape(1, width)
    ).astype(jnp.bfloat16)

    def absorb(k, cols, skip=0):
        e = n_chunks + k
        blocks = range(skip // LANES, cols // LANES)
        top = m_run[...]
        for b in blocks:
            sl = pl.ds(b * LANES, LANES)
            z = acc[e, :, sl] + (tail_block(b) if k is n_full else y_rx[k, :, sl])
            logits[k, :, sl] = z
            if k is n_full and (b + 1) * LANES > rem:
                z = jnp.where(lane < rem - b * LANES, z, -jnp.inf)
            top = jnp.maximum(top, z)
        total = s_run[...] * jnp.exp(m_run[...] - top)
        for b in blocks:
            z = logits[k, :, pl.ds(b * LANES, LANES)]
            if k is n_full and (b + 1) * LANES > rem:
                z = jnp.where(lane < rem - b * LANES, z, -jnp.inf)
            total = total + jnp.exp(z - top)
        m_run[...] = top
        s_run[...] = total

    def absorb_body(k, carry):
        y_copy(k).wait_recv()
        absorb(k, CHUNK)
        tx_copy(k).wait_send()
        tx_copy(n_chunks + k).wait_send()
        return carry

    y_tail_copy().wait_recv()
    absorb(n_full, rem_pad)
    pl.semaphore_wait(near_sem.at[2], 3)
    tx_copy(n_full, rem_pad).wait_send()
    tx_copy(n_chunks + n_full, rem_pad).wait_send()
    y_tail_copy().wait_send()
    all_of(stat_slots, stat_send, 3).wait()
    all_of(stat2_slots, stat2_send, 3).wait()
    for dz in range(1, n_vp):
        pick_copy(dz).wait_send()
    lax.fori_loop(0, n_full - 1, absorb_body, 0)
    tx_copy(n_full - 1).wait_send()
    tx_copy(n_chunks + n_full - 1).wait_send()
    y_last(0).wait_recv()
    absorb(n_full - 1, cut)
    y_last(1).wait_recv()
    absorb(n_full - 1, CHUNK, cut)

    m_t = m_run[...].T
    top = jnp.max(m_t, axis=0, keepdims=True)
    tot = jnp.sum(s_run[...].T * jnp.exp(m_t - top), axis=0, keepdims=True)
    lse_slots[pl.ds(my_rank, 1), :, 0:rows] = top[None]
    lse_slots[pl.ds(my_rank, 1), :, rows:LANES] = tot[None]

    def lse_copy(dz, dt, j):
        return pltpu.make_async_remote_copy(
            src_ref=lse_slots.at[my_rank], dst_ref=lse_slots.at[my_rank],
            send_sem=lse_send.at[0], recv_sem=lse_recv.at[0],
            device_id=peer_id(dz, dt), device_id_type=MESH,
        )

    for dz, dt, j in peers:
        lse_copy(dz, dt, j).start()

    for e in range(n_full - 1):
        y_copy(e).wait_send()
    y_last(0).wait_send()
    y_last(1).wait_send()
    all_of(lse_slots, lse_recv, len(peers)).wait()
    pairs = lse_slots[:, 0, :]
    top = jnp.max(pairs, axis=0, keepdims=True)
    scaled = pltpu.roll(pairs, rows, axis=1) * jnp.exp(pairs - top)
    tot = jnp.sum(scaled, axis=0, keepdims=True)
    lse_out[...] = jnp.broadcast_to(top + jnp.log(tot), (8, LANES))
    all_of(lse_slots, lse_send, len(peers)).wait()


def finish_kernel(n_full, rem, logits, lse, next_rows, out_hbm, sum_hbm, next_hbm, stage, sums, sem, small_sem):
    rows = stage.shape[0]
    next_copy = pltpu.make_async_copy(next_rows, next_hbm, small_sem.at[0])
    next_copy.start()
    sums[...] = lse[0:1, 0:rows]
    sum_copy = pltpu.make_async_copy(sums, sum_hbm, small_sem.at[1])
    sum_copy.start()
    log_sum = lse[...].T[:rows, 0:1]
    copies = []
    for r in range(rows // 8):
        here = slice(8 * r, 8 * r + 8)
        part = jnp.broadcast_to(log_sum[here], (8, LANES))
        for k in range(n_full + 1):
            cols = CHUNK if k < n_full else rem
            for b in range(0, cols, LANES):
                w = min(LANES, cols - b)
                at = k * CHUNK + b
                stage[here, at:at + w] = logits[k, here, b:b + w] - part[:, :w]
        copy = pltpu.make_async_copy(stage.at[here, :], out_hbm.at[here, :], sem.at[r])
        copy.start()
        copies.append(copy)
    for copy in [next_copy, sum_copy] + copies:
        copy.wait()


def solution(mesh):
    n_vp = mesh.shape["vp"]
    assert mesh.shape["tp"] == 4

    def per_device(hidden, lnf_gain, lnf_bias, emb_table, next_tok, eln_gain, eln_bias):
        rows, width = hidden.shape
        seg = emb_table.shape[0] // 4
        n_full, rem = divmod(seg, CHUNK)
        n_chunks = n_full + 1
        rem_pad = -(-rem // LANES) * LANES
        assert 2 * rows == LANES and n_vp == 4 and rem == 2 * LANES + LANES // 2 and n_full > DEPTH
        f32, bf16 = jnp.float32, jnp.bfloat16
        dma = pltpu.SemaphoreType.DMA
        hbm = pl.BlockSpec(memory_space=pltpu.HBM)
        vmem = pl.BlockSpec(memory_space=pltpu.VMEM)
        logits, lse, next_rows = pl.pallas_call(
            functools.partial(head_kernel, n_vp, n_full, rem, width),
            out_shape=(
                pltpu.VMEM((n_chunks, rows, CHUNK), f32),
                pltpu.VMEM((8, LANES), f32),
                pltpu.VMEM((rows, width), bf16),
            ),
            in_specs=[hbm] * 7,
            out_specs=(vmem, vmem, vmem),
            scratch_shapes=[
                pltpu.VMEM((rows, width), bf16),
                *[pltpu.VMEM((width,), f32)] * 4,
                pltpu.VMEM((1, rows), jnp.int32),
                pltpu.VMEM((DEPTH, 2, CHUNK, width), bf16),
                pltpu.VMEM((4, rem_pad, width), bf16),
                pltpu.VMEM((rows, width), bf16),
                pltpu.VMEM((rows, width), f32),
                pltpu.VMEM((n_vp, rows, width), f32),
                pltpu.VMEM((2 * n_chunks, rows, CHUNK), f32),
                pltpu.VMEM((2 * n_chunks, rows, CHUNK), f32),
                pltpu.VMEM((2 * n_chunks, rows, CHUNK), f32),
                pltpu.VMEM((n_chunks, rows, CHUNK), f32),
                pltpu.VMEM((rows, LANES), f32),
                pltpu.VMEM((rows, LANES), f32),
                pltpu.VMEM((4, 1, LANES), f32),
                pltpu.VMEM((4, 1, LANES), f32),
                pltpu.VMEM((n_vp * 4, 1, LANES), f32),
                dma((6,)), dma((DEPTH, 2)), dma((4,)),
                dma((1,)), dma((1,)), dma((1,)), dma((1,)),
                dma((2 * n_chunks,)), dma((2 * n_chunks,)),
                dma((n_chunks + 1,)), dma((n_chunks + 1,)),
                dma((n_vp - 1,)), dma((n_vp - 1,)),
                dma((1,)), dma((1,)),
                pltpu.SemaphoreType.REGULAR((3,)),
                pltpu.VMEM((rows + rows // 4, 2 * LANES), f32), pltpu.VMEM((rows + rows // 4, 2 * LANES), f32),
            ],
            compiler_params=pltpu.CompilerParams(
                collective_id=0, has_side_effects=True, vmem_limit_bytes=52 * 1024 * 1024
            ),
            name="head",
        )(
            *[
                pltpu.with_memory_space_constraint(a, pltpu.HBM)
                for a in (hidden, lnf_gain, lnf_bias, emb_table, next_tok.reshape(1, rows), eln_gain, eln_bias)
            ]
        )
        logprobs, log_sum, next_in = pl.pallas_call(
            functools.partial(finish_kernel, n_full, rem),
            out_shape=(
                jax.ShapeDtypeStruct((rows, seg), f32),
                jax.ShapeDtypeStruct((1, rows), f32),
                jax.ShapeDtypeStruct((rows, width), bf16),
            ),
            in_specs=[vmem, vmem, vmem],
            out_specs=(hbm, hbm, hbm),
            scratch_shapes=[pltpu.VMEM((rows, seg), f32), pltpu.VMEM((1, rows), f32), dma((rows // 8,)), dma((2,))],
            compiler_params=pltpu.CompilerParams(vmem_limit_bytes=24 * 1024 * 1024),
            name="finish",
        )(logits, lse, next_rows)
        return logprobs, log_sum.reshape(rows), next_in

    return jax.shard_map(
        per_device,
        mesh=mesh,
        in_specs=(P("dp", "tp"), P("tp"), P("tp"), P("vp", "tp"), P("dp"), P("tp"), P("tp")),
        out_specs=(P("dp", ("vp", "tp")), P("dp"), P("dp", "tp")),
        check_vma=False,
    )
```

```python
import functools

import jax
import jax.numpy as jnp
from jax import lax
from jax.experimental import pallas as pl
from jax.experimental.pallas import tpu as pltpu
from jax.sharding import PartitionSpec as P

NORM_EPS = 1e-5
CHUNK = 1536
LANES = 128
DEPTH = 3
LOWEST = -3.0e38
MESH = pl.DeviceIdType.MESH


def head_kernel(
    n_vp, n_full, rem, width,
    hid_hbm, gain1_hbm, bias1_hbm, tab_hbm, tok_hbm, gain2_hbm, bias2_hbm,
    logits, lse_out, next_out,
    hid, gain1, bias1, gain2, bias2, tok, tab, tab_rem, normed, picked, picked_rx,
    tx, rx, acc, y_rx, m_run, s_run, stat_slots, stat2_slots, lse_slots,
    in_sem, tab_sem, rem_sem, stat_send, stat_recv, stat2_send, stat2_recv,
    tx_send, tx_recv, y_send, y_recv, pick_send, pick_recv, lse_send, lse_recv, near_sem, y_tail, y_tail_rx,
):
    rows = hid.shape[0]
    n_chunks = n_full + 1
    seg = n_full * CHUNK + rem
    rem_pad = tab_rem.shape[1]
    vp = lax.axis_index("vp")
    tp = lax.axis_index("tp")
    chip_y = tp // 2
    core = lax.rem(tp, 2)
    sibling = tp + 1 - 2 * core
    across = lax.rem(tp + 2, 4)
    my_rank = vp * 4 + tp

    peers = []
    for dz in (*range(1, n_vp), 0):
        for dt in (2, 1, 3, 0):
            if dz or dt:
                peers.append((dz, dt, dz * 4 + dt))

    def peer_id(dz, dt):
        return {"vp": lax.rem(vp + dz, n_vp), "tp": lax.rem(tp + dt, 4)}

    hid_copy = pltpu.make_async_copy(hid_hbm, hid, in_sem.at[0])
    hid_copy.start()

    has_low = jnp.where(vp > 0, 1, 0)
    has_high = jnp.where(vp < n_vp - 1, 1, 0)

    def signal_vp(sem):
        @pl.when(vp > 0)
        def _():
            pl.semaphore_signal(sem, inc=1, device_id={"vp": vp - 1}, device_id_type=MESH)

        @pl.when(vp < n_vp - 1)
        def _():
            pl.semaphore_signal(sem, inc=1, device_id={"vp": vp + 1}, device_id_type=MESH)

    def signal_tp(sem):
        for dt in (2, 3, 1):
            pl.semaphore_signal(sem, inc=1, device_id=peer_id(0, dt), device_id_type=MESH)

    barrier = pltpu.get_barrier_semaphore()
    signal_tp(barrier)
    signal_vp(barrier)

    def seg_start(phase, which):
        y = chip_y + (1 - phase) * (1 - 2 * chip_y)
        c = core + (1 - which) * (1 - 2 * core)
        return (y * 2 + c) * seg

    def row_start(i, which):
        phase = jnp.where(i >= n_full, 1, 0)
        k = i - phase * n_full
        return pl.multiple_of(seg_start(phase, which) + k * CHUNK, 64)

    def tab_copy(i, which):
        slot = lax.rem(i, DEPTH)
        return pltpu.make_async_copy(
            tab_hbm.at[pl.ds(row_start(i, which), CHUNK), :], tab.at[slot, which], tab_sem.at[slot, which]
        )

    def rem_start(phase, which):
        return pl.multiple_of(seg_start(phase, which) + n_full * CHUNK, 64)

    def rem_copy(phase, which):
        return pltpu.make_async_copy(
            tab_hbm.at[pl.ds(rem_start(phase, which), rem), :],
            tab_rem.at[phase * 2 + which, pl.ds(0, rem), :],
            rem_sem.at[phase * 2 + which],
        )

    small = [
        pltpu.make_async_copy(gain1_hbm, gain1, in_sem.at[1]),
        pltpu.make_async_copy(bias1_hbm, bias1, in_sem.at[2]),
        pltpu.make_async_copy(gain2_hbm, gain2, in_sem.at[3]),
        pltpu.make_async_copy(bias2_hbm, bias2, in_sem.at[4]),
        pltpu.make_async_copy(tok_hbm, tok, in_sem.at[5]),
    ]

    picked[...] = jnp.zeros_like(picked)
    m_run[...] = jnp.full_like(m_run, LOWEST)
    s_run[...] = jnp.zeros_like(s_run)
    tab_rem[:, rem:, :] = jnp.zeros((4, rem_pad - rem, width), jnp.bfloat16)

    lane = lax.broadcasted_iota(jnp.int32, (rows, LANES), 1)

    def stat_row(x):
        s1 = jnp.sum(x, axis=1, keepdims=True)
        s2 = jnp.sum(x * x, axis=1, keepdims=True)
        return jnp.broadcast_to(jnp.concatenate([s1, s2], axis=0), (LANES, LANES)).T[0:1, :]

    def stat_copy(slots, send, recv, d):
        return pltpu.make_async_remote_copy(
            src_ref=slots.at[tp], dst_ref=slots.at[tp], send_sem=send.at[0], recv_sem=recv.at[0],
            device_id=peer_id(0, d), device_id_type=MESH,
        )

    def all_of(slots, sem, count):
        return pltpu.make_async_copy(slots.at[pl.ds(0, count)], slots.at[pl.ds(0, count)], sem.at[0])

    def norm(x, slots, send, recv, gain, bias):
        all_of(slots, recv, 3).wait()
        total = (slots[0] + slots[1]) + (slots[2] + slots[3])
        full_width = 4.0 * width
        total = jnp.broadcast_to(total, (8, LANES)) / full_width
        mean = total
        var = pltpu.roll(total, rows, axis=1) - mean * mean
        inv = lax.rsqrt(var + NORM_EPS)
        row = lax.broadcasted_iota(jnp.int32, (8, LANES), 0)
        back = jnp.where(row == 0, mean, inv).T
        mean_c = back[:rows, 0:1]
        inv_c = back[:rows, 1:2]
        return (x - mean_c) * inv_c * gain + bias

    hid_copy.wait()
    x1 = hid[...].astype(jnp.float32)
    stat_slots[pl.ds(tp, 1)] = stat_row(x1)[None]
    pl.semaphore_wait(barrier, 3 + has_low + has_high)
    for d in (2, 3, 1):
        stat_copy(stat_slots, stat_send, stat_recv, d).start()
    for copy in small:
        copy.start()
    for which in range(2):
        rem_copy(0, which).start()
    for i in range(min(DEPTH - 1, 2 * n_full)):
        for which in range(2):
            tab_copy(i, which).start()
    for which in range(2):
        rem_copy(1, which).start()
    for copy in small:
        copy.wait()
    normed[...] = norm(
        x1, stat_slots, stat_send, stat_recv, gain1[...].reshape(1, width), bias1[...].reshape(1, width)
    ).astype(jnp.bfloat16)

    def tx_copy(e, cols=None):
        view = (lambda r: r.at[e]) if cols is None else (lambda r: r.at[e, :, pl.ds(0, cols)])
        return pltpu.make_async_remote_copy(
            src_ref=view(tx), dst_ref=view(rx), send_sem=tx_send.at[e], recv_sem=tx_recv.at[e],
            device_id={"tp": sibling}, device_id_type=MESH,
        )

    middle = n_full - 8
    sizes = [1, 1, 2] + [4] * (middle // 4) + [middle % 4] * (middle % 4 > 0) + [2, 1, 1]
    groups = [(sum(sizes[:g]), n) for g, n in enumerate(sizes)]

    def y_copy(e, n):
        return pltpu.make_async_remote_copy(
            src_ref=acc.at[pl.ds(e, n)], dst_ref=y_rx.at[pl.ds(e, n)],
            send_sem=y_send.at[e], recv_sem=y_recv.at[e],
            device_id={"tp": across}, device_id_type=MESH,
        )

    half = LANES // 2
    whole = rem - half

    def y_tail_copy():
        return pltpu.make_async_remote_copy(
            src_ref=y_tail, dst_ref=y_tail_rx, send_sem=y_send.at[n_full], recv_sem=y_recv.at[n_full],
            device_id={"tp": across}, device_id_type=MESH,
        )

    def pack_tail(block):
        y_tail[0:rows, :] = block[:, 0:whole]
        low = block[0:rows // 2, whole:whole + LANES]
        high = pltpu.roll(block[rows // 2:rows, whole:whole + LANES], half, axis=1)
        both = jnp.where(lane[0:rows // 2] < half, low, high)
        y_tail[rows:rows + rows // 4, 0:LANES] = both[0:rows // 4]
        y_tail[rows:rows + rows // 4, LANES:2 * LANES] = both[rows // 4:rows // 2]

    def tail_block(b):
        if (b + 1) * LANES <= whole:
            return y_tail_rx[0:rows, b * LANES:(b + 1) * LANES]
        both = jnp.concatenate(
            [y_tail_rx[rows:rows + rows // 4, 0:LANES], y_tail_rx[rows:rows + rows // 4, LANES:2 * LANES]], axis=0
        )
        return jnp.concatenate([both, pltpu.roll(both, half, axis=1)], axis=0)

    def partial(block):
        return lax.dot_general(
            normed[...], block, (((1,), (1,)), ((), ())), preferred_element_type=jnp.float32
        )

    tok_col = jnp.broadcast_to(tok[...], (8, rows)).T[:, 0:1]
    tok_local = tok_col - vp * (4 * seg)

    def add_picked(block, start):
        n = block.shape[0]
        at = lax.broadcasted_iota(jnp.int32, (rows, n), 1)
        hot = jnp.where(at == tok_local - start, 1.0, 0.0).astype(jnp.bfloat16)
        picked[...] += lax.dot_general(
            hot, block, (((1,), (0,)), ((), ())), preferred_element_type=jnp.float32
        )

    def add_picked_rem(phase, which):
        at = lax.broadcasted_iota(jnp.int32, (rows, rem_pad), 1)
        hit = (at == tok_local - rem_start(phase, which)) & (at < rem)
        hot = jnp.where(hit, 1.0, 0.0).astype(jnp.bfloat16)
        picked[...] += lax.dot_general(
            hot, tab_rem[phase * 2 + which], (((1,), (0,)), ((), ())), preferred_element_type=jnp.float32
        )

    def run_phase(phase):
        base = phase * n_chunks

        last = base + n_full
        first = phase * n_full
        slot0 = first % DEPTH
        rem_copy(phase, 0).wait()
        tx[last, :, 0:rem_pad] = partial(tab_rem[phase * 2])
        tx_copy(last, rem_pad).start()
        tab_copy(first, 0).wait()
        tx[base] = partial(tab[slot0, 0])
        tx_copy(base).start()
        rem_copy(phase, 1).wait()
        mine = partial(tab_rem[phase * 2 + 1])
        acc[last, :, 0:rem_pad] = mine
        tab_copy(first, 1).wait()
        acc[base] = partial(tab[slot0, 1])
        tx_copy(last, rem_pad).wait_recv()
        if phase == 0:
            pack_tail(acc[last, :, 0:rem_pad] + rx[last, :, 0:rem_pad])
            y_tail_copy().start()
        else:
            acc[last, :, 0:rem_pad] = acc[last, :, 0:rem_pad] + rx[last, :, 0:rem_pad]

        def finish(e):
            tx_copy(e).wait_recv()
            acc[e] = acc[e] + rx[e]
            if phase == 0:
                for g, n in groups:
                    @pl.when(e == g + n - 1)
                    def _(g=g, n=n):
                        y_copy(g, n).start()

        tab_copy(first + DEPTH - 1, 0).start()
        tab_copy(first + DEPTH - 1, 1).start()
        add_picked_rem(phase, 0)
        add_picked_rem(phase, 1)
        finish(base)
        add_picked(tab[slot0, 0], row_start(first, 0))
        add_picked(tab[slot0, 1], row_start(first, 1))

        def body(i, carry):
            k = i - phase * n_full
            e = base + k

            @pl.when(i + DEPTH - 1 < 2 * n_full)
            def _():
                tab_copy(i + DEPTH - 1, 0).start()
                tab_copy(i + DEPTH - 1, 1).start()

            slot = lax.rem(i, DEPTH)
            tab_copy(i, 0).wait()
            tx[e] = partial(tab[slot, 0])
            tx_copy(e).start()
            tab_copy(i, 1).wait()
            acc[e] = partial(tab[slot, 1])

            @pl.when(k > 1)
            def _():
                finish(e - 1)

            add_picked(tab[slot, 0], row_start(i, 0))
            add_picked(tab[slot, 1], row_start(i, 1))
            return carry

        lax.fori_loop(first + 1, first + n_full, body, 0)
        finish(last - 1)

    signal_vp(near_sem.at[0])
    run_phase(0)
    pl.semaphore_wait(near_sem.at[0], has_low + has_high)
    signal_vp(near_sem.at[1])
    run_phase(1)
    pl.semaphore_wait(near_sem.at[1], has_low + has_high)
    signal_tp(near_sem.at[2])

    def pick_copy(dz):
        return pltpu.make_async_remote_copy(
            src_ref=picked, dst_ref=picked_rx.at[vp], send_sem=pick_send.at[dz - 1], recv_sem=pick_recv.at[dz - 1],
            device_id=peer_id(dz, 0), device_id_type=MESH,
        )

    for dz in range(1, n_vp):
        pick_copy(dz).start()
    picked_rx[pl.ds(vp, 1)] = picked[...][None]
    for dz in range(1, n_vp):
        pick_copy(dz).wait_recv()
    x2 = picked_rx[0]
    for z in range(1, n_vp):
        x2 = x2 + picked_rx[z]
    stat2_slots[pl.ds(tp, 1)] = stat_row(x2)[None]
    for d in (2, 3, 1):
        stat_copy(stat2_slots, stat2_send, stat2_recv, d).start()
    next_out[...] = norm(
        x2, stat2_slots, stat2_send, stat2_recv, gain2[...].reshape(1, width), bias2[...].reshape(1, width)
    ).astype(jnp.bfloat16)

    def absorb(k, cols):
        e = n_chunks + k
        blocks = cols // LANES
        top = m_run[...]
        for b in range(blocks):
            sl = pl.ds(b * LANES, LANES)
            z = acc[e, :, sl] + (y_rx[k, :, sl] if cols == CHUNK else tail_block(b))
            logits[k, :, sl] = z
            if cols != CHUNK and (b + 1) * LANES > rem:
                z = jnp.where(lane < rem - b * LANES, z, -jnp.inf)
            top = jnp.maximum(top, z)
        total = s_run[...] * jnp.exp(m_run[...] - top)
        for b in range(blocks):
            z = logits[k, :, pl.ds(b * LANES, LANES)]
            if cols != CHUNK and (b + 1) * LANES > rem:
                z = jnp.where(lane < rem - b * LANES, z, -jnp.inf)
            total = total + jnp.exp(z - top)
        m_run[...] = top
        s_run[...] = total

    def absorb_body(k, carry):
        absorb(k, CHUNK)
        tx_copy(k).wait_send()
        tx_copy(n_chunks + k).wait_send()
        return carry

    y_tail_copy().wait_recv()
    absorb(n_full, rem_pad)
    pl.semaphore_wait(near_sem.at[2], 3)
    tx_copy(n_full, rem_pad).wait_send()
    tx_copy(n_chunks + n_full, rem_pad).wait_send()
    y_tail_copy().wait_send()
    all_of(stat_slots, stat_send, 3).wait()
    all_of(stat2_slots, stat2_send, 3).wait()
    for dz in range(1, n_vp):
        pick_copy(dz).wait_send()
    for g, n in groups:
        y_copy(g, n).wait_recv()
        lax.fori_loop(g, g + n, absorb_body, 0)

    m_t = m_run[...].T
    top = jnp.max(m_t, axis=0, keepdims=True)
    tot = jnp.sum(s_run[...].T * jnp.exp(m_t - top), axis=0, keepdims=True)
    lse_slots[pl.ds(my_rank, 1), :, 0:rows] = top[None]
    lse_slots[pl.ds(my_rank, 1), :, rows:LANES] = tot[None]

    def lse_copy(dz, dt, j):
        return pltpu.make_async_remote_copy(
            src_ref=lse_slots.at[my_rank], dst_ref=lse_slots.at[my_rank],
            send_sem=lse_send.at[0], recv_sem=lse_recv.at[0],
            device_id=peer_id(dz, dt), device_id_type=MESH,
        )

    for dz, dt, j in peers:
        lse_copy(dz, dt, j).start()

    for g, n in groups:
        y_copy(g, n).wait_send()
    all_of(lse_slots, lse_recv, len(peers)).wait()
    pairs = lse_slots[:, 0, :]
    top = jnp.max(pairs, axis=0, keepdims=True)
    scaled = pltpu.roll(pairs, rows, axis=1) * jnp.exp(pairs - top)
    tot = jnp.sum(scaled, axis=0, keepdims=True)
    lse_out[...] = jnp.broadcast_to(top + jnp.log(tot), (8, LANES))
    all_of(lse_slots, lse_send, len(peers)).wait()


def finish_kernel(n_full, rem, logits, lse, next_rows, out_hbm, sum_hbm, next_hbm, stage, sums, sem, small_sem):
    rows = stage.shape[0]
    next_copy = pltpu.make_async_copy(next_rows, next_hbm, small_sem.at[0])
    next_copy.start()
    sums[...] = lse[0:1, 0:rows]
    sum_copy = pltpu.make_async_copy(sums, sum_hbm, small_sem.at[1])
    sum_copy.start()
    log_sum = lse[...].T[:rows, 0:1]
    copies = []
    for r in range(rows // 8):
        here = slice(8 * r, 8 * r + 8)
        part = jnp.broadcast_to(log_sum[here], (8, LANES))
        for k in range(n_full + 1):
            cols = CHUNK if k < n_full else rem
            for b in range(0, cols, LANES):
                w = min(LANES, cols - b)
                at = k * CHUNK + b
                stage[here, at:at + w] = logits[k, here, b:b + w] - part[:, :w]
        copy = pltpu.make_async_copy(stage.at[here, :], out_hbm.at[here, :], sem.at[r])
        copy.start()
        copies.append(copy)
    for copy in [next_copy, sum_copy] + copies:
        copy.wait()


def solution(mesh):
    n_vp = mesh.shape["vp"]
    assert mesh.shape["tp"] == 4

    def per_device(hidden, lnf_gain, lnf_bias, emb_table, next_tok, eln_gain, eln_bias):
        rows, width = hidden.shape
        seg = emb_table.shape[0] // 4
        n_full, rem = divmod(seg, CHUNK)
        n_chunks = n_full + 1
        rem_pad = -(-rem // LANES) * LANES
        assert 2 * rows == LANES and n_vp == 4 and rem == 2 * LANES + LANES // 2 and n_full >= 8
        f32, bf16 = jnp.float32, jnp.bfloat16
        dma = pltpu.SemaphoreType.DMA
        hbm = pl.BlockSpec(memory_space=pltpu.HBM)
        vmem = pl.BlockSpec(memory_space=pltpu.VMEM)
        logits, lse, next_rows = pl.pallas_call(
            functools.partial(head_kernel, n_vp, n_full, rem, width),
            out_shape=(
                pltpu.VMEM((n_chunks, rows, CHUNK), f32),
                pltpu.VMEM((8, LANES), f32),
                pltpu.VMEM((rows, width), bf16),
            ),
            in_specs=[hbm] * 7,
            out_specs=(vmem, vmem, vmem),
            scratch_shapes=[
                pltpu.VMEM((rows, width), bf16),
                *[pltpu.VMEM((width,), f32)] * 4,
                pltpu.VMEM((1, rows), jnp.int32),
                pltpu.VMEM((DEPTH, 2, CHUNK, width), bf16),
                pltpu.VMEM((4, rem_pad, width), bf16),
                pltpu.VMEM((rows, width), bf16),
                pltpu.VMEM((rows, width), f32),
                pltpu.VMEM((n_vp, rows, width), f32),
                pltpu.VMEM((2 * n_chunks, rows, CHUNK), f32),
                pltpu.VMEM((2 * n_chunks, rows, CHUNK), f32),
                pltpu.VMEM((2 * n_chunks, rows, CHUNK), f32),
                pltpu.VMEM((n_chunks, rows, CHUNK), f32),
                pltpu.VMEM((rows, LANES), f32),
                pltpu.VMEM((rows, LANES), f32),
                pltpu.VMEM((4, 1, LANES), f32),
                pltpu.VMEM((4, 1, LANES), f32),
                pltpu.VMEM((n_vp * 4, 1, LANES), f32),
                dma((6,)), dma((DEPTH, 2)), dma((4,)),
                dma((1,)), dma((1,)), dma((1,)), dma((1,)),
                dma((2 * n_chunks,)), dma((2 * n_chunks,)),
                dma((n_chunks,)), dma((n_chunks,)),
                dma((n_vp - 1,)), dma((n_vp - 1,)),
                dma((1,)), dma((1,)),
                pltpu.SemaphoreType.REGULAR((3,)),
                pltpu.VMEM((rows + rows // 4, 2 * LANES), f32), pltpu.VMEM((rows + rows // 4, 2 * LANES), f32),
            ],
            compiler_params=pltpu.CompilerParams(
                collective_id=0, has_side_effects=True, vmem_limit_bytes=52 * 1024 * 1024
            ),
            name="head",
        )(
            *[
                pltpu.with_memory_space_constraint(a, pltpu.HBM)
                for a in (hidden, lnf_gain, lnf_bias, emb_table, next_tok.reshape(1, rows), eln_gain, eln_bias)
            ]
        )
        logprobs, log_sum, next_in = pl.pallas_call(
            functools.partial(finish_kernel, n_full, rem),
            out_shape=(
                jax.ShapeDtypeStruct((rows, seg), f32),
                jax.ShapeDtypeStruct((1, rows), f32),
                jax.ShapeDtypeStruct((rows, width), bf16),
            ),
            in_specs=[vmem, vmem, vmem],
            out_specs=(hbm, hbm, hbm),
            scratch_shapes=[pltpu.VMEM((rows, seg), f32), pltpu.VMEM((1, rows), f32), dma((rows // 8,)), dma((2,))],
            compiler_params=pltpu.CompilerParams(vmem_limit_bytes=24 * 1024 * 1024),
            name="finish",
        )(logits, lse, next_rows)
        return logprobs, log_sum.reshape(rows), next_in

    return jax.shard_map(
        per_device,
        mesh=mesh,
        in_specs=(P("dp", "tp"), P("tp"), P("tp"), P("vp", "tp"), P("dp"), P("tp"), P("tp")),
        out_specs=(P("dp", ("vp", "tp")), P("dp"), P("dp", "tp")),
        check_vma=False,
    )
```
